32 devices in a mesh: rep: 16 (over z, y, core), shard: 2 (over x).
Axes of the slice: x: 2, y: 2, z: 4, core: 2. Of those that a mesh axis runs over, the one named last changes fastest.
Arguments:
- tokens: bfloat16 [32768, 768], P(('rep', 'shard')), may hold values from -6 to 6
- ln1_gain: bfloat16 [768], P('shard'), may hold values from 0.5 to 1.5
- ln1_bias: bfloat16 [768], P('shard'), may hold values from -1.5 to 1.5
- qkv_weight: bfloat16 [768, 2304], P('shard'), may hold values from -0.21875 to 0.21875
- qv_bias: bfloat16 [1536], P('shard'), may hold values from -1.5 to 1.5
- proj_weight: bfloat16 [768, 768], P('shard'), may hold values from -0.875 to 0.875
- proj_bias: bfloat16 [768], P('shard'), may hold values from -1.5 to 1.5
- ln2_gain: bfloat16 [768], P('shard'), may hold values from 0.5 to 1.5
- ln2_bias: bfloat16 [768], P('shard'), may hold values from -1.5 to 1.5
- fc_weight: bfloat16 [768, 3072], P('shard'), may hold values from -0.21875 to 0.21875
- fc_bias: bfloat16 [3072], P('shard'), may hold values from -1.5 to 1.5
- out_weight: bfloat16 [3072, 768], P('shard'), may hold values from -0.15625 to 0.15625
- out_bias: bfloat16 [768], P('shard'), may hold values from -1.5 to 1.5
- cotangent: bfloat16 [32768, 768], P(('rep', 'shard')), may hold values from -6 to 6
Outputs:
- block_out: bfloat16 [32768, 768], P(('rep', 'shard'))
- input_gradient: bfloat16 [32768, 768], P(('rep', 'shard'))
- ln1_gain_grad: float32 [768], P('shard')
- ln1_bias_grad: float32 [768], P('shard')
- qkv_weight_grad: float32 [768, 2304], P('shard')
- qv_bias_grad: float32 [1536], P('shard')
- proj_weight_grad: float32 [768, 768], P('shard')
- proj_bias_grad: float32 [768], P('shard')
- ln2_gain_grad: float32 [768], P('shard')
- ln2_bias_grad: float32 [768], P('shard')
- fc_weight_grad: float32 [768, 3072], P('shard')
- fc_bias_grad: float32 [3072], P('shard')
- out_weight_grad: float32 [3072, 768], P('shard')
- out_bias_grad: float32 [768], P('shard')
The draws below stay inside these ranges and needn't reach their ends.
All inputs are finite; a program needn't handle non-finite values.
Results may differ from the reference program's by a relative error of at most 0.018.
Values may be sent and summed in bfloat16 or wider, within the bound.
A program may use at most 256 MiB of HBM per device.

```python
import jax
import jax.numpy as jnp
from jax import lax

D = 768
HEADS = 12
HEAD_DIM = 64
FF = 3072
SEQ_LEN = 512
TOKENS = 32768


def block_levels(key, dims, cuts, smallest, high):
    level, own = 1.0, jax.random.fold_in(key, 6)
    for axis_at, shards_of in cuts:
        steps = jnp.exp(jax.random.uniform(jax.random.fold_in(own, axis_at), (shards_of,), jnp.float32, smallest / len(cuts), high / len(cuts)))
        level = level * jnp.repeat(steps, dims[axis_at] // shards_of).reshape([-1 if axis == axis_at else 1 for axis in range(len(dims))])
    return level


def gaussian(own_key, shape, deviation, limit, shards=(), kind=jnp.bfloat16):
    level = block_levels(own_key, shape, shards, -0.22, 0.18) if shards else 1.0
    result = jax.random.normal(own_key, shape, jnp.float32) * deviation * level
    return jnp.minimum(jnp.maximum(result, -limit), limit).astype(kind)


def setup_inputs(seed: int = 0) -> dict:
    key_list = jax.random.split(jax.random.key(seed), 15)
    tokens = gaussian(key_list[0], (TOKENS, D), 1.0, 6.0, ((0, 32),))
    ln1_gain = jnp.clip(1.0 + 0.1 * jax.random.normal(key_list[1], (D,), jnp.float32), 0.5, 1.5).astype(jnp.bfloat16)
    ln1_bias = gaussian(key_list[2], (D,), 0.3, 1.5, ((0, 2),))
    qkv_weight = gaussian(key_list[3], (D, 3 * D), D ** -0.5, 0.21875, ((0, 2),))
    qv_bias = gaussian(key_list[4], (2 * D,), 0.3, 1.5, ((0, 2),))
    proj_weight = gaussian(key_list[5], (D, D), (D // 16) ** -0.5, 0.875, ((0, 2),))
    proj_bias = gaussian(key_list[6], (D,), 0.3, 1.5, ((0, 2),))
    ln2_gain = jnp.clip(1.0 + 0.1 * jax.random.normal(key_list[7], (D,), jnp.float32), 0.5, 1.5).astype(jnp.bfloat16)
    ln2_bias = gaussian(key_list[8], (D,), 0.3, 1.5, ((0, 2),))
    fc_weight = gaussian(key_list[9], (D, FF), D ** -0.5, 0.21875, ((0, 2),))
    fc_bias = gaussian(key_list[10], (FF,), 0.3, 1.5, ((0, 2),))
    out_weight = gaussian(key_list[11], (FF, D), (FF // 2) ** -0.5, 0.15625, ((0, 2),))
    out_bias = gaussian(key_list[12], (D,), 0.3, 1.5, ((0, 2),))
    cotangent = gaussian(key_list[13], (TOKENS, D), 1.0, 6.0, ((0, 32),))
    return dict(tokens=tokens, ln1_gain=ln1_gain, ln1_bias=ln1_bias, qkv_weight=qkv_weight, qv_bias=qv_bias, proj_weight=proj_weight, proj_bias=proj_bias, ln2_gain=ln2_gain, ln2_bias=ln2_bias, fc_weight=fc_weight, fc_bias=fc_bias, out_weight=out_weight, out_bias=out_bias, cotangent=cotangent)


EPS = 1e-05
GELU_C = 0.7978845608028654

def layer_norm_rows(value_rows):
    center = value_rows - lax.optimization_barrier(jnp.mean(value_rows, axis=-1, keepdims=True))
    inverse_deviation = lax.rsqrt(lax.optimization_barrier(jnp.mean(center * center, axis=-1, keepdims=True)) + EPS)
    return (center * inverse_deviation, inverse_deviation)

def causal_scores(query_rows, key_portion):
    scores = jnp.einsum('sqhd,skhd->shqk', query_rows.astype(jnp.float32), key_portion.astype(jnp.float32)) * HEAD_DIM ** (-0.5)
    rows = lax.broadcasted_iota(jnp.int32, (SEQ_LEN, SEQ_LEN), 0)
    cols = lax.broadcasted_iota(jnp.int32, (SEQ_LEN, SEQ_LEN), 1)
    return jnp.where(cols <= rows, scores, -1e+30)

def forward(tokens, params):
    first_norm_gain, first_norm_bias, wqkv, bqv, wproj, bproj, second_norm_gain, second_norm_bias, wfc, bfc, wout, bout = params
    width = tokens.shape[1]
    seqs = tokens.shape[0] // SEQ_LEN
    input_wide = tokens.astype(jnp.float32)
    first_centered_normalized, first_inverse_deviation = layer_norm_rows(input_wide)
    first_normalized = (first_centered_normalized * first_norm_gain.astype(jnp.float32) + first_norm_bias.astype(jnp.float32)).astype(jnp.bfloat16)
    bias_full = jnp.concatenate([bqv[:width].astype(jnp.float32), jnp.zeros((width,), jnp.float32), bqv[width:].astype(jnp.float32)])
    qkv = (jnp.dot(first_normalized, wqkv, preferred_element_type=jnp.float32) + bias_full).astype(jnp.bfloat16)
    qkv = qkv.reshape(seqs, SEQ_LEN, 3, HEADS, HEAD_DIM)
    query_rows, key_portion, value_rows = (qkv[:, :, 0], qkv[:, :, 1], qkv[:, :, 2])
    scores = causal_scores(query_rows, key_portion)
    top = lax.optimization_barrier(jnp.max(scores, axis=-1, keepdims=True))
    log_sum_exponent = top + jnp.log(lax.optimization_barrier(jnp.sum(jnp.exp(scores - top), axis=-1, keepdims=True)))
    probs = jnp.exp(scores - log_sum_exponent).astype(jnp.bfloat16)
    attention_result = jnp.einsum('shqk,skhd->sqhd', probs.astype(jnp.float32), value_rows.astype(jnp.float32)).astype(jnp.bfloat16)
    attention_result = attention_result.reshape(seqs * SEQ_LEN, width)
    residual_hidden = input_wide + jnp.dot(attention_result, wproj, preferred_element_type=jnp.float32) + bproj.astype(jnp.float32)
    second_centered_normalized, second_inverse_deviation = layer_norm_rows(residual_hidden)
    second_normalized = (second_centered_normalized * second_norm_gain.astype(jnp.float32) + second_norm_bias.astype(jnp.float32)).astype(jnp.bfloat16)
    preactivation = jnp.dot(second_normalized, wfc, preferred_element_type=jnp.float32) + bfc.astype(jnp.float32)
    tanh_term = jnp.tanh(GELU_C * (preactivation + 0.044715 * preactivation * preactivation * preactivation))
    activation_output = (0.5 * preactivation * (1.0 + tanh_term)).astype(jnp.bfloat16)
    block_out = (residual_hidden + jnp.dot(activation_output, wout, preferred_element_type=jnp.float32) + bout.astype(jnp.float32)).astype(jnp.bfloat16)
    saved_residuals = (first_centered_normalized, first_inverse_deviation, first_normalized, query_rows, key_portion, value_rows, log_sum_exponent, attention_result, second_centered_normalized, second_inverse_deviation, second_normalized, preactivation, activation_output)
    return (block_out, saved_residuals)

def layer_norm_backward(normalized_gradient, norm_gain, centered_normalized, inverse_deviation):
    scaled_scores = normalized_gradient * norm_gain.astype(jnp.float32)
    return inverse_deviation * (scaled_scores - lax.optimization_barrier(jnp.mean(scaled_scores, axis=-1, keepdims=True)) - centered_normalized * lax.optimization_barrier(jnp.mean(scaled_scores * centered_normalized, axis=-1, keepdims=True)))

def backward(saved_residuals, params, cotangent):
    first_norm_gain, first_norm_bias, wqkv, bqv, wproj, bproj, second_norm_gain, second_norm_bias, wfc, bfc, wout, bout = params
    first_centered_normalized, first_inverse_deviation, first_normalized, query_rows, key_portion, value_rows, log_sum_exponent, attention_result, second_centered_normalized, second_inverse_deviation, second_normalized, preactivation, activation_output = saved_residuals
    width = cotangent.shape[1]
    seqs = cotangent.shape[0] // SEQ_LEN
    output_gradient_wide = cotangent.astype(jnp.float32)
    out_w_grad = jnp.dot(activation_output.T, cotangent, preferred_element_type=jnp.float32)
    out_b_grad = lax.optimization_barrier(jnp.sum(output_gradient_wide, axis=0))
    d_act = jnp.dot(cotangent, wout.T, preferred_element_type=jnp.float32)
    tanh_term = jnp.tanh(GELU_C * (preactivation + 0.044715 * preactivation * preactivation * preactivation))
    slope = 0.5 * (1.0 + tanh_term) + 0.5 * preactivation * (1.0 - tanh_term * tanh_term) * GELU_C * (1.0 + 0.134145 * preactivation * preactivation)
    d_pre32 = d_act * slope
    fc_b_grad = lax.optimization_barrier(jnp.sum(d_pre32, axis=0))
    d_pre = d_pre32.astype(jnp.bfloat16)
    fc_w_grad = jnp.dot(second_normalized.T, d_pre, preferred_element_type=jnp.float32)
    second_normalized_gradient = jnp.dot(d_pre, wfc.T, preferred_element_type=jnp.float32)
    second_gain_gradient = lax.optimization_barrier(jnp.sum(second_normalized_gradient * second_centered_normalized, axis=0))
    b2_grad = lax.optimization_barrier(jnp.sum(second_normalized_gradient, axis=0))
    residual_gradient = output_gradient_wide + layer_norm_backward(second_normalized_gradient, second_norm_gain, second_centered_normalized, second_inverse_deviation)
    d_hres_b = residual_gradient.astype(jnp.bfloat16)
    proj_w_grad = jnp.dot(attention_result.T, d_hres_b, preferred_element_type=jnp.float32)
    proj_b_grad = lax.optimization_barrier(jnp.sum(residual_gradient, axis=0))
    d_att = jnp.dot(d_hres_b, wproj.T, preferred_element_type=jnp.float32).astype(jnp.bfloat16)
    d_att = d_att.reshape(seqs, SEQ_LEN, HEADS, HEAD_DIM)
    att4 = attention_result.reshape(seqs, SEQ_LEN, HEADS, HEAD_DIM)
    delta = jnp.einsum('sqhd,sqhd->shq', d_att.astype(jnp.float32), att4.astype(jnp.float32))
    scores = causal_scores(query_rows, key_portion)
    probs32 = jnp.exp(scores - log_sum_exponent)
    probs = probs32.astype(jnp.bfloat16)
    d_value = jnp.einsum('shqk,sqhd->skhd', probs.astype(jnp.float32), d_att.astype(jnp.float32))
    d_prob = jnp.einsum('sqhd,skhd->shqk', d_att.astype(jnp.float32), value_rows.astype(jnp.float32))
    d_scores = (probs32 * (d_prob - delta[..., None]) * HEAD_DIM ** (-0.5)).astype(jnp.bfloat16)
    d_query = jnp.einsum('shqk,skhd->sqhd', d_scores.astype(jnp.float32), key_portion.astype(jnp.float32))
    d_key = jnp.einsum('shqk,sqhd->skhd', d_scores.astype(jnp.float32), query_rows.astype(jnp.float32))
    d_qkv32 = jnp.stack([d_query, d_key, d_value], axis=2).reshape(seqs * SEQ_LEN, 3 * width)
    qv_b_grad = jnp.concatenate([lax.optimization_barrier(jnp.sum(d_qkv32[:, :width], axis=0)), lax.optimization_barrier(jnp.sum(d_qkv32[:, 2 * width:], axis=0))])
    d_qkv = d_qkv32.astype(jnp.bfloat16)
    qkv_w_grad = jnp.dot(first_normalized.T, d_qkv, preferred_element_type=jnp.float32)
    first_normalized_gradient = jnp.dot(d_qkv, wqkv.T, preferred_element_type=jnp.float32)
    first_gain_gradient = lax.optimization_barrier(jnp.sum(first_normalized_gradient * first_centered_normalized, axis=0))
    b1_grad = lax.optimization_barrier(jnp.sum(first_normalized_gradient, axis=0))
    input_gradient = (residual_gradient + layer_norm_backward(first_normalized_gradient, first_norm_gain, first_centered_normalized, first_inverse_deviation)).astype(jnp.bfloat16)
    grads = (first_gain_gradient, b1_grad, qkv_w_grad, qv_b_grad, proj_w_grad, proj_b_grad, second_gain_gradient, b2_grad, fc_w_grad, fc_b_grad, out_w_grad, out_b_grad)
    return (input_gradient, grads)

def reference(tokens, ln1_gain, ln1_bias, qkv_weight, qv_bias, proj_weight, proj_bias, ln2_gain, ln2_bias, fc_weight, fc_bias, out_weight, out_bias, cotangent):
    params = (ln1_gain, ln1_bias, qkv_weight, qv_bias, proj_weight, proj_bias, ln2_gain, ln2_bias, fc_weight, fc_bias, out_weight, out_bias)
    width = tokens.shape[1]
    group_rows = 8 * SEQ_LEN
    groups = tokens.shape[0] // group_rows
    tok_groups = tokens.reshape(groups, group_rows, width)
    cot_groups = cotangent.reshape(groups, group_rows, width)
    zeros = tuple((jnp.zeros(p.shape, jnp.float32) for p in params))

    def one_group(carry, pair):
        block_out, saved_residuals = forward(pair[0], params)
        input_gradient, grads = backward(saved_residuals, params, pair[1])
        carry = tuple((c + g for c, g in zip(carry, grads)))
        return (carry, (block_out, input_gradient))
    totals, (outs, dxs) = lax.scan(one_group, zeros, (tok_groups, cot_groups))
    outs = outs.reshape(tokens.shape)
    dxs = dxs.reshape(tokens.shape)
    return (outs, dxs, totals[0], totals[1], totals[2], totals[3], totals[4], totals[5], totals[6], totals[7], totals[8], totals[9], totals[10], totals[11])
```

```python
import functools
import types

import jax
import jax.numpy as jnp
from jax import lax
from jax.experimental import pallas as pl
from jax.experimental.pallas import tpu as pltpu
from jax.sharding import PartitionSpec as P

HEAD_DIM = 64
SEQ_LEN = 512
EPS = 1e-05
GELU_C = 0.7978845608028654
F32, BF16 = jnp.float32, jnp.bfloat16
MESH = pl.DeviceIdType.MESH
LANES = 128
BLK = 256
NEG = -1e30
VECS = ("ln1g", "ln1b", "qvb", "projb", "ln2g", "ln2b", "outb", "fcb")


def dims_of(mesh, rows, width, ff):
    d = types.SimpleNamespace()
    d.R, d.S = mesh.shape["rep"], mesh.shape["shard"]
    d.nb = d.R.bit_length() - 1
    assert d.S == 2 and d.R == 1 << d.nb and d.nb >= 4
    d.M, d.D, d.FF = rows, width, ff
    d.DH, d.FH = width // 2, ff // 2
    d.NJ = ff // BLK
    d.NP = width // BLK
    d.NH2 = width // LANES
    d.NSEQ = rows // SEQ_LEN
    d.NCH = 2 * d.NJ + 4 * d.NP
    d.PR = d.DH // 8
    d.PO = LANES // 8
    half = {"qvb": width, "fcb": ff // 2}
    d.off, at = {}, 0
    for name in VECS:
        d.off[name] = (at, half.get(name, width // 2))
        at += d.off[name][1]
    d.NV = at
    d.lag = [2, 3, 3, 2, 2] + [2] * (d.nb - 4) + [2, 2, 3, 2]
    d.NS = 2 * max(d.lag)
    d.first_ag = d.nb + 1
    d.B, d.E, at = [], [], 0
    for i, lag in enumerate(d.lag + [2]):
        at += i == d.first_ag
        d.B.append(at)
        at += lag
        d.E.append(at)
    d.V0 = 2 * d.NJ + d.NP
    d.GU = 2 * d.NSEQ
    d.GV = d.GU + 3
    d.NVS = d.V0 + d.NP * d.GV
    d.NQP = 6
    d.QW = 3 * width // d.NQP
    return d


def scratch_of(d):
    vm, sem = pltpu.VMEM, pltpu.SemaphoreType.DMA
    P8 = (2, d.PR, LANES)
    n_x = d.nb - 4
    items = [
        ("WQ", vm((d.D, 3 * d.D), BF16)),
        ("WP", vm((d.D, d.D), BF16)),
        ("WF", vm((d.NJ, d.D, BLK), BF16)),
        ("WO", vm((d.NJ, BLK, d.D), BF16)),
        ("ACC", vm((d.NCH, 2, 8) + P8, BF16)),
        ("R0", vm((d.NS, 2, 4) + P8, BF16)),
        ("R1", vm((d.NS, 4) + P8, BF16)),
        ("R2", vm((d.NS, 2) + P8, BF16)),
        ("R3", vm((d.NS, 1) + P8, BF16)),
        ("R4", vm((d.NS, d.PR, LANES), BF16)),
        ("RX", vm((max(n_x, 1), d.NS, d.PR, LANES), BF16)),
        ("QKV", vm((d.M, 3 * d.D), BF16)),
        ("T", vm((d.M, d.D), BF16)),
        ("COT", vm((d.M, d.D), BF16)),
        ("N1", vm((d.M, d.D), BF16)),
        ("ATT", vm((d.M, d.D), BF16)),
        ("N2", vm((d.M, d.D), BF16)),
        ("N2T", vm((d.D, d.M), BF16)),
        ("HRES", vm((d.M, d.D), F32)),
        ("OUTACC", vm((d.M, d.D), F32)),
        ("DN2", vm((d.M, d.D), F32)),
        ("ACTT", vm((BLK, d.M), BF16)),
        ("DPRE", vm((d.M, BLK), BF16)),
        ("VA", vm((1, d.NV), F32)),
        ("VB", vm((1, d.NV), F32)),
        ("VX", vm((1, d.NV), F32)),
        ("VG", vm((2, 1, d.NV), F32)),
        ("VR", vm((d.nb + 1, 1, d.NV), F32)),
        ("LS", sem((4 + d.NJ,))),
        ("GS", sem((3, d.NQP + 1 + d.NJ))),
        ("GR", sem((3, d.NQP + 1 + d.NJ))),
        ("SS", sem((len(d.lag), d.NS))),
        ("SR", sem((len(d.lag), d.NS))),
        ("OS", sem((d.NS,))),
        ("CR", pltpu.SemaphoreType.REGULAR((4,))),
        ("VS", sem((d.nb + 2,))),
        ("VQ", sem((d.nb + 2,))),
    ]
    return [n for n, _ in items], [s for _, s in items]


def nt(a, b):
    return lax.dot_general(a, b, (((1,), (1,)), ((), ())), preferred_element_type=F32)


def nn(a, b):
    return jnp.dot(a, b, preferred_element_type=F32)


def tn(a, b):
    return lax.dot_general(a, b, (((0,), (0,)), ((), ())), preferred_element_type=F32)


def norm_rows(v):
    c = v - jnp.mean(v, axis=-1, keepdims=True)
    r = lax.rsqrt(jnp.mean(c * c, axis=-1, keepdims=True) + EPS)
    return c * r, r


def mult(x, m):
    return x if isinstance(x, int) else pl.multiple_of(x, m)


def guarded(cond, fn):
    if isinstance(cond, bool):
        if cond:
            fn()
    else:
        pl.when(cond)(fn)


def both(a, b):
    if isinstance(a, bool):
        return b if a else False
    if isinstance(b, bool):
        return a if b else False
    return jnp.logical_and(a, b)


def block_kernel(d, names, tok, cot, wq, wp, wf, wo, vec, out_o, dx_o, gr_o, vo_o, *scratch):
    k = types.SimpleNamespace(**dict(zip(names, scratch)))
    rep, s = lax.axis_index("rep"), lax.axis_index("shard")
    bit = [lax.rem(lax.div(rep, 1 << i), 2) for i in range(d.nb)]

    def rep_peer(i):
        return {"rep": rep + (1 - 2 * bit[i]) * (1 << i), "shard": s}

    x_peer = {"rep": rep, "shard": 1 - s}
    b0, b1, b2, b3 = bit[:4]
    o = 1 - s

    barrier = pltpu.get_barrier_semaphore()
    peers = [x_peer] + [rep_peer(i) for i in range(d.nb)]
    for peer in peers:
        pl.semaphore_signal(barrier, inc=1, device_id=peer, device_id_type=MESH)
    pl.semaphore_wait(barrier, len(peers))

    def remote(src, dst, ss, rs, peer):
        return pltpu.make_async_remote_copy(
            src_ref=src, dst_ref=dst, send_sem=ss, recv_sem=rs, device_id=peer, device_id_type=MESH
        )

    g = b0 * 2 + b1
    QR, OR = d.DH // 4, LANES // 4
    NQP, NG = d.NQP, d.NQP + 1 + d.NJ
    vcopy = remote(vec, k.VX, k.VS.at[d.nb + 1], k.VQ.at[d.nb + 1], x_peer)
    vcopy.start()
    tcopy = pltpu.make_async_copy(tok, k.T, k.LS.at[0])
    tcopy.start()

    def gather_copies(hop, p):
        if isinstance(p, int) and p <= NQP:
            ref, src = (k.WQ, wq) if p < NQP else (k.WP, wp)
            cols = pl.ds(p * d.QW, d.QW) if p < NQP else pl.ds(0, d.D)
            if hop == 0:
                return [(src.at[pl.ds(g * QR, QR), cols], ref.at[pl.ds(s * d.DH + g * QR, QR), cols])]
            if hop == 1:
                at = ref.at[pl.ds(o * d.DH + g * QR, QR), cols]
            else:
                at = ref.at[pl.ds(o * d.DH + b0 * 2 * QR, 2 * QR), cols]
            return [(at, at)]
        j = p - NQP - 1
        if hop == 0:
            pairs = []
            for strip in range(2):
                col = mult(strip * d.FH + j * LANES, LANES)
                pairs.append((
                    wf.at[pl.ds(g * QR, QR), pl.ds(col, LANES)],
                    k.WF.at[j, pl.ds(s * d.DH + g * QR, QR), pl.ds(strip * LANES, LANES)],
                ))
            pairs.append((
                wo.at[pl.ds(mult(j * LANES + g * OR, OR), OR), :],
                k.WO.at[j, pl.ds(s * LANES + g * OR, OR), :],
            ))
            return pairs
        if hop == 1:
            fa = k.WF.at[j, pl.ds(o * d.DH + g * QR, QR), :]
            oa = k.WO.at[j, pl.ds(o * LANES + g * OR, OR), :]
        else:
            fa = k.WF.at[j, pl.ds(o * d.DH + b0 * 2 * QR, 2 * QR), :]
            oa = k.WO.at[j, pl.ds(o * LANES + b0 * 2 * OR, 2 * OR), :]
        return [(fa, fa), (oa, oa)]

    hop_peer = [x_peer, rep_peer(1), rep_peer(0)]

    def g_start(hop, p):
        for a, b in gather_copies(hop, p):
            remote(a, b, k.GS.at[hop, p], k.GR.at[hop, p], hop_peer[hop]).start()

    def g_wait(hop, p):
        if isinstance(p, int) and p <= NQP:
            (a, b), = gather_copies(hop, p)
            remote(a, b, k.GS.at[hop, p], k.GR.at[hop, p], hop_peer[hop]).wait()
        else:
            rows = k.WF.at[0, pl.ds(0, d.D // 4 * (2 if hop == 2 else 1)), :]
            pltpu.make_async_copy(rows, rows, k.GS.at[hop, p]).wait()
            pltpu.make_async_copy(rows, rows, k.GR.at[hop, p]).wait()

    own_q = pltpu.make_async_copy(wq, k.WQ.at[pl.ds(s * d.DH, d.DH), :], k.LS.at[1])
    own_q.start()
    for p in range(NQP + 1):
        g_start(0, p)

    def start_blocks(j, _):
        g_start(0, j + NQP + 1)
        return 0

    lax.fori_loop(0, d.NJ, start_blocks, 0)
    own_p = pltpu.make_async_copy(wp, k.WP.at[pl.ds(s * d.DH, d.DH), :], k.LS.at[2])
    own_p.start()
    ccopy = pltpu.make_async_copy(cot, k.COT, k.LS.at[3])
    ccopy.start()

    def start_own(j, _):
        for strip in range(2):
            pltpu.make_async_copy(
                wf.at[:, pl.ds(mult(strip * d.FH + j * LANES, LANES), LANES)],
                k.WF.at[j, pl.ds(s * d.DH, d.DH), pl.ds(strip * LANES, LANES)],
                k.LS.at[4 + j],
            ).start()
        pltpu.make_async_copy(
            wo.at[pl.ds(mult(j * LANES, LANES), LANES), :],
            k.WO.at[j, pl.ds(s * LANES, LANES), :],
            k.LS.at[4 + j],
        ).start()
        return 0

    lax.fori_loop(0, d.NJ, start_own, 0)

    def wait_own(j):
        pltpu.make_async_copy(k.WF.at[0], k.WF.at[0], k.LS.at[4 + j]).wait()

    vcopy.wait()
    own, oth = vec[...], k.VX[...]
    first = s == 0
    k.VA[...] = jnp.where(first, own, oth)
    k.VB[...] = jnp.where(first, oth, own)

    def full(name):
        at, n = d.off[name]
        return jnp.concatenate([k.VA[:, at:at + n], k.VB[:, at:at + n]], axis=1)

    def put_vec(name, value):
        at, n = d.off[name]
        k.VG[0, :, at:at + n] = value[:, :n]
        k.VG[1, :, at:at + n] = value[:, n:]

    tcopy.wait()
    LR = 64

    def norm1(i, _):
        rows = pl.ds(pl.multiple_of(i * LR, LR), LR)
        xhat, _r = norm_rows(k.T[rows, :].astype(F32))
        k.N1[rows, :] = (xhat * full("ln1g") + full("ln1b")).astype(BF16)
        return 0

    lax.fori_loop(0, d.M // LR, norm1, 0)
    own_q.wait()
    for p in range(NQP + 2):
        for hop in range(2, -1, -1):
            if 0 <= p - hop < NQP:
                g_wait(hop, p - hop)
                if hop < 2:
                    g_start(hop + 1, p - hop)

    bq = k.VA[:, d.off["qvb"][0]:d.off["qvb"][0] + d.D]
    bv = k.VB[:, d.off["qvb"][0]:d.off["qvb"][0] + d.D]
    RB = 256

    def qkv_rows(i, _):
        rows = pl.ds(pl.multiple_of(i * RB, RB), RB)
        x = k.N1[rows, :]
        for part in range(3):
            y = nn(x, k.WQ[:, part * d.D:(part + 1) * d.D])
            if part == 0:
                y = (y + bq).astype(BF16) * jnp.asarray(HEAD_DIM ** -0.5, BF16)
            elif part == 1:
                y = y.astype(BF16)
            else:
                y = (y + bv).astype(BF16)
            k.QKV[rows, part * d.D:(part + 1) * d.D] = y
        return 0

    lax.fori_loop(0, d.M // RB, qkv_rows, 0)

    lane = lax.broadcasted_iota(jnp.int32, (1, LANES), 1)
    head_mask = [lane < HEAD_DIM, lane >= HEAD_DIM]
    zero = jnp.zeros((), BF16)
    QB = 256
    NQB = SEQ_LEN // QB
    tri = lax.broadcasted_iota(jnp.int32, (QB, QB), 1) <= lax.broadcasted_iota(jnp.int32, (QB, QB), 0)
    tri_t = lax.broadcasted_iota(jnp.int32, (QB, QB), 0) <= lax.broadcasted_iota(jnp.int32, (QB, QB), 1)

    def unit_refs(seq, hp):
        rows = pl.ds(pl.multiple_of(seq * SEQ_LEN, SEQ_LEN), SEQ_LEN)
        cols = [pl.ds(pl.multiple_of(part * d.D + hp * LANES, LANES), LANES) for part in range(3)]
        return rows, cols

    g_wait(0, NQP)
    g_start(1, NQP)
    g_wait(1, NQP)
    g_start(2, NQP)
    g_wait(2, NQP)

    def attend_loop(u, _):
        attend_body(u)
        return 0

    def g_block_tick(p):
        for hop in range(2, -1, -1):
            q = p - hop

            def do(hop=hop, q=q):
                g_wait(hop, q)
                if hop < 2:
                    g_start(hop + 1, q)

            guarded(jnp.logical_and(q > NQP, q < NG), do)

    def attend_body(u):
        seq, hp = lax.div(u, d.NH2), lax.rem(u, d.NH2)
        rows, cols = unit_refs(seq, hp)
        q2, k2, v2 = (k.QKV[rows, c] for c in cols)
        for i in range(NQB):
            klen = (i + 1) * QB
            total = None
            for mask in head_mask:
                qm = jnp.where(mask, q2[i * QB:klen], zero)
                vm = jnp.where(mask, v2[:klen], zero)
                sc = nt(qm, k2[:klen])
                diag = jnp.where(tri, sc[:, klen - QB:], NEG)
                sc = diag if i == 0 else jnp.concatenate([sc[:, :klen - QB], diag], axis=1)
                top = jnp.max(sc, axis=1, keepdims=True)
                e = jnp.exp(sc - top)
                den = jnp.sum(e, axis=1, keepdims=True)
                part = nn(e.astype(BF16), vm) * (1.0 / den)
                total = part if total is None else total + part
            out_rows = pl.ds(pl.multiple_of(seq * SEQ_LEN + i * QB, QB), QB)
            k.ATT[out_rows, pl.ds(pl.multiple_of(hp * LANES, LANES), LANES)] = total.astype(BF16)
        g_block_tick(u + NQP + 1)

    lax.fori_loop(0, d.NSEQ * d.NH2, attend_loop, 0)
    own_p.wait()

    HB = 128

    def hres_rows(i, _):
        rows = pl.ds(pl.multiple_of(i * HB, HB), HB)
        h = k.T[rows, :].astype(F32) + nn(k.ATT[rows, :], k.WP[...]) + full("projb")
        k.HRES[rows, :] = h
        k.OUTACC[rows, :] = h + full("outb")
        xhat, _r = norm_rows(h)
        n2 = (xhat * full("ln2g") + full("ln2b")).astype(BF16)
        k.N2[rows, :] = n2
        k.N2T[:, rows] = n2.T
        k.DN2[rows, :] = jnp.zeros((HB, d.D), F32)
        return 0

    lax.fori_loop(0, d.M // HB, hres_rows, 0)
    ccopy.wait()

    def cot_sum(i, total):
        rows = pl.ds(pl.multiple_of(i * LR, LR), LR)
        return total + jnp.sum(k.COT[rows, :].astype(F32), axis=0, keepdims=True)

    put_vec("outb", lax.fori_loop(0, d.M // LR, cot_sum, jnp.zeros((1, d.D), F32)))

    lo4, lo2 = 4 * b0, 4 * b0 + 2 * b1
    lo1 = lo2 + b2
    n_x = d.nb - 4
    last = len(d.lag)

    def stage(i, c):
        slot = lax.rem(c, d.NS)
        sems = (k.SS.at[i, slot], k.SR.at[i, slot])
        A = k.ACC
        if i == 0:
            return A.at[c, :, pl.ds(4 - lo4, 4)], k.R0.at[slot], sems, rep_peer(0), (A.at[c, :, pl.ds(lo4, 4)], k.R0.at[slot])
        if i == 1:
            return A.at[c, o, pl.ds(lo4, 4)], k.R1.at[slot], sems, x_peer, (A.at[c, s, pl.ds(lo4, 4)], k.R1.at[slot])
        if i == 2:
            return (A.at[c, s, pl.ds(lo4 + 2 - 2 * b1, 2)], k.R2.at[slot], sems, rep_peer(1),
                    (A.at[c, s, pl.ds(lo2, 2)], k.R2.at[slot]))
        if i == 3:
            return (A.at[c, s, pl.ds(lo2 + 1 - b2, 1)], k.R3.at[slot], sems, rep_peer(2),
                    (A.at[c, s, pl.ds(lo1, 1)], k.R3.at[slot]))
        if i == 4:
            return A.at[c, s, lo1, 1 - b3], k.R4.at[slot], sems, rep_peer(3), (A.at[c, s, lo1, b3], k.R4.at[slot])
        if i < 5 + n_x:
            dst = k.RX.at[i - 5, slot]
            return A.at[c, s, lo1, b3], dst, sems, rep_peer(i - 1), (A.at[c, s, lo1, b3], dst)
        at = [A.at[c, s, lo1, b3], A.at[c, s, pl.ds(lo1, 1)], A.at[c, s, pl.ds(lo2, 2)], A.at[c, s, pl.ds(lo4, 4)]][i - 5 - n_x]
        return at, at, sems, rep_peer(3 - (i - 5 - n_x)), None

    def chunk_of(v):
        w = v - d.V0
        if isinstance(v, int):
            if v < d.V0:
                return v, 0 <= v
            grp, r = divmod(w, d.GV)
            return d.V0 + 3 * grp + r - d.GU, v < d.NVS and r >= d.GU
        late = v >= d.V0
        w = jnp.maximum(w, 0)
        grp, r = lax.div(w, d.GV), lax.rem(w, d.GV)
        c = jnp.where(late, d.V0 + 3 * grp + r - d.GU, v)
        ok = jnp.logical_and(v >= 0, jnp.logical_and(v < d.NVS, jnp.logical_or(v < d.V0, r >= d.GU)))
        return c, ok

    def out_copy(c):
        return pltpu.make_async_copy(k.ACC.at[c, s], gr_o.at[c], k.OS.at[lax.rem(c, d.NS)])

    def begin(i, c):
        if i == last:
            out_copy(c).start()
            return
        src, dst, (ss, rs), peer, _ = stage(i, c)
        if i >= d.first_ag:
            pl.semaphore_wait(k.CR.at[i - d.first_ag], 1)
        remote(src, dst, ss, rs, peer).start()

    def finish(i, c):
        if i == last:
            out_copy(c).wait()
            return
        src, dst, (ss, rs), peer, add = stage(i, c)
        remote(src, dst, ss, rs, peer).wait()
        if add is not None:
            add[0][...] = add[0][...] + add[1][...]
        if i in credit_of:
            pl.semaphore_signal(k.CR.at[credit_of[i]], inc=1, device_id=peer, device_id_type=MESH)

    credit_of = {4: 0, 3: 1, 2: 2, 0: 3}

    def tick(t):
        for i in range(last, -1, -1):
            c, ok = chunk_of(t - d.E[i])
            guarded(ok, functools.partial(finish, i, c))
        for i in range(last, -1, -1):
            c, ok = chunk_of(t - d.B[i])
            guarded(ok, functools.partial(begin, i, c))

    def put_cols(c, sh, value):
        value = value.astype(BF16)
        for p in range(8):
            for z in range(2):
                k.ACC[c, sh, p, z, :, :] = value[p * d.PR:(p + 1) * d.PR, z * LANES:(z + 1) * LANES]

    def put_out(c, n, value):
        value = value.astype(BF16)
        per = d.D // LANES // 2
        for sh in range(2):
            for p in range(8):
                for h in range(BLK // LANES):
                    t = n * (BLK // LANES) + h
                    k.ACC[c, sh, p, t // per, pl.ds((t % per) * d.PO, d.PO), :] = value[
                        sh * LANES + p * d.PO:sh * LANES + (p + 1) * d.PO, h * LANES:(h + 1) * LANES
                    ]

    f_at = d.off["fcb"][0]
    C1, C3 = GELU_C, GELU_C * 0.044715
    S1, S3 = 2.0 * GELU_C, 2.0 * GELU_C * 0.134145

    def mlp(j, _):
        wait_own(j)
        fcb = jnp.concatenate(
            [v[:, pl.ds(pl.multiple_of(f_at + j * LANES, LANES), LANES)] for v in (k.VA, k.VB)], axis=1
        )

        def rows_step(i, total):
            rows = pl.ds(pl.multiple_of(i * RB, RB), RB)
            wfj, woj = k.WF[j], k.WO[j]
            c = k.COT[rows, :]
            pre = nn(k.N2[rows, :], wfj) + fcb
            d_act = nt(c, woj)
            sq = pre * pre
            h = 0.5 + 0.5 * jnp.tanh(pre * (C1 + C3 * sq))
            a = pre * h
            slope = h + a * (1.0 - h) * (S1 + S3 * sq)
            d_pre = d_act * slope
            ab, db = a.astype(BF16), d_pre.astype(BF16)
            k.ACTT[:, rows] = ab.T
            k.DPRE[rows, :] = db
            k.OUTACC[rows, :] += nn(ab, woj)
            k.DN2[rows, :] += nt(db, wfj)
            return total + jnp.sum(d_pre, axis=0, keepdims=True)

        total = lax.fori_loop(0, d.M // RB, rows_step, jnp.zeros((1, BLK), F32))
        at = pl.ds(pl.multiple_of(f_at + j * LANES, LANES), LANES)
        k.VG[0, :, at] = total[:, :LANES]
        k.VG[1, :, at] = total[:, LANES:]
        for n in range(d.NP):
            put_out(2 * j, n, nn(k.ACTT[...], k.COT[:, n * BLK:(n + 1) * BLK]))
        tick(2 * j)
        for sh in range(2):
            put_cols(2 * j + 1, sh, nn(k.N2T[sh * d.DH:(sh + 1) * d.DH, :], k.DPRE[...]))
        tick(2 * j + 1)
        return 0

    g_wait(1, NG - 1)
    g_start(2, NG - 1)
    g_wait(2, NG - 2)
    g_wait(2, NG - 1)
    lax.fori_loop(0, d.NJ, mlp, 0)

    g2 = full("ln2g")

    def norm2_back(i, sums):
        rows = pl.ds(pl.multiple_of(i * LR, LR), LR)
        k.N1[rows, :] = k.OUTACC[rows, :].astype(BF16)
        xhat, r = norm_rows(k.HRES[rows, :])
        dn = k.DN2[rows, :]
        gg = dn * g2
        dh = k.COT[rows, :].astype(F32) + r * (
            gg - jnp.mean(gg, axis=-1, keepdims=True) - xhat * jnp.mean(gg * xhat, axis=-1, keepdims=True)
        )
        k.DN2[rows, :] = dh
        k.N2[rows, :] = dh.astype(BF16)
        add = lambda v: jnp.sum(v, axis=0, keepdims=True)
        return sums[0] + add(dn * xhat), sums[1] + add(dn), sums[2] + add(dh)

    zrow = jnp.zeros((1, d.D), F32)
    sums = lax.fori_loop(0, d.M // LR, norm2_back, (zrow, zrow, zrow))
    put_vec("ln2g", sums[0])
    put_vec("ln2b", sums[1])
    put_vec("projb", sums[2])
    bcopy = pltpu.make_async_copy(k.N1, out_o, k.LS.at[0])
    bcopy.start()

    def transpose_att(i, _):
        rows = pl.ds(pl.multiple_of(i * HB, HB), HB)
        k.N2T[:, rows] = k.ATT[rows, :].T
        return 0

    lax.fori_loop(0, d.M // HB, transpose_att, 0)

    def proj_cols(n, _):
        c = 2 * d.NJ + n
        cols = pl.ds(pl.multiple_of(n * BLK, BLK), BLK)
        for sh in range(2):
            put_cols(c, sh, nn(k.N2T[sh * d.DH:(sh + 1) * d.DH, :], k.N2[:, cols]))
        tick(c)
        return 0

    lax.fori_loop(0, d.NP, proj_cols, 0)
    bcopy.wait()

    def att_rows(i, _):
        rows = pl.ds(pl.multiple_of(i * RB, RB), RB)
        k.N1[rows, :] = nt(k.N2[rows, :], k.WP[...]).astype(BF16)
        return 0

    lax.fori_loop(0, d.M // RB, att_rows, 0)

    g1, be1 = full("ln1g"), full("ln1b")

    def transpose_n1(i, _):
        rows = pl.ds(pl.multiple_of(i * HB, HB), HB)
        xhat, _r = norm_rows(k.T[rows, :].astype(F32))
        k.N2T[:, rows] = (xhat * g1 + be1).astype(BF16).T
        return 0

    lax.fori_loop(0, d.M // HB, transpose_n1, 0)

    def attend_back(seq, hp):
        rows, cols = unit_refs(seq, hp)
        q2, k2, v2 = (k.QKV[rows, c] for c in cols)
        do2 = k.N1[rows, pl.ds(pl.multiple_of(hp * LANES, LANES), LANES)]
        dq = [None] * NQB
        dk = [None] * NQB
        dv = [None] * NQB

        def acc(lst, n, value):
            lst[n] = value if lst[n] is None else lst[n] + value

        for mask in head_mask:
            km = jnp.where(mask, k2, zero)
            for i in range(NQB):
                klen = (i + 1) * QB
                qm = jnp.where(mask, q2[i * QB:klen], zero)
                dom = jnp.where(mask, do2[i * QB:klen], zero)
                sc = nt(k2[:klen], qm)
                diag = jnp.where(tri_t, sc[klen - QB:], NEG)
                sc = diag if i == 0 else jnp.concatenate([sc[:klen - QB], diag], axis=0)
                top = jnp.max(sc, axis=0, keepdims=True)
                e = jnp.exp(sc - top)
                pr = e * (1.0 / jnp.sum(e, axis=0, keepdims=True))
                dp = nt(v2[:klen], dom)
                delta = jnp.sum(pr * dp, axis=0, keepdims=True)
                ds = (pr * (dp - delta)).astype(BF16)
                dvi = nn(pr.astype(BF16), dom)
                dki = nn(ds, qm)
                for n in range(i + 1):
                    acc(dv, n, dvi[n * QB:(n + 1) * QB])
                    acc(dk, n, dki[n * QB:(n + 1) * QB])
                acc(dq, i, tn(ds, km[:klen]))
        sq = sv = None
        for n in range(NQB):
            r = pl.ds(pl.multiple_of(seq * SEQ_LEN + n * QB, QB), QB)
            dqn = dq[n] * (HEAD_DIM ** -0.5)
            k.QKV[r, cols[0]] = dqn.astype(BF16)
            k.QKV[r, cols[1]] = dk[n].astype(BF16)
            k.QKV[r, cols[2]] = dv[n].astype(BF16)
            a, b = jnp.sum(dqn, axis=0, keepdims=True), jnp.sum(dv[n], axis=0, keepdims=True)
            sq, sv = (a, b) if sq is None else (sq + a, sv + b)
        at = pl.ds(pl.multiple_of(d.off["qvb"][0] + hp * LANES, LANES), LANES)
        for half, value in ((0, sq), (1, sv)):
            k.VG[half, :, at] = k.VG[half, :, at] + value

    for half in range(2):
        at, n = d.off["qvb"]
        k.VG[half, :, at:at + n] = jnp.zeros((1, n), F32)

    def zero_dn1(i, _):
        rows = pl.ds(pl.multiple_of(i * LR, LR), LR)
        k.OUTACC[rows, :] = jnp.zeros((LR, d.D), F32)
        return 0

    lax.fori_loop(0, d.M // LR, zero_dn1, 0)

    def group(grp, _):
        v0 = d.V0 + grp * d.GV

        def unit(u, _):
            attend_back(lax.div(u, 2), 2 * grp + lax.rem(u, 2))
            tick(v0 + u)
            return 0

        lax.fori_loop(0, d.GU, unit, 0)

        def part_step(part, _):
            c = d.V0 + 3 * grp + part
            cols = pl.ds(pl.multiple_of(part * d.D + grp * BLK, BLK), BLK)
            for sh in range(2):
                put_cols(c, sh, nn(k.N2T[sh * d.DH:(sh + 1) * d.DH, :], k.QKV[:, cols]))

            def rows_step(i, _):
                rows = pl.ds(pl.multiple_of(i * RB, RB), RB)
                k.OUTACC[rows, :] += nt(k.QKV[rows, cols], k.WQ[:, cols])
                return 0

            lax.fori_loop(0, d.M // RB, rows_step, 0)
            tick(v0 + d.GU + part)
            return 0

        lax.fori_loop(0, 3, part_step, 0)
        return 0

    lax.fori_loop(0, d.NP, group, 0)

    def norm1_back(i, sums):
        rows = pl.ds(pl.multiple_of(i * LR, LR), LR)
        xhat, r = norm_rows(k.T[rows, :].astype(F32))
        dn = k.OUTACC[rows, :]
        gg = dn * g1
        dx = k.DN2[rows, :] + r * (
            gg - jnp.mean(gg, axis=-1, keepdims=True) - xhat * jnp.mean(gg * xhat, axis=-1, keepdims=True)
        )
        k.COT[rows, :] = dx.astype(BF16)
        add = lambda v: jnp.sum(v, axis=0, keepdims=True)
        return sums[0] + add(dn * xhat), sums[1] + add(dn)

    sums = lax.fori_loop(0, d.M // LR, norm1_back, (zrow, zrow))
    put_vec("ln1g", sums[0])
    put_vec("ln1b", sums[1])
    xcopy = pltpu.make_async_copy(k.COT, dx_o, k.LS.at[0])
    xcopy.start()

    def vec_copy(i):
        src = k.VG.at[o] if i == 0 else k.VG.at[s]
        peer = x_peer if i == 0 else rep_peer(i - 1)
        return remote(src, k.VR.at[i], k.VS.at[i], k.VQ.at[i], peer)

    end = d.NVS + d.E[-1]
    n_v = d.nb + 1
    vec_copy(0).start()
    step = 0
    for t in range(d.NVS, end):
        tick(t)
        if step < n_v and (t - d.NVS) % 2 == 1:
            vec_copy(step).wait()
            k.VG[s] = k.VG[s] + k.VR[step]
            step += 1
            if step < n_v:
                vec_copy(step).start()
    assert step == n_v
    vo_o[...] = k.VG[s]
    xcopy.wait()


def per_device(d, tok, g1, be1, wq, qvb, wp, pb, g2, be2, wf, fb, wo, ob, cot):
    names, scratch = scratch_of(d)
    vec = jnp.concatenate([v.astype(F32) for v in (g1, be1, qvb, pb, g2, be2, ob, fb)]).reshape(1, d.NV)
    hbm = pl.BlockSpec(memory_space=pl.ANY)
    vmem = pl.BlockSpec(memory_space=pltpu.VMEM)
    out, dx, gr, vo = pl.pallas_call(
        functools.partial(block_kernel, d, names),
        out_shape=(
            jax.ShapeDtypeStruct((d.M, d.D), BF16),
            jax.ShapeDtypeStruct((d.M, d.D), BF16),
            jax.ShapeDtypeStruct((d.NCH, 8, 2, d.PR, LANES), BF16),
            jax.ShapeDtypeStruct((1, d.NV), F32),
        ),
        in_specs=[hbm] * 6 + [vmem],
        out_specs=(hbm, hbm, hbm, vmem),
        scratch_shapes=scratch,
        compiler_params=pltpu.CompilerParams(
            collective_id=0, has_side_effects=True, vmem_limit_bytes=67_043_328
        ),
        name="block",
    )(tok, cot, wq, wp, wf, wo, vec)
    vo = vo.reshape(d.NV)
    v = {n: vo[at:at + size] for n, (at, size) in d.off.items()}
    NJ, NP, PR, PO = d.NJ, d.NP, d.PR, d.PO
    mlp = gr[:2 * NJ].reshape(NJ, 2, 8, 2, PR, LANES)
    g_out = mlp[:, 0].reshape(NJ, 8, 2, PR // PO, PO, LANES).transpose(0, 1, 4, 2, 3, 5).reshape(d.FH, d.D)
    g_fc = mlp[:, 1].transpose(1, 3, 2, 0, 4).reshape(d.DH, d.FF)
    g_p = gr[2 * NJ:d.V0].transpose(1, 3, 0, 2, 4).reshape(d.DH, d.D)
    g_q = gr[d.V0:].reshape(NP, 3, 8, 2, PR, LANES).transpose(2, 4, 1, 0, 3, 5).reshape(d.DH, 3 * d.D)
    return (
        out, dx, v["ln1g"], v["ln1b"], g_q.astype(F32), v["qvb"], g_p.astype(F32), v["projb"],
        v["ln2g"], v["ln2b"], g_fc.astype(F32), v["fcb"], g_out.astype(F32), v["outb"],
    )


def solution(mesh):
    def whole(tok, *rest):
        d = dims_of(mesh, tok.shape[0] // (mesh.shape["rep"] * mesh.shape["shard"]), tok.shape[1], rest[9].shape[0])
        both_axes, one, two = P(("rep", "shard"), None), P("shard"), P("shard", None)
        in_specs = (both_axes, one, one, two, one, two, one, one, one, two, one, two, one, both_axes)
        out_specs = (both_axes, both_axes, one, one, two, one, two, one, one, one, two, one, two, one)
        return jax.shard_map(
            functools.partial(per_device, d), mesh=mesh, in_specs=in_specs, out_specs=out_specs, check_vma=False
        )(tok, *rest)

    return whole
```

```python
import functools
import types

import jax
import jax.numpy as jnp
from jax import lax
from jax.experimental import pallas as pl
from jax.experimental.pallas import tpu as pltpu
from jax.sharding import PartitionSpec as P

HEAD_DIM = 64
SEQ_LEN = 512
EPS = 1e-05
GELU_C = 0.7978845608028654
F32, BF16 = jnp.float32, jnp.bfloat16
MESH = pl.DeviceIdType.MESH
LANES = 128
BLK = 256
NEG = -1e30
VECS = ("ln1g", "ln1b", "qvb", "projb", "ln2g", "ln2b", "outb", "fcb")


def dims_of(mesh, rows, width, ff):
    d = types.SimpleNamespace()
    d.R, d.S = mesh.shape["rep"], mesh.shape["shard"]
    d.nb = d.R.bit_length() - 1
    assert d.S == 2 and d.R == 1 << d.nb and d.nb >= 4
    d.M, d.D, d.FF = rows, width, ff
    d.DH, d.FH = width // 2, ff // 2
    d.NJ = ff // BLK
    d.NP = width // BLK
    d.NH2 = width // LANES
    d.NSEQ = rows // SEQ_LEN
    d.NCH = 2 * d.NJ + 4 * d.NP
    d.PR = d.DH // 8
    d.PO = LANES // 8
    half = {"qvb": width, "fcb": ff // 2}
    d.off, at = {}, 0
    for name in VECS:
        d.off[name] = (at, half.get(name, width // 2))
        at += d.off[name][1]
    d.NV = at
    d.lag = [2, 3, 3, 2, 2] + [2] * (d.nb - 4) + [2, 2, 3, 2]
    d.NS = 2 * max(d.lag)
    d.first_ag = d.nb + 1
    d.B, d.E, at = [], [], 0
    for i, lag in enumerate(d.lag + [2]):
        at += i == d.first_ag
        d.B.append(at)
        at += lag
        d.E.append(at)
    d.V0 = 2 * d.NJ + d.NP
    d.GU = 2 * d.NSEQ
    d.GV = d.GU + 3
    d.NVS = d.V0 + d.NP * d.GV
    d.NQP = 6
    d.QW = 3 * width // d.NQP
    return d


def scratch_of(d):
    vm, sem = pltpu.VMEM, pltpu.SemaphoreType.DMA
    P8 = (2, d.PR, LANES)
    n_x = d.nb - 4
    items = [
        ("WQ", vm((d.D, 3 * d.D), BF16)),
        ("WP", vm((d.D, d.D), BF16)),
        ("WF", vm((d.NJ, d.D, BLK), BF16)),
        ("WO", vm((d.NJ, BLK, d.D), BF16)),
        ("ACC", vm((d.NCH, 2, 8) + P8, BF16)),
        ("R0", vm((d.NS, 2, 4) + P8, BF16)),
        ("R1", vm((d.NS, 4) + P8, BF16)),
        ("R2", vm((d.NS, 2) + P8, BF16)),
        ("R3", vm((d.NS, 1) + P8, BF16)),
        ("R4", vm((d.NS, d.PR, LANES), BF16)),
        ("RX", vm((max(n_x, 1), d.NS, d.PR, LANES), BF16)),
        ("QKV", vm((d.M, 3 * d.D), BF16)),
        ("T", vm((d.M, d.D), BF16)),
        ("COT", vm((d.M, d.D), BF16)),
        ("N1", vm((d.M, d.D), BF16)),
        ("ATT", vm((d.M, d.D), BF16)),
        ("N2", vm((d.M, d.D), BF16)),
        ("N2T", vm((d.D, d.M), BF16)),
        ("HRES", vm((d.M, d.D), F32)),
        ("OUTACC", vm((d.M, d.D), F32)),
        ("DN2", vm((d.M, d.D), F32)),
        ("ACTT", vm((BLK, d.M), BF16)),
        ("DPRE", vm((d.M, BLK), BF16)),
        ("VA", vm((1, d.NV), F32)),
        ("VB", vm((1, d.NV), F32)),
        ("VX", vm((1, d.NV), F32)),
        ("VG", vm((2, 1, d.NV), F32)),
        ("VR", vm((d.nb + 1, 1, d.NV), F32)),
        ("LS", sem((4 + d.NJ,))),
        ("GS", sem((3, d.NQP + 1 + d.NJ))),
        ("GR", sem((3, d.NQP + 1 + d.NJ))),
        ("SS", sem((len(d.lag), d.NS))),
        ("SR", sem((len(d.lag), d.NS))),
        ("OS", sem((d.NS,))),
        ("CR", pltpu.SemaphoreType.REGULAR((4,))),
        ("VS", sem((d.nb + 2,))),
        ("VQ", sem((d.nb + 2,))),
    ]
    return [n for n, _ in items], [s for _, s in items]


def nt(a, b):
    return lax.dot_general(a, b, (((1,), (1,)), ((), ())), preferred_element_type=F32)


def nn(a, b):
    return jnp.dot(a, b, preferred_element_type=F32)


def tn(a, b):
    return lax.dot_general(a, b, (((0,), (0,)), ((), ())), preferred_element_type=F32)


def norm_rows(v):
    c = v - jnp.mean(v, axis=-1, keepdims=True)
    r = lax.rsqrt(jnp.mean(c * c, axis=-1, keepdims=True) + EPS)
    return c * r, r


def mult(x, m):
    return x if isinstance(x, int) else pl.multiple_of(x, m)


def guarded(cond, fn):
    if isinstance(cond, bool):
        if cond:
            fn()
    else:
        pl.when(cond)(fn)


def both(a, b):
    if isinstance(a, bool):
        return b if a else False
    if isinstance(b, bool):
        return a if b else False
    return jnp.logical_and(a, b)


def block_kernel(d, names, tok, cot, wq, wp, wf, wo, vec, out_o, dx_o, gr_o, vo_o, *scratch):
    k = types.SimpleNamespace(**dict(zip(names, scratch)))
    rep, s = lax.axis_index("rep"), lax.axis_index("shard")
    bit = [lax.rem(lax.div(rep, 1 << i), 2) for i in range(d.nb)]

    def rep_peer(i):
        return {"rep": rep + (1 - 2 * bit[i]) * (1 << i), "shard": s}

    x_peer = {"rep": rep, "shard": 1 - s}
    b0, b1, b2, b3 = bit[:4]
    o = 1 - s

    barrier = pltpu.get_barrier_semaphore()
    peers = [x_peer] + [rep_peer(i) for i in range(d.nb)]
    for peer in peers:
        pl.semaphore_signal(barrier, inc=1, device_id=peer, device_id_type=MESH)
    pl.semaphore_wait(barrier, len(peers))

    def remote(src, dst, ss, rs, peer):
        return pltpu.make_async_remote_copy(
            src_ref=src, dst_ref=dst, send_sem=ss, recv_sem=rs, device_id=peer, device_id_type=MESH
        )

    g = b0 * 2 + b1
    QR, OR = d.DH // 4, LANES // 4
    NQP, NG = d.NQP, d.NQP + 1 + d.NJ
    vcopy = remote(vec, k.VX, k.VS.at[d.nb + 1], k.VQ.at[d.nb + 1], x_peer)
    vcopy.start()
    tcopy = pltpu.make_async_copy(tok, k.T, k.LS.at[0])
    tcopy.start()

    def gather_copies(hop, p):
        if isinstance(p, int) and p <= NQP:
            ref, src = (k.WQ, wq) if p < NQP else (k.WP, wp)
            cols = pl.ds(p * d.QW, d.QW) if p < NQP else pl.ds(0, d.D)
            if hop == 0:
                return [(src.at[pl.ds(g * QR, QR), cols], ref.at[pl.ds(s * d.DH + g * QR, QR), cols])]
            if hop == 1:
                at = ref.at[pl.ds(o * d.DH + g * QR, QR), cols]
            else:
                at = ref.at[pl.ds(o * d.DH + b0 * 2 * QR, 2 * QR), cols]
            return [(at, at)]
        j = p - NQP - 1
        if hop == 0:
            pairs = []
            for strip in range(2):
                col = mult(strip * d.FH + j * LANES, LANES)
                pairs.append((
                    wf.at[pl.ds(g * QR, QR), pl.ds(col, LANES)],
                    k.WF.at[j, pl.ds(s * d.DH + g * QR, QR), pl.ds(strip * LANES, LANES)],
                ))
            pairs.append((
                wo.at[pl.ds(mult(j * LANES + g * OR, OR), OR), :],
                k.WO.at[j, pl.ds(s * LANES + g * OR, OR), :],
            ))
            return pairs
        if hop == 1:
            fa = k.WF.at[j, pl.ds(o * d.DH + g * QR, QR), :]
            oa = k.WO.at[j, pl.ds(o * LANES + g * OR, OR), :]
        else:
            fa = k.WF.at[j, pl.ds(o * d.DH + b0 * 2 * QR, 2 * QR), :]
            oa = k.WO.at[j, pl.ds(o * LANES + b0 * 2 * OR, 2 * OR), :]
        return [(fa, fa), (oa, oa)]

    hop_peer = [x_peer, rep_peer(1), rep_peer(0)]

    def g_start(hop, p):
        for a, b in gather_copies(hop, p):
            remote(a, b, k.GS.at[hop, p], k.GR.at[hop, p], hop_peer[hop]).start()

    def g_wait(hop, p):
        if isinstance(p, int) and p <= NQP:
            (a, b), = gather_copies(hop, p)
            remote(a, b, k.GS.at[hop, p], k.GR.at[hop, p], hop_peer[hop]).wait()
        else:
            rows = k.WF.at[0, pl.ds(0, d.D // 4 * (2 if hop == 2 else 1)), :]
            pltpu.make_async_copy(rows, rows, k.GS.at[hop, p]).wait()
            pltpu.make_async_copy(rows, rows, k.GR.at[hop, p]).wait()

    G_LAG = (0, 2, 3)

    def g_tick(t):
        for hop in range(2, -1, -1):
            q = t - G_LAG[hop]

            def do(hop=hop, q=q):
                g_wait(hop, q + NQP + 1)
                if hop < 2:
                    g_start(hop + 1, q + NQP + 1)

            guarded(both(q >= 0, q < d.NJ), do)

    own_q = pltpu.make_async_copy(wq, k.WQ.at[pl.ds(s * d.DH, d.DH), :], k.LS.at[1])
    own_q.start()
    for p in range(NQP + 1):
        g_start(0, p)

    def start_blocks(j, _):
        g_start(0, j + NQP + 1)
        return 0

    lax.fori_loop(0, d.NJ, start_blocks, 0)
    own_p = pltpu.make_async_copy(wp, k.WP.at[pl.ds(s * d.DH, d.DH), :], k.LS.at[2])
    own_p.start()
    ccopy = pltpu.make_async_copy(cot, k.COT, k.LS.at[3])
    ccopy.start()

    def start_own(j, _):
        for strip in range(2):
            pltpu.make_async_copy(
                wf.at[:, pl.ds(mult(strip * d.FH + j * LANES, LANES), LANES)],
                k.WF.at[j, pl.ds(s * d.DH, d.DH), pl.ds(strip * LANES, LANES)],
                k.LS.at[4 + j],
            ).start()
        pltpu.make_async_copy(
            wo.at[pl.ds(mult(j * LANES, LANES), LANES), :],
            k.WO.at[j, pl.ds(s * LANES, LANES), :],
            k.LS.at[4 + j],
        ).start()
        return 0

    lax.fori_loop(0, d.NJ, start_own, 0)

    def wait_own(j):
        pltpu.make_async_copy(k.WF.at[0], k.WF.at[0], k.LS.at[4 + j]).wait()

    vcopy.wait()
    own, oth = vec[...], k.VX[...]
    first = s == 0
    k.VA[...] = jnp.where(first, own, oth)
    k.VB[...] = jnp.where(first, oth, own)

    def full(name):
        at, n = d.off[name]
        return jnp.concatenate([k.VA[:, at:at + n], k.VB[:, at:at + n]], axis=1)

    def put_vec(name, value):
        at, n = d.off[name]
        k.VG[0, :, at:at + n] = value[:, :n]
        k.VG[1, :, at:at + n] = value[:, n:]

    tcopy.wait()
    LR = 64

    def norm1(i, _):
        rows = pl.ds(pl.multiple_of(i * LR, LR), LR)
        xhat, _r = norm_rows(k.T[rows, :].astype(F32))
        k.N1[rows, :] = (xhat * full("ln1g") + full("ln1b")).astype(BF16)
        return 0

    lax.fori_loop(0, d.M // LR, norm1, 0)
    own_q.wait()
    for p in range(NQP + 2):
        for hop in range(2, -1, -1):
            if 0 <= p - hop < NQP:
                g_wait(hop, p - hop)
                if hop < 2:
                    g_start(hop + 1, p - hop)

    bq = k.VA[:, d.off["qvb"][0]:d.off["qvb"][0] + d.D]
    bv = k.VB[:, d.off["qvb"][0]:d.off["qvb"][0] + d.D]
    RB = 256

    def qkv_rows(i, _):
        rows = pl.ds(pl.multiple_of(i * RB, RB), RB)
        x = k.N1[rows, :]
        for part in range(3):
            y = nn(x, k.WQ[:, part * d.D:(part + 1) * d.D])
            if part == 0:
                y = (y + bq).astype(BF16) * jnp.asarray(HEAD_DIM ** -0.5, BF16)
            elif part == 1:
                y = y.astype(BF16)
            else:
                y = (y + bv).astype(BF16)
            k.QKV[rows, part * d.D:(part + 1) * d.D] = y
        return 0

    g_wait(0, NQP)
    g_start(1, NQP)
    lax.fori_loop(0, d.M // RB, qkv_rows, 0)
    g_wait(1, NQP)
    g_start(2, NQP)

    lane = lax.broadcasted_iota(jnp.int32, (1, LANES), 1)
    head_mask = [lane < HEAD_DIM, lane >= HEAD_DIM]
    zero = jnp.zeros((), BF16)
    QB = 256
    NQB = SEQ_LEN // QB
    tri = lax.broadcasted_iota(jnp.int32, (QB, QB), 1) <= lax.broadcasted_iota(jnp.int32, (QB, QB), 0)
    tri_t = lax.broadcasted_iota(jnp.int32, (QB, QB), 0) <= lax.broadcasted_iota(jnp.int32, (QB, QB), 1)

    def unit_refs(seq, hp):
        rows = pl.ds(pl.multiple_of(seq * SEQ_LEN, SEQ_LEN), SEQ_LEN)
        cols = [pl.ds(pl.multiple_of(part * d.D + hp * LANES, LANES), LANES) for part in range(3)]
        return rows, cols

    def attend_loop(u, _):
        attend_body(u)

        def do():
            g_tick(lax.div(u, 2))

        pl.when(lax.rem(u, 2) == 1)(do)
        return 0

    def attend_body(u):
        seq, hp = lax.div(u, d.NH2), lax.rem(u, d.NH2)
        rows, cols = unit_refs(seq, hp)
        q2, k2, v2 = (k.QKV[rows, c] for c in cols)
        for i in range(NQB):
            klen = (i + 1) * QB
            total = None
            for mask in head_mask:
                qm = jnp.where(mask, q2[i * QB:klen], zero)
                vm = jnp.where(mask, v2[:klen], zero)
                sc = nt(qm, k2[:klen])
                diag = jnp.where(tri, sc[:, klen - QB:], NEG)
                sc = diag if i == 0 else jnp.concatenate([sc[:, :klen - QB], diag], axis=1)
                top = jnp.max(sc, axis=1, keepdims=True)
                e = jnp.exp(sc - top)
                den = jnp.sum(e, axis=1, keepdims=True)
                part = nn(e.astype(BF16), vm) * (1.0 / den)
                total = part if total is None else total + part
            out_rows = pl.ds(pl.multiple_of(seq * SEQ_LEN + i * QB, QB), QB)
            k.ATT[out_rows, pl.ds(pl.multiple_of(hp * LANES, LANES), LANES)] = total.astype(BF16)

    lax.fori_loop(0, d.NSEQ * d.NH2, attend_loop, 0)
    own_p.wait()
    g_wait(2, NQP)

    HB = 128

    def hres_rows(i, _):
        rows = pl.ds(pl.multiple_of(i * HB, HB), HB)
        h = k.T[rows, :].astype(F32) + nn(k.ATT[rows, :], k.WP[...]) + full("projb")
        k.HRES[rows, :] = h
        k.OUTACC[rows, :] = h + full("outb")
        xhat, _r = norm_rows(h)
        n2 = (xhat * full("ln2g") + full("ln2b")).astype(BF16)
        k.N2[rows, :] = n2
        k.N2T[:, rows] = n2.T
        k.DN2[rows, :] = jnp.zeros((HB, d.D), F32)
        pl.when(lax.rem(i, 4) == 3)(lambda: g_tick(n_att + lax.div(i, 4)))
        return 0

    n_att = d.NSEQ * d.NH2 // 2
    lax.fori_loop(0, d.M // HB, hres_rows, 0)
    ccopy.wait()

    def cot_sum(i, total):
        rows = pl.ds(pl.multiple_of(i * LR, LR), LR)
        return total + jnp.sum(k.COT[rows, :].astype(F32), axis=0, keepdims=True)

    put_vec("outb", lax.fori_loop(0, d.M // LR, cot_sum, jnp.zeros((1, d.D), F32)))

    lo4, lo2 = 4 * b0, 4 * b0 + 2 * b1
    lo1 = lo2 + b2
    n_x = d.nb - 4
    last = len(d.lag)

    def stage(i, c):
        slot = lax.rem(c, d.NS)
        sems = (k.SS.at[i, slot], k.SR.at[i, slot])
        A = k.ACC
        if i == 0:
            return A.at[c, :, pl.ds(4 - lo4, 4)], k.R0.at[slot], sems, rep_peer(0), (A.at[c, :, pl.ds(lo4, 4)], k.R0.at[slot])
        if i == 1:
            return A.at[c, o, pl.ds(lo4, 4)], k.R1.at[slot], sems, x_peer, (A.at[c, s, pl.ds(lo4, 4)], k.R1.at[slot])
        if i == 2:
            return (A.at[c, s, pl.ds(lo4 + 2 - 2 * b1, 2)], k.R2.at[slot], sems, rep_peer(1),
                    (A.at[c, s, pl.ds(lo2, 2)], k.R2.at[slot]))
        if i == 3:
            return (A.at[c, s, pl.ds(lo2 + 1 - b2, 1)], k.R3.at[slot], sems, rep_peer(2),
                    (A.at[c, s, pl.ds(lo1, 1)], k.R3.at[slot]))
        if i == 4:
            return A.at[c, s, lo1, 1 - b3], k.R4.at[slot], sems, rep_peer(3), (A.at[c, s, lo1, b3], k.R4.at[slot])
        if i < 5 + n_x:
            dst = k.RX.at[i - 5, slot]
            return A.at[c, s, lo1, b3], dst, sems, rep_peer(i - 1), (A.at[c, s, lo1, b3], dst)
        at = [A.at[c, s, lo1, b3], A.at[c, s, pl.ds(lo1, 1)], A.at[c, s, pl.ds(lo2, 2)], A.at[c, s, pl.ds(lo4, 4)]][i - 5 - n_x]
        return at, at, sems, rep_peer(3 - (i - 5 - n_x)), None

    def chunk_of(v):
        w = v - d.V0
        if isinstance(v, int):
            if v < d.V0:
                return v, 0 <= v
            grp, r = divmod(w, d.GV)
            return d.V0 + 3 * grp + r - d.GU, v < d.NVS and r >= d.GU
        late = v >= d.V0
        w = jnp.maximum(w, 0)
        grp, r = lax.div(w, d.GV), lax.rem(w, d.GV)
        c = jnp.where(late, d.V0 + 3 * grp + r - d.GU, v)
        ok = jnp.logical_and(v >= 0, jnp.logical_and(v < d.NVS, jnp.logical_or(v < d.V0, r >= d.GU)))
        return c, ok

    def out_copy(c):
        return pltpu.make_async_copy(k.ACC.at[c, s], gr_o.at[c], k.OS.at[lax.rem(c, d.NS)])

    def begin(i, c):
        if i == last:
            out_copy(c).start()
            return
        src, dst, (ss, rs), peer, _ = stage(i, c)
        if i >= d.first_ag:
            pl.semaphore_wait(k.CR.at[i - d.first_ag], 1)
        remote(src, dst, ss, rs, peer).start()

    def finish(i, c):
        if i == last:
            out_copy(c).wait()
            return
        src, dst, (ss, rs), peer, add = stage(i, c)
        remote(src, dst, ss, rs, peer).wait()
        if add is not None:
            add[0][...] = add[0][...] + add[1][...]
        if i in credit_of:
            pl.semaphore_signal(k.CR.at[credit_of[i]], inc=1, device_id=peer, device_id_type=MESH)

    credit_of = {4: 0, 3: 1, 2: 2, 0: 3}

    def tick(t):
        for i in range(last, -1, -1):
            c, ok = chunk_of(t - d.E[i])
            guarded(ok, functools.partial(finish, i, c))
        for i in range(last, -1, -1):
            c, ok = chunk_of(t - d.B[i])
            guarded(ok, functools.partial(begin, i, c))

    def put_cols(c, sh, value):
        value = value.astype(BF16)
        for p in range(8):
            for z in range(2):
                k.ACC[c, sh, p, z, :, :] = value[p * d.PR:(p + 1) * d.PR, z * LANES:(z + 1) * LANES]

    def put_out(c, n, value):
        value = value.astype(BF16)
        per = d.D // LANES // 2
        for sh in range(2):
            for p in range(8):
                for h in range(BLK // LANES):
                    t = n * (BLK // LANES) + h
                    k.ACC[c, sh, p, t // per, pl.ds((t % per) * d.PO, d.PO), :] = value[
                        sh * LANES + p * d.PO:sh * LANES + (p + 1) * d.PO, h * LANES:(h + 1) * LANES
                    ]

    f_at = d.off["fcb"][0]
    C1, C3 = GELU_C, GELU_C * 0.044715
    S1, S3 = 2.0 * GELU_C, 2.0 * GELU_C * 0.134145

    g_done = n_att + d.M // HB // 4
    assert g_done >= G_LAG[2]

    def mlp(j, _):
        wait_own(j)
        g_tick(j + g_done)
        fcb = jnp.concatenate(
            [v[:, pl.ds(pl.multiple_of(f_at + j * LANES, LANES), LANES)] for v in (k.VA, k.VB)], axis=1
        )

        def rows_step(i, total):
            rows = pl.ds(pl.multiple_of(i * RB, RB), RB)
            wfj, woj = k.WF[j], k.WO[j]
            c = k.COT[rows, :]
            pre = nn(k.N2[rows, :], wfj) + fcb
            d_act = nt(c, woj)
            sq = pre * pre
            h = 0.5 + 0.5 * jnp.tanh(pre * (C1 + C3 * sq))
            a = pre * h
            slope = h + a * (1.0 - h) * (S1 + S3 * sq)
            d_pre = d_act * slope
            ab, db = a.astype(BF16), d_pre.astype(BF16)
            k.ACTT[:, rows] = ab.T
            k.DPRE[rows, :] = db
            k.OUTACC[rows, :] += nn(ab, woj)
            k.DN2[rows, :] += nt(db, wfj)
            return total + jnp.sum(d_pre, axis=0, keepdims=True)

        total = lax.fori_loop(0, d.M // RB, rows_step, jnp.zeros((1, BLK), F32))
        at = pl.ds(pl.multiple_of(f_at + j * LANES, LANES), LANES)
        k.VG[0, :, at] = total[:, :LANES]
        k.VG[1, :, at] = total[:, LANES:]
        for n in range(d.NP):
            put_out(2 * j, n, nn(k.ACTT[...], k.COT[:, n * BLK:(n + 1) * BLK]))
        tick(2 * j)
        for sh in range(2):
            put_cols(2 * j + 1, sh, nn(k.N2T[sh * d.DH:(sh + 1) * d.DH, :], k.DPRE[...]))
        tick(2 * j + 1)
        return 0

    lax.fori_loop(0, d.NJ, mlp, 0)

    g2 = full("ln2g")

    def norm2_back(i, sums):
        rows = pl.ds(pl.multiple_of(i * LR, LR), LR)
        k.N1[rows, :] = k.OUTACC[rows, :].astype(BF16)
        xhat, r = norm_rows(k.HRES[rows, :])
        dn = k.DN2[rows, :]
        gg = dn * g2
        dh = k.COT[rows, :].astype(F32) + r * (
            gg - jnp.mean(gg, axis=-1, keepdims=True) - xhat * jnp.mean(gg * xhat, axis=-1, keepdims=True)
        )
        k.DN2[rows, :] = dh
        k.N2[rows, :] = dh.astype(BF16)
        add = lambda v: jnp.sum(v, axis=0, keepdims=True)
        return sums[0] + add(dn * xhat), sums[1] + add(dn), sums[2] + add(dh)

    zrow = jnp.zeros((1, d.D), F32)
    sums = lax.fori_loop(0, d.M // LR, norm2_back, (zrow, zrow, zrow))
    put_vec("ln2g", sums[0])
    put_vec("ln2b", sums[1])
    put_vec("projb", sums[2])
    bcopy = pltpu.make_async_copy(k.N1, out_o, k.LS.at[0])
    bcopy.start()

    def transpose_att(i, _):
        rows = pl.ds(pl.multiple_of(i * HB, HB), HB)
        k.N2T[:, rows] = k.ATT[rows, :].T
        return 0

    lax.fori_loop(0, d.M // HB, transpose_att, 0)

    def proj_cols(n, _):
        c = 2 * d.NJ + n
        cols = pl.ds(pl.multiple_of(n * BLK, BLK), BLK)
        for sh in range(2):
            put_cols(c, sh, nn(k.N2T[sh * d.DH:(sh + 1) * d.DH, :], k.N2[:, cols]))
        tick(c)
        return 0

    lax.fori_loop(0, d.NP, proj_cols, 0)
    bcopy.wait()

    def att_rows(i, _):
        rows = pl.ds(pl.multiple_of(i * RB, RB), RB)
        k.N1[rows, :] = nt(k.N2[rows, :], k.WP[...]).astype(BF16)
        return 0

    lax.fori_loop(0, d.M // RB, att_rows, 0)

    g1, be1 = full("ln1g"), full("ln1b")

    def transpose_n1(i, _):
        rows = pl.ds(pl.multiple_of(i * HB, HB), HB)
        xhat, _r = norm_rows(k.T[rows, :].astype(F32))
        k.N2T[:, rows] = (xhat * g1 + be1).astype(BF16).T
        return 0

    lax.fori_loop(0, d.M // HB, transpose_n1, 0)

    def attend_back(seq, hp):
        rows, cols = unit_refs(seq, hp)
        q2, k2, v2 = (k.QKV[rows, c] for c in cols)
        do2 = k.N1[rows, pl.ds(pl.multiple_of(hp * LANES, LANES), LANES)]
        dq = [None] * NQB
        dk = [None] * NQB
        dv = [None] * NQB

        def acc(lst, n, value):
            lst[n] = value if lst[n] is None else lst[n] + value

        for mask in head_mask:
            km = jnp.where(mask, k2, zero)
            for i in range(NQB):
                klen = (i + 1) * QB
                qm = jnp.where(mask, q2[i * QB:klen], zero)
                dom = jnp.where(mask, do2[i * QB:klen], zero)
                sc = nt(k2[:klen], qm)
                diag = jnp.where(tri_t, sc[klen - QB:], NEG)
                sc = diag if i == 0 else jnp.concatenate([sc[:klen - QB], diag], axis=0)
                top = jnp.max(sc, axis=0, keepdims=True)
                e = jnp.exp(sc - top)
                pr = e * (1.0 / jnp.sum(e, axis=0, keepdims=True))
                dp = nt(v2[:klen], dom)
                delta = jnp.sum(pr * dp, axis=0, keepdims=True)
                ds = (pr * (dp - delta)).astype(BF16)
                dvi = nn(pr.astype(BF16), dom)
                dki = nn(ds, qm)
                for n in range(i + 1):
                    acc(dv, n, dvi[n * QB:(n + 1) * QB])
                    acc(dk, n, dki[n * QB:(n + 1) * QB])
                acc(dq, i, tn(ds, km[:klen]))
        sq = sv = None
        for n in range(NQB):
            r = pl.ds(pl.multiple_of(seq * SEQ_LEN + n * QB, QB), QB)
            dqn = dq[n] * (HEAD_DIM ** -0.5)
            k.QKV[r, cols[0]] = dqn.astype(BF16)
            k.QKV[r, cols[1]] = dk[n].astype(BF16)
            k.QKV[r, cols[2]] = dv[n].astype(BF16)
            a, b = jnp.sum(dqn, axis=0, keepdims=True), jnp.sum(dv[n], axis=0, keepdims=True)
            sq, sv = (a, b) if sq is None else (sq + a, sv + b)
        at = pl.ds(pl.multiple_of(d.off["qvb"][0] + hp * LANES, LANES), LANES)
        for half, value in ((0, sq), (1, sv)):
            k.VG[half, :, at] = k.VG[half, :, at] + value

    for half in range(2):
        at, n = d.off["qvb"]
        k.VG[half, :, at:at + n] = jnp.zeros((1, n), F32)

    def zero_dn1(i, _):
        rows = pl.ds(pl.multiple_of(i * LR, LR), LR)
        k.OUTACC[rows, :] = jnp.zeros((LR, d.D), F32)
        return 0

    lax.fori_loop(0, d.M // LR, zero_dn1, 0)

    def group(grp, _):
        v0 = d.V0 + grp * d.GV

        def unit(u, _):
            attend_back(lax.div(u, 2), 2 * grp + lax.rem(u, 2))
            tick(v0 + u)
            return 0

        lax.fori_loop(0, d.GU, unit, 0)

        def part_step(part, _):
            c = d.V0 + 3 * grp + part
            cols = pl.ds(pl.multiple_of(part * d.D + grp * BLK, BLK), BLK)
            for sh in range(2):
                put_cols(c, sh, nn(k.N2T[sh * d.DH:(sh + 1) * d.DH, :], k.QKV[:, cols]))

            def rows_step(i, _):
                rows = pl.ds(pl.multiple_of(i * RB, RB), RB)
                k.OUTACC[rows, :] += nt(k.QKV[rows, cols], k.WQ[:, cols])
                return 0

            lax.fori_loop(0, d.M // RB, rows_step, 0)
            tick(v0 + d.GU + part)
            return 0

        lax.fori_loop(0, 3, part_step, 0)
        return 0

    lax.fori_loop(0, d.NP, group, 0)

    def norm1_back(i, sums):
        rows = pl.ds(pl.multiple_of(i * LR, LR), LR)
        xhat, r = norm_rows(k.T[rows, :].astype(F32))
        dn = k.OUTACC[rows, :]
        gg = dn * g1
        dx = k.DN2[rows, :] + r * (
            gg - jnp.mean(gg, axis=-1, keepdims=True) - xhat * jnp.mean(gg * xhat, axis=-1, keepdims=True)
        )
        k.COT[rows, :] = dx.astype(BF16)
        add = lambda v: jnp.sum(v, axis=0, keepdims=True)
        return sums[0] + add(dn * xhat), sums[1] + add(dn)

    sums = lax.fori_loop(0, d.M // LR, norm1_back, (zrow, zrow))
    put_vec("ln1g", sums[0])
    put_vec("ln1b", sums[1])
    xcopy = pltpu.make_async_copy(k.COT, dx_o, k.LS.at[0])
    xcopy.start()

    def vec_copy(i):
        src = k.VG.at[o] if i == 0 else k.VG.at[s]
        peer = x_peer if i == 0 else rep_peer(i - 1)
        return remote(src, k.VR.at[i], k.VS.at[i], k.VQ.at[i], peer)

    end = d.NVS + d.E[-1]
    n_v = d.nb + 1
    vec_copy(0).start()
    step = 0
    for t in range(d.NVS, end):
        tick(t)
        if step < n_v and (t - d.NVS) % 2 == 1:
            vec_copy(step).wait()
            k.VG[s] = k.VG[s] + k.VR[step]
            step += 1
            if step < n_v:
                vec_copy(step).start()
    assert step == n_v
    vo_o[...] = k.VG[s]
    xcopy.wait()


def per_device(d, tok, g1, be1, wq, qvb, wp, pb, g2, be2, wf, fb, wo, ob, cot):
    names, scratch = scratch_of(d)
    vec = sum(
        lax.pad(v.astype(F32), jnp.zeros((), F32), [(at, d.NV - at - n, 0)])
        for v, (at, n) in zip((g1, be1, qvb, pb, g2, be2, ob, fb), d.off.values())
    ).reshape(1, d.NV)
    hbm = pl.BlockSpec(memory_space=pl.ANY)
    vmem = pl.BlockSpec(memory_space=pltpu.VMEM)
    out, dx, gr, vo = pl.pallas_call(
        functools.partial(block_kernel, d, names),
        out_shape=(
            jax.ShapeDtypeStruct((d.M, d.D), BF16),
            jax.ShapeDtypeStruct((d.M, d.D), BF16),
            jax.ShapeDtypeStruct((d.NCH, 8, 2, d.PR, LANES), BF16),
            jax.ShapeDtypeStruct((1, d.NV), F32),
        ),
        in_specs=[hbm] * 6 + [vmem],
        out_specs=(hbm, hbm, hbm, vmem),
        scratch_shapes=scratch,
        compiler_params=pltpu.CompilerParams(
            collective_id=0, has_side_effects=True, vmem_limit_bytes=67_043_328
        ),
        name="block",
    )(tok, cot, wq, wp, wf, wo, vec)
    vecs_out = tuple(jax.ShapeDtypeStruct((n,), F32) for _, n in d.off.values())
    g_q, g_p, g_fc, g_out, *v = pl.pallas_call(
        functools.partial(finish_kernel, d),
        out_shape=tuple(
            jax.ShapeDtypeStruct(shape, F32)
            for shape in ((d.DH, 3 * d.D), (d.DH, d.D), (d.DH, d.FF), (d.FH, d.D))
        ) + vecs_out,
        in_specs=[hbm, vmem],
        out_specs=(hbm,) * 4 + (vmem,) * len(vecs_out),
        scratch_shapes=[
            pltpu.VMEM((d.NCH, 8, 2, d.PR, LANES), BF16),
            pltpu.VMEM((2 * d.NJ + 8 * d.NP, d.DH, LANES), F32),
            pltpu.VMEM((d.NJ, LANES, d.D), F32),
            pltpu.SemaphoreType.DMA((d.NCH,)),
            pltpu.SemaphoreType.DMA((d.NCH,)),
        ],
        compiler_params=pltpu.CompilerParams(vmem_limit_bytes=67_043_328),
        name="finish",
    )(gr, vo)
    v = dict(zip(d.off, v))
    return (
        out, dx, v["ln1g"], v["ln1b"], g_q, v["qvb"], g_p, v["projb"],
        v["ln2g"], v["ln2b"], g_fc, v["fcb"], g_out, v["outb"],
    )


def finish_kernel(d, gr, vo, g_q, g_p, g_fc, g_out, *refs):
    outs, (G, C, O, si, so) = refs[:len(d.off)], refs[len(d.off):]
    for ref, (at, n) in zip(outs, d.off.values()):
        ref[...] = vo[0, at:at + n]

    def load(c, _):
        pltpu.make_async_copy(gr.at[c], G.at[c], si.at[c]).start()
        return 0

    lax.fori_loop(0, d.NCH, load, 0)

    def arrived(c):
        pltpu.make_async_copy(gr.at[c], G.at[c], si.at[c]).wait()

    def cols_of(c, slot):
        arrived(c)
        for z in range(2):
            for p in range(8):
                C[slot + z, p * d.PR:(p + 1) * d.PR, :] = G[c, p, z].astype(F32)

    per = d.D // LANES // 2

    def out_copy(j):
        return pltpu.make_async_copy(O.at[j], g_out.at[pl.ds(mult(j * LANES, LANES), LANES), :], so.at[2 * j])

    def col_copies(dst, slot, cols, sem):
        return [
            pltpu.make_async_copy(C.at[slot + z], dst.at[:, pl.ds(mult(col, LANES), LANES)], sem)
            for z, col in enumerate(cols)
        ]

    def fc_copies(j):
        return col_copies(g_fc, 2 * j, (j * LANES, d.FH + j * LANES), so.at[2 * j + 1])

    def wide_copies(i):
        c, slot = 2 * d.NJ + i, 2 * (d.NJ + i)
        if i < d.NP:
            return col_copies(g_p, slot, (i * BLK, i * BLK + LANES), so.at[c])
        grp, part = divmod(i - d.NP, 3)
        col = part * d.D + grp * BLK
        return col_copies(g_q, slot, (col, col + LANES), so.at[c])

    def mlp(j, _):
        c = 2 * j
        arrived(c)
        for p in range(8):
            for t in range(2 * per):
                O[j, p * d.PO:(p + 1) * d.PO, t * LANES:(t + 1) * LANES] = G[
                    c, p, t // per, (t % per) * d.PO:(t % per + 1) * d.PO, :
                ].astype(F32)
        out_copy(j).start()
        cols_of(c + 1, 2 * j)
        for copy in fc_copies(j):
            copy.start()
        return 0

    lax.fori_loop(0, d.NJ, mlp, 0)
    for i in range(4 * d.NP):
        cols_of(2 * d.NJ + i, 2 * (d.NJ + i))
        for copy in wide_copies(i):
            copy.start()

    def drain(j, _):
        out_copy(j).wait()
        pair = C.at[pl.ds(0, 2)]
        pltpu.make_async_copy(pair, pair, so.at[2 * j + 1]).wait()
        return 0

    lax.fori_loop(0, d.NJ, drain, 0)
    for i in range(4 * d.NP):
        pair = C.at[pl.ds(0, 2)]
        pltpu.make_async_copy(pair, pair, so.at[2 * d.NJ + i]).wait()


def solution(mesh):
    def whole(tok, *rest):
        d = dims_of(mesh, tok.shape[0] // (mesh.shape["rep"] * mesh.shape["shard"]), tok.shape[1], rest[9].shape[0])
        both_axes, one, two = P(("rep", "shard"), None), P("shard"), P("shard", None)
        in_specs = (both_axes, one, one, two, one, two, one, one, one, two, one, two, one, both_axes)
        out_specs = (both_axes, both_axes, one, one, two, one, two, one, one, one, two, one, two, one)
        return jax.shard_map(
            functools.partial(per_device, d), mesh=mesh, in_specs=in_specs, out_specs=out_specs, check_vma=False
        )(tok, *rest)

    return whole
```

```python
import functools
import types

import jax
import jax.numpy as jnp
from jax import lax
from jax.experimental import pallas as pl
from jax.experimental.pallas import tpu as pltpu
from jax.sharding import PartitionSpec as P

HEAD_DIM = 64
SEQ_LEN = 512
EPS = 1e-05
GELU_C = 0.7978845608028654
F32, BF16 = jnp.float32, jnp.bfloat16
MESH = pl.DeviceIdType.MESH
LANES = 128
BLK = 256
NEG = -1e30
VECS = ("ln1g", "ln1b", "qvb", "projb", "ln2g", "ln2b", "outb", "fcb")


def dims_of(mesh, rows, width, ff):
    d = types.SimpleNamespace()
    d.R, d.S = mesh.shape["rep"], mesh.shape["shard"]
    d.nb = d.R.bit_length() - 1
    assert d.S == 2 and d.R == 1 << d.nb and d.nb >= 4
    d.M, d.D, d.FF = rows, width, ff
    d.DH, d.FH = width // 2, ff // 2
    d.NJ = ff // BLK
    d.NP = width // BLK
    d.NH2 = width // LANES
    d.NSEQ = rows // SEQ_LEN
    d.NCH = 2 * d.NJ + 4 * d.NP
    d.PR = d.DH // 8
    d.PO = LANES // 8
    half = {"qvb": width, "fcb": ff // 2}
    d.off, at = {}, 0
    for name in VECS:
        d.off[name] = (at, half.get(name, width // 2))
        at += d.off[name][1]
    d.NV = at
    d.lag = [2, 3, 3, 2, 2] + [2] * (d.nb - 4) + [2, 2, 3, 2]
    d.NS = [2 * lag for lag in d.lag]
    d.NSX = max(d.NS)
    d.first_ag = d.nb + 1
    d.B, d.E, at = [], [], 0
    for i, lag in enumerate(d.lag + [2]):
        at += i == d.first_ag
        d.B.append(at)
        at += lag
        d.E.append(at)
    d.V0 = 2 * d.NJ + d.NP
    d.GU = 2 * d.NSEQ
    d.GV = d.GU + 3
    d.NVS = d.V0 + d.NP * d.GV
    d.NQP = 6
    d.QW = 3 * width // d.NQP
    return d


def scratch_of(d):
    vm, sem = pltpu.VMEM, pltpu.SemaphoreType.DMA
    P8 = (2, d.PR, LANES)
    n_x = d.nb - 4
    items = [
        ("WQ", vm((d.D, 3 * d.D), BF16)),
        ("WP", vm((d.D, d.D), BF16)),
        ("WF", vm((d.NJ, d.D, BLK), BF16)),
        ("WO", vm((d.FF, d.D), BF16)),
        ("ACC", vm((d.NCH, 2, 8) + P8, BF16)),
        ("R0", vm((d.NS[0], 2, 4) + P8, BF16)),
        ("R1", vm((d.NS[1], 4) + P8, BF16)),
        ("R2", vm((d.NS[2], 2) + P8, BF16)),
        ("R3", vm((d.NS[3], 1) + P8, BF16)),
        ("R4", vm((d.NS[4], d.PR, LANES), BF16)),
        ("RX", vm((max(n_x, 1), d.NSX, d.PR, LANES), BF16)),
        ("QKV", vm((d.M, 3 * d.D), BF16)),
        ("T", vm((d.M, d.D), BF16)),
        ("COT", vm((d.M, d.D), BF16)),
        ("N1", vm((d.M, d.D), BF16)),
        ("ATT", vm((d.M, d.D), BF16)),
        ("N2", vm((d.M, d.D), BF16)),
        ("N2T", vm((d.D, d.M), BF16)),
        ("HRES", vm((d.M, d.D), F32)),
        ("OUTACC", vm((d.M, d.D), F32)),
        ("DN2", vm((d.M, d.D), F32)),
        ("ACT", vm((d.M, d.FF), BF16)),
        ("ACTT", vm((BLK, d.M), BF16)),
        ("DPRE", vm((d.M, BLK), BF16)),
        ("VA", vm((1, d.NV), F32)),
        ("VB", vm((1, d.NV), F32)),
        ("VX", vm((1, d.NV), F32)),
        ("VG", vm((2, 1, d.NV), F32)),
        ("VR", vm((d.nb + 1, 1, d.NV), F32)),
        ("LS", sem((4 + d.NJ,))),
        ("GS", sem((3, d.NQP + 1 + d.NJ))),
        ("GR", sem((3, d.NQP + 1 + d.NJ))),
        ("SS", sem((len(d.lag), d.NSX))),
        ("SR", sem((len(d.lag), d.NSX))),
        ("OS", sem((d.NSX,))),
        ("CR", pltpu.SemaphoreType.REGULAR((4,))),
        ("VS", sem((d.nb + 2,))),
        ("VQ", sem((d.nb + 2,))),
    ]
    return [n for n, _ in items], [s for _, s in items]


def nt(a, b):
    return lax.dot_general(a, b, (((1,), (1,)), ((), ())), preferred_element_type=F32)


def nn(a, b):
    return jnp.dot(a, b, preferred_element_type=F32)


def tn(a, b):
    return lax.dot_general(a, b, (((0,), (0,)), ((), ())), preferred_element_type=F32)


def norm_rows(v):
    c = v - jnp.mean(v, axis=-1, keepdims=True)
    r = lax.rsqrt(jnp.mean(c * c, axis=-1, keepdims=True) + EPS)
    return c * r, r


def mult(x, m):
    return x if isinstance(x, int) else pl.multiple_of(x, m)


def guarded(cond, fn):
    if isinstance(cond, bool):
        if cond:
            fn()
    else:
        pl.when(cond)(fn)


def both(a, b):
    if isinstance(a, bool):
        return b if a else False
    if isinstance(b, bool):
        return a if b else False
    return jnp.logical_and(a, b)


def block_kernel(d, names, tok, cot, wq, wp, wf, wo, vec, out_o, dx_o, gr_o, vo_o, *scratch):
    k = types.SimpleNamespace(**dict(zip(names, scratch)))
    rep, s = lax.axis_index("rep"), lax.axis_index("shard")
    bit = [lax.rem(lax.div(rep, 1 << i), 2) for i in range(d.nb)]

    def rep_peer(i):
        return {"rep": rep + (1 - 2 * bit[i]) * (1 << i), "shard": s}

    x_peer = {"rep": rep, "shard": 1 - s}
    b0, b1, b2, b3 = bit[:4]
    o = 1 - s

    barrier = pltpu.get_barrier_semaphore()
    peers = [x_peer] + [rep_peer(i) for i in range(d.nb)]
    for peer in peers:
        pl.semaphore_signal(barrier, inc=1, device_id=peer, device_id_type=MESH)
    pl.semaphore_wait(barrier, len(peers))

    def remote(src, dst, ss, rs, peer):
        return pltpu.make_async_remote_copy(
            src_ref=src, dst_ref=dst, send_sem=ss, recv_sem=rs, device_id=peer, device_id_type=MESH
        )

    g = b0 * 2 + b1
    QR, OR = d.DH // 4, LANES // 4
    NQP, NG = d.NQP, d.NQP + 1 + d.NJ
    vcopy = remote(vec, k.VX, k.VS.at[d.nb + 1], k.VQ.at[d.nb + 1], x_peer)
    vcopy.start()
    tcopy = pltpu.make_async_copy(tok, k.T, k.LS.at[0])
    tcopy.start()

    def gather_copies(hop, p):
        if isinstance(p, int) and p <= NQP:
            ref, src = (k.WQ, wq) if p < NQP else (k.WP, wp)
            cols = pl.ds(p * d.QW, d.QW) if p < NQP else pl.ds(0, d.D)
            if hop == 0:
                return [(src.at[pl.ds(g * QR, QR), cols], ref.at[pl.ds(s * d.DH + g * QR, QR), cols])]
            if hop == 1:
                at = ref.at[pl.ds(o * d.DH + g * QR, QR), cols]
            else:
                at = ref.at[pl.ds(o * d.DH + b0 * 2 * QR, 2 * QR), cols]
            return [(at, at)]
        j = p - NQP - 1
        if hop == 0:
            pairs = []
            for strip in range(2):
                col = mult(strip * d.FH + j * LANES, LANES)
                pairs.append((
                    wf.at[pl.ds(g * QR, QR), pl.ds(col, LANES)],
                    k.WF.at[j, pl.ds(s * d.DH + g * QR, QR), pl.ds(strip * LANES, LANES)],
                ))
            pairs.append((
                wo.at[pl.ds(mult(j * LANES + g * OR, OR), OR), :],
                k.WO.at[pl.ds(j * BLK + s * LANES + g * OR, OR), :],
            ))
            return pairs
        if hop == 1:
            fa = k.WF.at[j, pl.ds(o * d.DH + g * QR, QR), :]
            oa = k.WO.at[pl.ds(j * BLK + o * LANES + g * OR, OR), :]
        else:
            fa = k.WF.at[j, pl.ds(o * d.DH + b0 * 2 * QR, 2 * QR), :]
            oa = k.WO.at[pl.ds(j * BLK + o * LANES + b0 * 2 * OR, 2 * OR), :]
        return [(fa, fa), (oa, oa)]

    hop_peer = [x_peer, rep_peer(1), rep_peer(0)]

    def g_start(hop, p):
        for a, b in gather_copies(hop, p):
            remote(a, b, k.GS.at[hop, p], k.GR.at[hop, p], hop_peer[hop]).start()

    def g_wait(hop, p):
        if isinstance(p, int) and p <= NQP:
            (a, b), = gather_copies(hop, p)
            remote(a, b, k.GS.at[hop, p], k.GR.at[hop, p], hop_peer[hop]).wait()
        else:
            rows = k.WF.at[0, pl.ds(0, d.D // 4 * (2 if hop == 2 else 1)), :]
            pltpu.make_async_copy(rows, rows, k.GS.at[hop, p]).wait()
            pltpu.make_async_copy(rows, rows, k.GR.at[hop, p]).wait()

    G_LAG = (0, 2, 3)

    def g_tick(t):
        for hop in range(2, -1, -1):
            q = t - G_LAG[hop]

            def do(hop=hop, q=q):
                g_wait(hop, q + NQP + 1)
                if hop < 2:
                    g_start(hop + 1, q + NQP + 1)

            guarded(both(q >= 0, q < d.NJ), do)

    own_q = pltpu.make_async_copy(wq, k.WQ.at[pl.ds(s * d.DH, d.DH), :], k.LS.at[1])
    own_q.start()
    for p in range(NQP + 1):
        g_start(0, p)

    def start_blocks(j, _):
        g_start(0, j + NQP + 1)
        return 0

    lax.fori_loop(0, d.NJ, start_blocks, 0)
    own_p = pltpu.make_async_copy(wp, k.WP.at[pl.ds(s * d.DH, d.DH), :], k.LS.at[2])
    own_p.start()
    ccopy = pltpu.make_async_copy(cot, k.COT, k.LS.at[3])
    ccopy.start()

    def start_own(j, _):
        for strip in range(2):
            pltpu.make_async_copy(
                wf.at[:, pl.ds(mult(strip * d.FH + j * LANES, LANES), LANES)],
                k.WF.at[j, pl.ds(s * d.DH, d.DH), pl.ds(strip * LANES, LANES)],
                k.LS.at[4 + j],
            ).start()
        pltpu.make_async_copy(
            wo.at[pl.ds(mult(j * LANES, LANES), LANES), :],
            k.WO.at[pl.ds(j * BLK + s * LANES, LANES), :],
            k.LS.at[4 + j],
        ).start()
        return 0

    lax.fori_loop(0, d.NJ, start_own, 0)

    def wait_own(j):
        pltpu.make_async_copy(k.WF.at[0], k.WF.at[0], k.LS.at[4 + j]).wait()

    vcopy.wait()
    own, oth = vec[...], k.VX[...]
    first = s == 0
    k.VA[...] = jnp.where(first, own, oth)
    k.VB[...] = jnp.where(first, oth, own)

    def full(name):
        at, n = d.off[name]
        return jnp.concatenate([k.VA[:, at:at + n], k.VB[:, at:at + n]], axis=1)

    def put_vec(name, value):
        at, n = d.off[name]
        k.VG[0, :, at:at + n] = value[:, :n]
        k.VG[1, :, at:at + n] = value[:, n:]

    tcopy.wait()
    LR = 64

    def norm1(i, _):
        rows = pl.ds(pl.multiple_of(i * LR, LR), LR)
        xhat, _r = norm_rows(k.T[rows, :].astype(F32))
        k.N1[rows, :] = (xhat * full("ln1g") + full("ln1b")).astype(BF16)
        return 0

    lax.fori_loop(0, d.M // LR, norm1, 0)
    own_q.wait()
    RB = 256
    partial = (k.HRES, k.OUTACC, k.DN2)
    own_cols = pl.ds(pl.multiple_of(s * d.DH, LANES), d.DH)
    oth_cols = pl.ds(pl.multiple_of(o * d.DH, LANES), d.DH)
    own_rows, oth_rows = pl.ds(s * d.DH, d.DH), pl.ds(o * d.DH, d.DH)

    def own_part(part):
        def step(i, _):
            rows = pl.ds(pl.multiple_of(i * RB, RB), RB)
            partial[part][rows, :] = nn(k.N1[rows, own_cols], k.WQ[own_rows, part * d.D:(part + 1) * d.D])
            return 0

        lax.fori_loop(0, d.M // RB, step, 0)

    per_part = NQP // 3

    def oth_piece(p):
        part, col = p // per_part, p % per_part * d.QW
        bias = None
        if part != 1:
            at = d.off["qvb"][0] + col
            bias = (k.VA if part == 0 else k.VB)[:, at:at + d.QW]

        def step(i, _):
            rows = pl.ds(pl.multiple_of(i * RB, RB), RB)
            y = nn(k.N1[rows, oth_cols], k.WQ[oth_rows, p * d.QW:(p + 1) * d.QW]) + partial[part][rows, col:col + d.QW]
            y = (y if bias is None else y + bias).astype(BF16)
            if part == 0:
                y = y * jnp.asarray(HEAD_DIM ** -0.5, BF16)
            k.QKV[rows, p * d.QW:(p + 1) * d.QW] = y
            return 0

        lax.fori_loop(0, d.M // RB, step, 0)

    for p in range(NQP):
        g_wait(0, p)
        g_start(1, p)
        if p % per_part == 0:
            own_part(p // per_part)
    for p in range(NQP):
        g_wait(1, p)
        g_start(2, p)
        if p:
            g_wait(2, p - 1)
            oth_piece(p - 1)
    g_wait(0, NQP)
    g_start(1, NQP)
    g_wait(2, NQP - 1)
    oth_piece(NQP - 1)
    g_wait(1, NQP)
    g_start(2, NQP)

    lane = lax.broadcasted_iota(jnp.int32, (1, LANES), 1)
    head_mask = [lane < HEAD_DIM, lane >= HEAD_DIM]
    zero = jnp.zeros((), BF16)
    QB = 256
    NQB = SEQ_LEN // QB
    tri = lax.broadcasted_iota(jnp.int32, (QB, QB), 1) <= lax.broadcasted_iota(jnp.int32, (QB, QB), 0)
    tri_t = lax.broadcasted_iota(jnp.int32, (QB, QB), 0) <= lax.broadcasted_iota(jnp.int32, (QB, QB), 1)

    def unit_refs(seq, hp):
        rows = pl.ds(pl.multiple_of(seq * SEQ_LEN, SEQ_LEN), SEQ_LEN)
        cols = [pl.ds(pl.multiple_of(part * d.D + hp * LANES, LANES), LANES) for part in range(3)]
        return rows, cols

    def attend_loop(u, _):
        attend_body(2 * u)
        attend_body(2 * u + 1)
        g_tick(u)
        return 0

    def attend_body(u):
        seq, hp = lax.div(u, d.NH2), lax.rem(u, d.NH2)
        rows, cols = unit_refs(seq, hp)
        q2, k2, v2 = (k.QKV[rows, c] for c in cols)
        for i in range(NQB):
            klen = (i + 1) * QB
            total = None
            for mask in head_mask:
                qm = jnp.where(mask, q2[i * QB:klen], zero)
                vm = jnp.where(mask, v2[:klen], zero)
                sc = nt(qm, k2[:klen])
                diag = jnp.where(tri, sc[:, klen - QB:], NEG)
                sc = diag if i == 0 else jnp.concatenate([sc[:, :klen - QB], diag], axis=1)
                top = jnp.max(sc, axis=1, keepdims=True)
                e = jnp.exp(sc - top)
                den = jnp.sum(e, axis=1, keepdims=True)
                part = nn(e.astype(BF16), vm) * (1.0 / den)
                total = part if total is None else total + part
            out_rows = pl.ds(pl.multiple_of(seq * SEQ_LEN + i * QB, QB), QB)
            k.ATT[out_rows, pl.ds(pl.multiple_of(hp * LANES, LANES), LANES)] = total.astype(BF16)

    lax.fori_loop(0, d.NSEQ * d.NH2 // 2, attend_loop, 0)
    own_p.wait()
    g_wait(2, NQP)

    HA = SEQ_LEN

    def hres_rows(i, _):
        rows = pl.ds(pl.multiple_of(i * HA, HA), HA)
        h = k.T[rows, :].astype(F32) + nn(k.ATT[rows, :], k.WP[...]) + full("projb")
        k.HRES[rows, :] = h
        xhat, _r = norm_rows(h)
        n2 = (xhat * full("ln2g") + full("ln2b")).astype(BF16)
        k.N2[rows, :] = n2
        k.N2T[:, rows] = n2.T
        k.DN2[rows, :] = jnp.zeros((HA, d.D), F32)
        g_tick(n_att + i)
        return 0

    n_att = d.NSEQ * d.NH2 // 2
    lax.fori_loop(0, d.M // HA, hres_rows, 0)
    ccopy.wait()

    def cot_sum(i, total):
        rows = pl.ds(pl.multiple_of(i * LR, LR), LR)
        return total + jnp.sum(k.COT[rows, :].astype(F32), axis=0, keepdims=True)

    put_vec("outb", lax.fori_loop(0, d.M // LR, cot_sum, jnp.zeros((1, d.D), F32)))

    lo4, lo2 = 4 * b0, 4 * b0 + 2 * b1
    lo1 = lo2 + b2
    n_x = d.nb - 4
    last = len(d.lag)

    def stage(i, c):
        slot = lax.rem(c, d.NS[i])
        sems = (k.SS.at[i, slot], k.SR.at[i, slot])
        A = k.ACC
        if i == 0:
            return A.at[c, :, pl.ds(4 - lo4, 4)], k.R0.at[slot], sems, rep_peer(0), (A.at[c, :, pl.ds(lo4, 4)], k.R0.at[slot])
        if i == 1:
            return A.at[c, o, pl.ds(lo4, 4)], k.R1.at[slot], sems, x_peer, (A.at[c, s, pl.ds(lo4, 4)], k.R1.at[slot])
        if i == 2:
            return (A.at[c, s, pl.ds(lo4 + 2 - 2 * b1, 2)], k.R2.at[slot], sems, rep_peer(1),
                    (A.at[c, s, pl.ds(lo2, 2)], k.R2.at[slot]))
        if i == 3:
            return (A.at[c, s, pl.ds(lo2 + 1 - b2, 1)], k.R3.at[slot], sems, rep_peer(2),
                    (A.at[c, s, pl.ds(lo1, 1)], k.R3.at[slot]))
        if i == 4:
            return A.at[c, s, lo1, 1 - b3], k.R4.at[slot], sems, rep_peer(3), (A.at[c, s, lo1, b3], k.R4.at[slot])
        if i < 5 + n_x:
            dst = k.RX.at[i - 5, slot]
            return A.at[c, s, lo1, b3], dst, sems, rep_peer(i - 1), (A.at[c, s, lo1, b3], dst)
        at = [A.at[c, s, lo1, b3], A.at[c, s, pl.ds(lo1, 1)], A.at[c, s, pl.ds(lo2, 2)], A.at[c, s, pl.ds(lo4, 4)]][i - 5 - n_x]
        return at, at, sems, rep_peer(3 - (i - 5 - n_x)), None

    def chunk_of(v):
        w = v - d.V0
        if isinstance(v, int):
            if v < d.V0:
                return v, 0 <= v
            grp, r = divmod(w, d.GV)
            return d.V0 + 3 * grp + r - d.GU, v < d.NVS and r >= d.GU
        late = v >= d.V0
        w = jnp.maximum(w, 0)
        grp, r = lax.div(w, d.GV), lax.rem(w, d.GV)
        c = jnp.where(late, d.V0 + 3 * grp + r - d.GU, v)
        ok = jnp.logical_and(v >= 0, jnp.logical_and(v < d.NVS, jnp.logical_or(v < d.V0, r >= d.GU)))
        return c, ok

    def out_copy(c):
        return pltpu.make_async_copy(k.ACC.at[c, s], gr_o.at[c], k.OS.at[lax.rem(c, d.NSX)])

    def begin(i, c):
        if i == last:
            out_copy(c).start()
            return
        src, dst, (ss, rs), peer, _ = stage(i, c)
        if i >= d.first_ag:
            pl.semaphore_wait(k.CR.at[i - d.first_ag], 1)
        remote(src, dst, ss, rs, peer).start()

    def finish(i, c):
        if i == last:
            out_copy(c).wait()
            return
        src, dst, (ss, rs), peer, add = stage(i, c)
        remote(src, dst, ss, rs, peer).wait()
        if add is not None:
            add[0][...] = add[0][...] + add[1][...]
        if i in credit_of:
            pl.semaphore_signal(k.CR.at[credit_of[i]], inc=1, device_id=peer, device_id_type=MESH)

    credit_of = {4: 0, 3: 1, 2: 2, 0: 3}

    def tick(t):
        for i in range(last, -1, -1):
            c, ok = chunk_of(t - d.E[i])
            guarded(ok, functools.partial(finish, i, c))
        for i in range(last, -1, -1):
            c, ok = chunk_of(t - d.B[i])
            guarded(ok, functools.partial(begin, i, c))

    def put_cols(c, sh, value):
        value = value.astype(BF16)
        for p in range(8):
            for z in range(2):
                k.ACC[c, sh, p, z, :, :] = value[p * d.PR:(p + 1) * d.PR, z * LANES:(z + 1) * LANES]

    def put_out(c, n, value):
        value = value.astype(BF16)
        per = d.D // LANES // 2
        for sh in range(2):
            for p in range(8):
                for h in range(BLK // LANES):
                    t = n * (BLK // LANES) + h
                    k.ACC[c, sh, p, t // per, pl.ds((t % per) * d.PO, d.PO), :] = value[
                        sh * LANES + p * d.PO:sh * LANES + (p + 1) * d.PO, h * LANES:(h + 1) * LANES
                    ]

    f_at = d.off["fcb"][0]
    MB = SEQ_LEN
    C1, C3 = GELU_C, GELU_C * 0.044715
    S1, S3 = 2.0 * GELU_C, 2.0 * GELU_C * 0.134145

    g_done = n_att + d.M // HA
    assert g_done >= G_LAG[2]

    def mlp(j, _):
        wait_own(j)
        g_tick(j + g_done)
        fcb = jnp.concatenate(
            [v[:, pl.ds(pl.multiple_of(f_at + j * LANES, LANES), LANES)] for v in (k.VA, k.VB)], axis=1
        )

        def rows_step(i):
            rows = pl.ds(i * MB, MB)
            wfj, woj = k.WF[j], k.WO[pl.ds(pl.multiple_of(j * BLK, BLK), BLK), :]
            c = k.COT[rows, :]
            pre = nn(k.N2[rows, :], wfj) + fcb
            d_act = nt(c, woj)
            sq = pre * pre
            h = 0.5 + 0.5 * jnp.tanh(pre * (C1 + C3 * sq))
            a = pre * h
            slope = h + a * (1.0 - h) * (S1 + S3 * sq)
            d_pre = d_act * slope
            ab, db = a.astype(BF16), d_pre.astype(BF16)
            k.ACTT[:, rows] = ab.T
            k.DPRE[rows, :] = db
            k.ACT[rows, pl.ds(pl.multiple_of(j * BLK, BLK), BLK)] = ab
            k.DN2[rows, :] += nt(db, wfj)
            return jnp.sum(d_pre, axis=0, keepdims=True)

        total = sum(rows_step(i) for i in range(d.M // MB))
        at = pl.ds(pl.multiple_of(f_at + j * LANES, LANES), LANES)
        k.VG[0, :, at] = total[:, :LANES]
        k.VG[1, :, at] = total[:, LANES:]
        for n in range(d.NP):
            put_out(2 * j, n, nn(k.ACTT[...], k.COT[:, n * BLK:(n + 1) * BLK]))
        tick(2 * j)
        for sh in range(2):
            put_cols(2 * j + 1, sh, nn(k.N2T[sh * d.DH:(sh + 1) * d.DH, :], k.DPRE[...]))
        tick(2 * j + 1)
        return 0

    lax.fori_loop(0, d.NJ, mlp, 0)

    g2 = full("ln2g")

    def norm2_back(i, sums):
        rows = pl.ds(pl.multiple_of(i * LR, LR), LR)
        xhat, r = norm_rows(k.HRES[rows, :])
        dn = k.DN2[rows, :]
        gg = dn * g2
        dh = k.COT[rows, :].astype(F32) + r * (
            gg - jnp.mean(gg, axis=-1, keepdims=True) - xhat * jnp.mean(gg * xhat, axis=-1, keepdims=True)
        )
        k.DN2[rows, :] = dh
        k.N2[rows, :] = dh.astype(BF16)
        add = lambda v: jnp.sum(v, axis=0, keepdims=True)
        return sums[0] + add(dn * xhat), sums[1] + add(dn), sums[2] + add(dh)

    zrow = jnp.zeros((1, d.D), F32)
    sums = lax.fori_loop(0, d.M // LR, norm2_back, (zrow, zrow, zrow))
    put_vec("ln2g", sums[0])
    put_vec("ln2b", sums[1])
    put_vec("projb", sums[2])

    def transpose_att(i, _):
        rows = pl.ds(pl.multiple_of(i * HA, HA), HA)
        k.N2T[:, rows] = k.ATT[rows, :].T
        return 0

    lax.fori_loop(0, d.M // HA, transpose_att, 0)

    def proj_cols(n, _):
        c = 2 * d.NJ + n
        cols = pl.ds(pl.multiple_of(n * BLK, BLK), BLK)
        for sh in range(2):
            put_cols(c, sh, nn(k.N2T[sh * d.DH:(sh + 1) * d.DH, :], k.N2[:, cols]))
        tick(c)
        return 0

    lax.fori_loop(0, d.NP, proj_cols, 0)

    def att_rows(i, _):
        rows = pl.ds(pl.multiple_of(i * RB, RB), RB)
        k.N1[rows, :] = nt(k.N2[rows, :], k.WP[...]).astype(BF16)
        return 0

    lax.fori_loop(0, d.M // RB, att_rows, 0)

    g1, be1 = full("ln1g"), full("ln1b")

    def transpose_n1(i, _):
        rows = pl.ds(pl.multiple_of(i * HA, HA), HA)
        xhat, _r = norm_rows(k.T[rows, :].astype(F32))
        k.N2T[:, rows] = (xhat * g1 + be1).astype(BF16).T
        return 0

    lax.fori_loop(0, d.M // HA, transpose_n1, 0)

    def attend_back(seq, hp):
        rows, cols = unit_refs(seq, hp)
        q2, k2, v2 = (k.QKV[rows, c] for c in cols)
        do2 = k.N1[rows, pl.ds(pl.multiple_of(hp * LANES, LANES), LANES)]
        dq = [None] * NQB
        dk = [None] * NQB
        dv = [None] * NQB

        def acc(lst, n, value):
            lst[n] = value if lst[n] is None else lst[n] + value

        for mask in head_mask:
            km = jnp.where(mask, k2, zero)
            for i in range(NQB):
                klen = (i + 1) * QB
                qm = jnp.where(mask, q2[i * QB:klen], zero)
                dom = jnp.where(mask, do2[i * QB:klen], zero)
                sc = nt(k2[:klen], qm)
                diag = jnp.where(tri_t, sc[klen - QB:], NEG)
                sc = diag if i == 0 else jnp.concatenate([sc[:klen - QB], diag], axis=0)
                top = jnp.max(sc, axis=0, keepdims=True)
                e = jnp.exp(sc - top)
                pr = e * (1.0 / jnp.sum(e, axis=0, keepdims=True))
                dp = nt(v2[:klen], dom)
                delta = jnp.sum(pr * dp, axis=0, keepdims=True)
                ds = (pr * (dp - delta)).astype(BF16)
                dvi = nn(pr.astype(BF16), dom)
                dki = nn(ds, qm)
                for n in range(i + 1):
                    acc(dv, n, dvi[n * QB:(n + 1) * QB])
                    acc(dk, n, dki[n * QB:(n + 1) * QB])
                acc(dq, i, tn(ds, km[:klen]))
        sq = sv = None
        for n in range(NQB):
            r = pl.ds(pl.multiple_of(seq * SEQ_LEN + n * QB, QB), QB)
            dqn = dq[n] * (HEAD_DIM ** -0.5)
            k.QKV[r, cols[0]] = dqn.astype(BF16)
            k.QKV[r, cols[1]] = dk[n].astype(BF16)
            k.QKV[r, cols[2]] = dv[n].astype(BF16)
            a, b = jnp.sum(dqn, axis=0, keepdims=True), jnp.sum(dv[n], axis=0, keepdims=True)
            sq, sv = (a, b) if sq is None else (sq + a, sv + b)
        at = pl.ds(pl.multiple_of(d.off["qvb"][0] + hp * LANES, LANES), LANES)
        for half, value in ((0, sq), (1, sv)):
            k.VG[half, :, at] = k.VG[half, :, at] + value

    for half in range(2):
        at, n = d.off["qvb"]
        k.VG[half, :, at:at + n] = jnp.zeros((1, n), F32)

    def group(grp, _):
        v0 = d.V0 + grp * d.GV

        def unit(u, _):
            attend_back(lax.div(u, 2), 2 * grp + lax.rem(u, 2))
            tick(v0 + u)
            return 0

        lax.fori_loop(0, d.GU, unit, 0)

        def part_step(part, _):
            c = d.V0 + 3 * grp + part
            cols = pl.ds(pl.multiple_of(part * d.D + grp * BLK, BLK), BLK)
            for sh in range(2):
                put_cols(c, sh, nn(k.N2T[sh * d.DH:(sh + 1) * d.DH, :], k.QKV[:, cols]))

            tick(v0 + d.GU + part)
            return 0

        lax.fori_loop(0, 3, part_step, 0)
        return 0

    lax.fori_loop(0, d.NP, group, 0)

    HB, TB = 256, 2
    NB = d.M // HB

    def norm1_back(i, sums):
        rows = pl.ds(pl.multiple_of(i * HB, HB), HB)
        dn = nt(k.QKV[rows, :], k.WQ[...])
        xhat, r = norm_rows(k.T[rows, :].astype(F32))
        gg = dn * g1
        dx = k.DN2[rows, :] + r * (
            gg - jnp.mean(gg, axis=-1, keepdims=True) - xhat * jnp.mean(gg * xhat, axis=-1, keepdims=True)
        )
        k.COT[rows, :] = dx.astype(BF16)
        add = lambda v: jnp.sum(v, axis=0, keepdims=True)
        for u in range(TB):
            tick(d.NVS + TB * i + u)
        return sums[0] + add(dn * xhat), sums[1] + add(dn)

    sums = lax.fori_loop(0, NB, norm1_back, (zrow, zrow))
    put_vec("ln1g", sums[0])
    put_vec("ln1b", sums[1])
    xcopy = pltpu.make_async_copy(k.COT, dx_o, k.LS.at[0])
    xcopy.start()

    def vec_copy(i):
        src = k.VG.at[o] if i == 0 else k.VG.at[s]
        peer = x_peer if i == 0 else rep_peer(i - 1)
        return remote(src, k.VR.at[i], k.VS.at[i], k.VQ.at[i], peer)

    n_v = d.nb + 1

    def vec_step(i):
        vec_copy(i).wait()
        k.VG[s] = k.VG[s] + k.VR[i]
        if i + 1 < n_v:
            vec_copy(i + 1).start()

    vec_copy(0).start()
    bout = full("outb")

    def out_step(i, _):
        @pl.when(i < NB)
        def _():
            rows = pl.ds(pl.multiple_of(i * HB, HB), HB)
            y = k.HRES[rows, :] + nn(k.ACT[rows, :], k.WO[...]) + bout
            k.N2[rows, :] = y.astype(BF16)

        for u in range(TB):
            tick(d.NVS + TB * (NB + i) + u)
        for v in range(n_v):
            pl.when(i == v)(functools.partial(vec_step, v))
        return 0

    n_out = max(NB, n_v)
    lax.fori_loop(0, n_out, out_step, 0)
    bcopy = pltpu.make_async_copy(k.N2, out_o, k.LS.at[1])
    bcopy.start()

    def rest(t, _):
        tick(t)
        return 0

    lax.fori_loop(d.NVS + TB * (NB + n_out), d.NVS + d.E[-1], rest, 0)
    vo_o[...] = k.VG[s]
    xcopy.wait()
    bcopy.wait()


def per_device(d, tok, g1, be1, wq, qvb, wp, pb, g2, be2, wf, fb, wo, ob, cot):
    names, scratch = scratch_of(d)
    vec = sum(
        lax.pad(v.astype(F32), jnp.zeros((), F32), [(at, d.NV - at - n, 0)])
        for v, (at, n) in zip((g1, be1, qvb, pb, g2, be2, ob, fb), d.off.values())
    ).reshape(1, d.NV)
    hbm = pl.BlockSpec(memory_space=pl.ANY)
    vmem = pl.BlockSpec(memory_space=pltpu.VMEM)
    out, dx, gr, vo = pl.pallas_call(
        functools.partial(block_kernel, d, names),
        out_shape=(
            jax.ShapeDtypeStruct((d.M, d.D), BF16),
            jax.ShapeDtypeStruct((d.M, d.D), BF16),
            jax.ShapeDtypeStruct((d.NCH, 8, 2, d.PR, LANES), BF16),
            jax.ShapeDtypeStruct((1, d.NV), F32),
        ),
        in_specs=[hbm] * 6 + [vmem],
        out_specs=(hbm, hbm, hbm, vmem),
        scratch_shapes=scratch,
        compiler_params=pltpu.CompilerParams(
            collective_id=0, has_side_effects=True, vmem_limit_bytes=67_043_328
        ),
        name="block",
    )(tok, cot, wq, wp, wf, wo, vec)
    vecs_out = tuple(jax.ShapeDtypeStruct((n,), F32) for _, n in d.off.values())
    g_q, g_p, g_fc, g_out, *v = pl.pallas_call(
        functools.partial(finish_kernel, d),
        out_shape=tuple(
            jax.ShapeDtypeStruct(shape, F32)
            for shape in ((d.DH, 3 * d.D), (d.DH, d.D), (d.DH, d.FF), (d.FH, d.D))
        ) + vecs_out,
        in_specs=[hbm, vmem],
        out_specs=(hbm,) * 4 + (vmem,) * len(vecs_out),
        scratch_shapes=[
            pltpu.VMEM((d.NCH, 8, 2, d.PR, LANES), BF16),
            pltpu.VMEM((2 * d.NJ + 8 * d.NP, d.DH, LANES), F32),
            pltpu.VMEM((d.NJ, LANES, d.D), F32),
            pltpu.SemaphoreType.DMA((d.NCH,)),
            pltpu.SemaphoreType.DMA((d.NCH,)),
        ],
        compiler_params=pltpu.CompilerParams(vmem_limit_bytes=67_043_328),
        name="finish",
    )(gr, vo)
    v = dict(zip(d.off, v))
    return (
        out, dx, v["ln1g"], v["ln1b"], g_q, v["qvb"], g_p, v["projb"],
        v["ln2g"], v["ln2b"], g_fc, v["fcb"], g_out, v["outb"],
    )


def finish_kernel(d, gr, vo, g_q, g_p, g_fc, g_out, *refs):
    outs, (G, C, O, si, so) = refs[:len(d.off)], refs[len(d.off):]
    for ref, (at, n) in zip(outs, d.off.values()):
        ref[...] = vo[0, at:at + n]

    def load(c, _):
        pltpu.make_async_copy(gr.at[c], G.at[c], si.at[c]).start()
        return 0

    lax.fori_loop(0, d.NCH, load, 0)

    def arrived(c):
        pltpu.make_async_copy(gr.at[c], G.at[c], si.at[c]).wait()

    def cols_of(c, slot):
        arrived(c)
        for z in range(2):
            for p in range(8):
                C[slot + z, p * d.PR:(p + 1) * d.PR, :] = G[c, p, z].astype(F32)

    per = d.D // LANES // 2

    def out_copy(j):
        return pltpu.make_async_copy(O.at[j], g_out.at[pl.ds(mult(j * LANES, LANES), LANES), :], so.at[2 * j])

    def col_copies(dst, slot, cols, sem):
        return [
            pltpu.make_async_copy(C.at[slot + z], dst.at[:, pl.ds(mult(col, LANES), LANES)], sem)
            for z, col in enumerate(cols)
        ]

    def fc_copies(j):
        return col_copies(g_fc, 2 * j, (j * LANES, d.FH + j * LANES), so.at[2 * j + 1])

    def wide_copies(i):
        c, slot = 2 * d.NJ + i, 2 * (d.NJ + i)
        if i < d.NP:
            return col_copies(g_p, slot, (i * BLK, i * BLK + LANES), so.at[c])
        grp, part = divmod(i - d.NP, 3)
        col = part * d.D + grp * BLK
        return col_copies(g_q, slot, (col, col + LANES), so.at[c])

    def mlp(j, _):
        c = 2 * j
        arrived(c)
        for p in range(8):
            for t in range(2 * per):
                O[j, p * d.PO:(p + 1) * d.PO, t * LANES:(t + 1) * LANES] = G[
                    c, p, t // per, (t % per) * d.PO:(t % per + 1) * d.PO, :
                ].astype(F32)
        out_copy(j).start()
        cols_of(c + 1, 2 * j)
        for copy in fc_copies(j):
            copy.start()
        return 0

    lax.fori_loop(0, d.NJ, mlp, 0)
    for i in range(4 * d.NP):
        cols_of(2 * d.NJ + i, 2 * (d.NJ + i))
        for copy in wide_copies(i):
            copy.start()

    def drain(j, _):
        out_copy(j).wait()
        pair = C.at[pl.ds(0, 2)]
        pltpu.make_async_copy(pair, pair, so.at[2 * j + 1]).wait()
        return 0

    lax.fori_loop(0, d.NJ, drain, 0)
    for i in range(4 * d.NP):
        pair = C.at[pl.ds(0, 2)]
        pltpu.make_async_copy(pair, pair, so.at[2 * d.NJ + i]).wait()


def solution(mesh):
    def whole(tok, *rest):
        d = dims_of(mesh, tok.shape[0] // (mesh.shape["rep"] * mesh.shape["shard"]), tok.shape[1], rest[9].shape[0])
        both_axes, one, two = P(("rep", "shard"), None), P("shard"), P("shard", None)
        in_specs = (both_axes, one, one, two, one, two, one, one, one, two, one, two, one, both_axes)
        out_specs = (both_axes, both_axes, one, one, two, one, two, one, one, one, two, one, two, one)
        return jax.shard_map(
            functools.partial(per_device, d), mesh=mesh, in_specs=in_specs, out_specs=out_specs, check_vma=False
        )(tok, *rest)

    return whole
```

```python
import functools
import types

import jax
import jax.numpy as jnp
from jax import lax
from jax.experimental import pallas as pl
from jax.experimental.pallas import tpu as pltpu
from jax.sharding import PartitionSpec as P

HEAD_DIM = 64
SEQ_LEN = 512
EPS = 1e-05
GELU_C = 0.7978845608028654
F32, BF16 = jnp.float32, jnp.bfloat16
MESH = pl.DeviceIdType.MESH
LANES = 128
BLK = 256
NEG = -1e30
DRAIN = (0, 0, 2, 1, 1, 1, 1, 1, 1)
VECS = ("ln1g", "ln1b", "qvb", "projb", "ln2g", "ln2b", "outb", "fcb")


def dims_of(mesh, rows, width, ff):
    d = types.SimpleNamespace()
    d.R, d.S = mesh.shape["rep"], mesh.shape["shard"]
    d.nb = d.R.bit_length() - 1
    assert d.S == 2 and d.R == 1 << d.nb and d.nb >= 4
    d.M, d.D, d.FF = rows, width, ff
    d.DH, d.FH = width // 2, ff // 2
    d.NJ = ff // BLK
    d.NP = width // BLK
    d.NH2 = width // LANES
    d.NSEQ = rows // SEQ_LEN
    d.NCH = 2 * d.NJ + 4 * d.NP
    d.PR = d.DH // 8
    d.PO = LANES // 8
    half = {"qvb": width, "fcb": ff // 2}
    d.off, at = {}, 0
    for name in VECS:
        d.off[name] = (at, half.get(name, width // 2))
        at += d.off[name][1]
    d.NV = at
    d.lag = [1, 3, 2, 2] + [1] * (d.nb - 4) + [2, 2, 1]
    d.NS = [2 * lag for lag in d.lag]
    d.NSX = max(d.NS)
    d.first_ag = d.nb
    d.B, d.E, at = [], [], 0
    for i, lag in enumerate(d.lag + [1]):
        at += i == d.first_ag
        d.B.append(at)
        at += lag
        d.E.append(at)
    d.V0 = d.NJ + d.NP
    d.GU = 2 * d.NSEQ
    assert d.GU >= 3
    d.VD = d.V0 + d.NP * d.GU
    d.NVS = d.VD + 3
    d.NQP = 6
    d.QW = 3 * width // d.NQP
    return d


def scratch_of(d):
    vm, sem = pltpu.VMEM, pltpu.SemaphoreType.DMA
    P8 = (2, d.PR, LANES)
    n_x = d.nb - 4
    items = [
        ("WQ", vm((d.D, 3 * d.D), BF16)),
        ("WP", vm((d.D, d.D), BF16)),
        ("WF", vm((d.NJ, d.D, BLK), BF16)),
        ("WO", vm((d.FF, d.D), BF16)),
        ("ACC", vm((d.NCH, 2, 8) + P8, BF16)),
        ("R0", vm((d.NS[0], 2, 2, 4) + P8, BF16)),
        ("R1", vm((d.NS[1], 2, 4) + P8, BF16)),
        ("R2", vm((d.NS[2], 2, 2) + P8, BF16)),
        ("R3", vm((d.NS[3], 3, 2, d.PR, LANES), BF16)),
        ("RX", vm((max(n_x, 1), d.NSX, 2, d.PR, LANES), BF16)),
        ("QKV", vm((d.M, 3 * d.D), BF16)),
        ("T", vm((d.M, d.D), BF16)),
        ("COT", vm((d.M, d.D), BF16)),
        ("N1", vm((d.M, d.D), BF16)),
        ("ATT", vm((d.M, d.D), BF16)),
        ("N2", vm((d.M, d.D), BF16)),
        ("N2T", vm((d.D, d.M), BF16)),
        ("HRES", vm((d.M, d.D), F32)),
        ("DN2", vm((d.M, d.D), F32)),
        ("ACT", vm((d.M, d.FF), BF16)),
        ("ACTT", vm((BLK, d.M), BF16)),
        ("DPRE", vm((d.M, BLK), BF16)),
        ("VA", vm((1, d.NV), F32)),
        ("VB", vm((1, d.NV), F32)),
        ("VX", vm((1, d.NV), F32)),
        ("VG", vm((2, 1, d.NV), F32)),
        ("VR", vm((d.nb + 1, 1, d.NV), F32)),
        ("LS", sem((4 + d.NJ,))),
        ("GS", sem((3, d.NQP + 1 + d.NJ))),
        ("GR", sem((3, d.NQP + 1 + d.NJ))),
        ("SS", sem((len(d.lag), d.NSX, 3))),
        ("SR", sem((len(d.lag), d.NSX, 3))),
        ("OS", sem((d.NSX,))),
        ("CR", pltpu.SemaphoreType.REGULAR((5,))),
        ("VS", sem((d.nb + 2,))),
        ("VQ", sem((d.nb + 2,))),
    ]
    return [n for n, _ in items], [s for _, s in items]


def nt(a, b):
    return lax.dot_general(a, b, (((1,), (1,)), ((), ())), preferred_element_type=F32)


def nn(a, b):
    return jnp.dot(a, b, preferred_element_type=F32)


def tn(a, b):
    return lax.dot_general(a, b, (((0,), (0,)), ((), ())), preferred_element_type=F32)


def norm_rows(v):
    c = v - jnp.mean(v, axis=-1, keepdims=True)
    r = lax.rsqrt(jnp.mean(c * c, axis=-1, keepdims=True) + EPS)
    return c * r, r


def mult(x, m):
    return x if isinstance(x, int) else pl.multiple_of(x, m)


def guarded(cond, fn):
    if isinstance(cond, bool):
        if cond:
            fn()
    else:
        pl.when(cond)(fn)


def both(a, b):
    if isinstance(a, bool):
        return b if a else False
    if isinstance(b, bool):
        return a if b else False
    return jnp.logical_and(a, b)


def block_kernel(d, names, tok, cot, wq, wp, wf, wo, vec, out_o, dx_o, gr_o, vo_o, *scratch):
    k = types.SimpleNamespace(**dict(zip(names, scratch)))
    rep, s = lax.axis_index("rep"), lax.axis_index("shard")
    bit = [lax.rem(lax.div(rep, 1 << i), 2) for i in range(d.nb)]

    def rep_peer(i):
        return {"rep": rep + (1 - 2 * bit[i]) * (1 << i), "shard": s}

    x_peer = {"rep": rep, "shard": 1 - s}
    b0, b1, b2, b3 = bit[:4]
    o = 1 - s

    barrier = pltpu.get_barrier_semaphore()
    peers = [x_peer] + [rep_peer(i) for i in range(d.nb)]
    peers.append({"rep": rep + (1 - 2 * b2) * 4 + (1 - 2 * b3) * 8, "shard": s})
    for peer in peers:
        pl.semaphore_signal(barrier, inc=1, device_id=peer, device_id_type=MESH)
    pl.semaphore_wait(barrier, len(peers))

    def remote(src, dst, ss, rs, peer):
        return pltpu.make_async_remote_copy(
            src_ref=src, dst_ref=dst, send_sem=ss, recv_sem=rs, device_id=peer, device_id_type=MESH
        )

    g = b0 * 2 + b1
    QR, OR = d.DH // 4, LANES // 4
    NQP, NG = d.NQP, d.NQP + 1 + d.NJ
    vcopy = remote(vec, k.VX, k.VS.at[d.nb + 1], k.VQ.at[d.nb + 1], x_peer)
    vcopy.start()
    tcopy = pltpu.make_async_copy(tok, k.T, k.LS.at[0])
    tcopy.start()

    def gather_copies(hop, p):
        if isinstance(p, int) and p <= NQP:
            ref, src = (k.WQ, wq) if p < NQP else (k.WP, wp)
            cols = pl.ds(p * d.QW, d.QW) if p < NQP else pl.ds(0, d.D)
            if hop == 0:
                return [(src.at[pl.ds(g * QR, QR), cols], ref.at[pl.ds(s * d.DH + g * QR, QR), cols])]
            if hop == 1:
                at = ref.at[pl.ds(o * d.DH + g * QR, QR), cols]
            else:
                at = ref.at[pl.ds(o * d.DH + b0 * 2 * QR, 2 * QR), cols]
            return [(at, at)]
        j = p - NQP - 1
        if hop == 0:
            pairs = []
            for strip in range(2):
                col = mult(strip * d.FH + j * LANES, LANES)
                pairs.append((
                    wf.at[pl.ds(g * QR, QR), pl.ds(col, LANES)],
                    k.WF.at[j, pl.ds(s * d.DH + g * QR, QR), pl.ds(strip * LANES, LANES)],
                ))
            pairs.append((
                wo.at[pl.ds(mult(j * LANES + g * OR, OR), OR), :],
                k.WO.at[pl.ds(j * BLK + s * LANES + g * OR, OR), :],
            ))
            return pairs
        if hop == 1:
            fa = k.WF.at[j, pl.ds(o * d.DH + g * QR, QR), :]
            oa = k.WO.at[pl.ds(j * BLK + o * LANES + g * OR, OR), :]
        else:
            fa = k.WF.at[j, pl.ds(o * d.DH + b0 * 2 * QR, 2 * QR), :]
            oa = k.WO.at[pl.ds(j * BLK + o * LANES + b0 * 2 * OR, 2 * OR), :]
        return [(fa, fa), (oa, oa)]

    hop_peer = [x_peer, rep_peer(1), rep_peer(0)]

    def g_start(hop, p):
        for a, b in gather_copies(hop, p):
            remote(a, b, k.GS.at[hop, p], k.GR.at[hop, p], hop_peer[hop]).start()

    def g_wait(hop, p):
        if isinstance(p, int) and p <= NQP:
            (a, b), = gather_copies(hop, p)
            remote(a, b, k.GS.at[hop, p], k.GR.at[hop, p], hop_peer[hop]).wait()
        else:
            rows = k.WF.at[0, pl.ds(0, d.D // 4 * (2 if hop == 2 else 1)), :]
            pltpu.make_async_copy(rows, rows, k.GS.at[hop, p]).wait()
            pltpu.make_async_copy(rows, rows, k.GR.at[hop, p]).wait()

    G_LAG = (0, 2, 3)

    def g_tick(t):
        for hop in range(2, -1, -1):
            q = t - G_LAG[hop]

            def do(hop=hop, q=q):
                g_wait(hop, q + NQP + 1)
                if hop < 2:
                    g_start(hop + 1, q + NQP + 1)

            guarded(both(q >= 0, q < d.NJ), do)

    own_q = pltpu.make_async_copy(wq, k.WQ.at[pl.ds(s * d.DH, d.DH), :], k.LS.at[1])
    own_q.start()
    for p in range(NQP + 1):
        g_start(0, p)
    own_p = pltpu.make_async_copy(wp, k.WP.at[pl.ds(s * d.DH, d.DH), :], k.LS.at[2])
    ccopy = pltpu.make_async_copy(cot, k.COT, k.LS.at[3])

    def start_blocks(j, _):
        g_start(0, j + NQP + 1)
        return 0

    def start_own(j, _):
        for strip in range(2):
            pltpu.make_async_copy(
                wf.at[:, pl.ds(mult(strip * d.FH + j * LANES, LANES), LANES)],
                k.WF.at[j, pl.ds(s * d.DH, d.DH), pl.ds(strip * LANES, LANES)],
                k.LS.at[4 + j],
            ).start()
        pltpu.make_async_copy(
            wo.at[pl.ds(mult(j * LANES, LANES), LANES), :],
            k.WO.at[pl.ds(j * BLK + s * LANES, LANES), :],
            k.LS.at[4 + j],
        ).start()
        return 0

    def wait_own(j):
        pltpu.make_async_copy(k.WF.at[0], k.WF.at[0], k.LS.at[4 + j]).wait()

    vcopy.wait()
    own, oth = vec[...], k.VX[...]
    first = s == 0
    k.VA[...] = jnp.where(first, own, oth)
    k.VB[...] = jnp.where(first, oth, own)

    def full(name):
        at, n = d.off[name]
        return jnp.concatenate([k.VA[:, at:at + n], k.VB[:, at:at + n]], axis=1)

    def put_vec(name, value):
        at, n = d.off[name]
        k.VG[0, :, at:at + n] = value[:, :n]
        k.VG[1, :, at:at + n] = value[:, n:]

    tcopy.wait()
    LR = 64

    def norm1(i, _):
        rows = pl.ds(pl.multiple_of(i * LR, LR), LR)
        xhat, _r = norm_rows(k.T[rows, :].astype(F32))
        k.N1[rows, :] = (xhat * full("ln1g") + full("ln1b")).astype(BF16)
        return 0

    half = d.M // LR // 2
    lax.fori_loop(0, half, norm1, 0)
    g_wait(0, 0)
    g_start(1, 0)
    lax.fori_loop(half, 2 * half, norm1, 0)
    own_q.wait()
    RB = 512
    per_part = NQP // 3

    def qkv_piece(p):
        part, col = p // per_part, p % per_part * d.QW
        bias = None
        if part != 1:
            at = d.off["qvb"][0] + col
            bias = (k.VA if part == 0 else k.VB)[:, at:at + d.QW]

        def step(i, _):
            rows = pl.ds(pl.multiple_of(i * RB, RB), RB)
            y = nn(k.N1[rows, :], k.WQ[:, p * d.QW:(p + 1) * d.QW])
            y = (y if bias is None else y + bias).astype(BF16)
            if part == 0:
                y = y * jnp.asarray(HEAD_DIM ** -0.5, BF16)
            k.QKV[rows, p * d.QW:(p + 1) * d.QW] = y
            return 0

        lax.fori_loop(0, d.M // RB, step, 0)

    own_p.start()
    ccopy.start()
    for p in range(1, NQP):
        g_wait(0, p)
        g_start(1, p)
        if p >= 2:
            g_wait(1, p - 2)
            g_start(2, p - 2)
        if p >= 4:
            g_wait(2, p - 4)
            qkv_piece(p - 4)
        if p == 1:
            lax.fori_loop(0, d.NJ, start_blocks, 0)
        if p == NQP - 1:
            lax.fori_loop(0, d.NJ, start_own, 0)
    g_wait(1, NQP - 2)
    g_start(2, NQP - 2)
    for p in range(NQP - 4, NQP):
        g_wait(2, p)
        qkv_piece(p)
        if p == 2:
            g_wait(1, NQP - 1)
            g_start(2, NQP - 1)
            g_wait(0, NQP)
            g_start(1, NQP)
    g_wait(1, NQP)
    g_start(2, NQP)

    lane = lax.broadcasted_iota(jnp.int32, (1, LANES), 1)
    head_mask = [lane < HEAD_DIM, lane >= HEAD_DIM]
    zero, one = jnp.zeros((), BF16), jnp.ones((), BF16)
    QB = 256
    NQB = SEQ_LEN // QB
    tri = lax.broadcasted_iota(jnp.int32, (QB, QB), 1) <= lax.broadcasted_iota(jnp.int32, (QB, QB), 0)
    tri_t = lax.broadcasted_iota(jnp.int32, (QB, QB), 0) <= lax.broadcasted_iota(jnp.int32, (QB, QB), 1)

    def unit_refs(seq, hp):
        rows = pl.ds(pl.multiple_of(seq * SEQ_LEN, SEQ_LEN), SEQ_LEN)
        cols = [pl.ds(pl.multiple_of(part * d.D + hp * LANES, LANES), LANES) for part in range(3)]
        return rows, cols

    def attend_loop(u, _):
        attend_body(2 * u)
        attend_body(2 * u + 1)
        g_tick(u)
        return 0

    def attend_body(u):
        seq, hp = lax.div(u, d.NH2), lax.rem(u, d.NH2)
        rows, cols = unit_refs(seq, hp)
        q2, k2, v2 = (k.QKV[rows, c] for c in cols)
        for i in range(NQB):
            klen = (i + 1) * QB
            parts = []
            for mask in head_mask:
                qm = jnp.where(mask, q2[i * QB:klen], zero)
                vm = jnp.where(mask, v2[:klen], one)
                sc = nt(qm, k2[:klen])
                diag = jnp.where(tri, sc[:, klen - QB:], NEG)
                sc = diag if i == 0 else jnp.concatenate([sc[:, :klen - QB], diag], axis=1)
                top = jnp.max(sc, axis=1, keepdims=True)
                e = jnp.exp(sc - top)
                parts.append(nn(e.astype(BF16), vm))
            den = jnp.where(head_mask[0], *(pltpu.roll(p, HEAD_DIM, 1) for p in parts))
            total = jnp.where(head_mask[0], *parts) / den
            out_rows = pl.ds(pl.multiple_of(seq * SEQ_LEN + i * QB, QB), QB)
            k.ATT[out_rows, pl.ds(pl.multiple_of(hp * LANES, LANES), LANES)] = total.astype(BF16)

    lax.fori_loop(0, d.NSEQ * d.NH2 // 2, attend_loop, 0)
    own_p.wait()
    g_wait(2, NQP)

    HA = SEQ_LEN

    def hres_rows(i, _):
        rows = pl.ds(pl.multiple_of(i * HA, HA), HA)
        h = k.T[rows, :].astype(F32) + nn(k.ATT[rows, :], k.WP[...]) + full("projb")
        k.HRES[rows, :] = h
        xhat, _r = norm_rows(h)
        n2 = (xhat * full("ln2g") + full("ln2b")).astype(BF16)
        k.N2[rows, :] = n2
        k.N2T[:, rows] = n2.T
        k.DN2[rows, :] = jnp.zeros((HA, d.D), F32)
        g_tick(n_att + i)
        return 0

    n_att = d.NSEQ * d.NH2 // 2
    lax.fori_loop(0, d.M // HA, hres_rows, 0)
    ccopy.wait()

    def cot_sum(i, total):
        rows = pl.ds(pl.multiple_of(i * LR, LR), LR)
        return total + jnp.sum(k.COT[rows, :].astype(F32), axis=0, keepdims=True)

    put_vec("outb", lax.fori_loop(0, d.M // LR, cot_sum, jnp.zeros((1, d.D), F32)))

    lo4, lo2 = 4 * b0, 4 * b0 + 2 * b1
    lo1 = lo2 + b2
    n_x = d.nb - 4
    last = len(d.lag)

    def quad_peer(q):
        c2 = 1 - b2 if q & 1 else b2
        c3 = 1 - b3 if q & 2 else b3
        return {"rep": rep + (c2 - b2) * 4 + (c3 - b3) * 8, "shard": s}, c2, c3

    def order(v, c, n):
        return v if n == 2 else c - d.NJ

    def stage(i, v, c, n):
        slot = lax.rem(order(v, c, n), d.NS[i])
        A, it, first = k.ACC, pl.ds(c, n), pl.ds(0, n)
        if i == 0:
            dst = k.R0.at[slot, first]
            return [(A.at[it, :, pl.ds(4 - lo4, 4)], dst, rep_peer(0), 0)], A.at[it, :, pl.ds(lo4, 4)], [dst]
        if i == 1:
            dst = k.R1.at[slot, first]
            return [(A.at[it, o, pl.ds(lo4, 4)], dst, x_peer, None)], A.at[it, s, pl.ds(lo4, 4)], [dst]
        if i == 2:
            dst = k.R2.at[slot, first]
            src = A.at[it, s, pl.ds(lo2 + 2 - 4 * b1, 2)]
            return [(src, dst, rep_peer(1), 1)], A.at[it, s, pl.ds(lo2, 2)], [dst]
        mine = A.at[it, s, lo1, b3]
        if i == 3:
            copies = []
            for q in (1, 2, 3):
                peer, c2, c3 = quad_peer(q)
                copies.append((A.at[it, s, lo2 + c2, c3], k.R3.at[slot, q - 1, first], peer, 1 + q))
            return copies, mine, [k.R3.at[slot, q, first] for q in range(3)]
        if i < d.first_ag:
            dst = k.RX.at[i - 4, slot, first]
            return [(mine, dst, rep_peer(i), None)], mine, [dst]
        if i == d.first_ag:
            return [(mine, mine, quad_peer(q)[0], 1 + q) for q in (1, 2, 3)], None, None
        bitno = 1 - (i - d.first_ag - 1)
        at = A.at[it, s, pl.ds(lo2, 2)] if bitno == 1 else A.at[it, s, pl.ds(lo4, 4)]
        return [(at, at, rep_peer(bitno), bitno)], None, None

    def chunks_of(v, kinds):
        if isinstance(v, int):
            grp, r = divmod(max(v - d.V0, 0), d.GU)
            found = [(0 <= v < d.NJ, 2 * v, 2), (d.NJ <= v < d.V0, v + d.NJ, 1)]
            found.append((v >= d.V0 and v < d.NVS and grp > 0 and r < 3, 2 * d.NJ + d.NP + 3 * (grp - 1) + r, 1))
            return [f for f in found if f[0]]
        found = []
        if 2 in kinds:
            found.append((jnp.logical_and(v >= 0, v < d.NJ), 2 * v, 2))
        if 1 in kinds:
            w = jnp.maximum(v - d.V0, 0)
            grp, r = lax.div(w, d.GU), lax.rem(w, d.GU)
            late = v >= d.V0
            c = jnp.where(late, 2 * d.NJ + d.NP + 3 * (grp - 1) + r, v + d.NJ)
            ok = jnp.where(late, jnp.logical_and(grp > 0, r < 3), v >= d.NJ)
            found.append((jnp.logical_and(ok, v < d.NVS), c, 1))
        return found

    def out_copy(v, c, n):
        it = pl.ds(c, n)
        return pltpu.make_async_copy(k.ACC.at[it, s], gr_o.at[it], k.OS.at[lax.rem(order(v, c, n), d.NSX)])

    def begin(i, v, c, n):
        if i == last:
            out_copy(v, c, n).start()
            return
        copies, _, _ = stage(i, v, c, n)
        slot = lax.rem(order(v, c, n), d.NS[i])
        for at, (src, dst, peer, credit) in enumerate(copies):
            if i >= d.first_ag:
                pl.semaphore_wait(k.CR.at[credit], 1)
            remote(src, dst, k.SS.at[i, slot, at], k.SR.at[i, slot, at], peer).start()

    def finish(i, v, c, n):
        if i == last:
            out_copy(v, c, n).wait()
            return
        copies, target, terms = stage(i, v, c, n)
        slot = lax.rem(order(v, c, n), d.NS[i])
        for at, (src, dst, peer, credit) in enumerate(copies):
            remote(src, dst, k.SS.at[i, slot, at], k.SR.at[i, slot, at], peer).wait()
        if terms is not None:
            total = target[...].astype(F32) + terms[0][...].astype(F32)
            for term in terms[1:]:
                total = total + term[...].astype(F32)
            target[...] = total.astype(BF16)
            for _, _, peer, credit in copies:
                if credit is not None:
                    pl.semaphore_signal(k.CR.at[credit], inc=1, device_id=peer, device_id_type=MESH)

    def tick(t, kinds=(2, 1)):
        for what, ticks in ((finish, d.E), (begin, d.B)):
            for i in range(last, -1, -1):
                v = t - ticks[i]
                for cond, c, n in chunks_of(v, kinds):
                    guarded(cond, functools.partial(what, i, v, c, n))

    def put_cols(c, sh, value):
        value = value.astype(BF16)
        for p in range(8):
            for z in range(2):
                k.ACC[c, sh, p, z, :, :] = value[p * d.PR:(p + 1) * d.PR, z * LANES:(z + 1) * LANES]

    def put_out(c, n, value):
        value = value.astype(BF16)
        per = d.D // LANES // 2
        for sh in range(2):
            for p in range(8):
                for h in range(BLK // LANES):
                    t = n * (BLK // LANES) + h
                    k.ACC[c, sh, p, t // per, pl.ds((t % per) * d.PO, d.PO), :] = value[
                        sh * LANES + p * d.PO:sh * LANES + (p + 1) * d.PO, h * LANES:(h + 1) * LANES
                    ]

    f_at = d.off["fcb"][0]
    MB = SEQ_LEN
    C1, C3 = GELU_C, GELU_C * 0.044715
    S1, S3 = 2.0 * GELU_C, 2.0 * GELU_C * 0.134145

    g_done = n_att + d.M // HA
    assert g_done >= G_LAG[2]

    def mlp(j, _):
        wait_own(j)
        g_tick(j + g_done)
        fcb = jnp.concatenate(
            [v[:, pl.ds(pl.multiple_of(f_at + j * LANES, LANES), LANES)] for v in (k.VA, k.VB)], axis=1
        )

        def rows_step(i):
            rows = pl.ds(i * MB, MB)
            wfj, woj = k.WF[j], k.WO[pl.ds(pl.multiple_of(j * BLK, BLK), BLK), :]
            c = k.COT[rows, :]
            pre = nn(k.N2[rows, :], wfj) + fcb
            d_act = nt(c, woj)
            sq = pre * pre
            h = 0.5 + 0.5 * jnp.tanh(pre * (C1 + C3 * sq))
            a = pre * h
            slope = h + a * (1.0 - h) * (S1 + S3 * sq)
            d_pre = d_act * slope
            ab, db = a.astype(BF16), d_pre.astype(BF16)
            k.ACTT[:, rows] = ab.T
            k.DPRE[rows, :] = db
            k.ACT[rows, pl.ds(pl.multiple_of(j * BLK, BLK), BLK)] = ab
            k.DN2[rows, :] += nt(db, wfj)
            return jnp.sum(d_pre, axis=0, keepdims=True)

        total = sum(rows_step(i) for i in range(d.M // MB))
        at = pl.ds(pl.multiple_of(f_at + j * LANES, LANES), LANES)
        k.VG[0, :, at] = total[:, :LANES]
        k.VG[1, :, at] = total[:, LANES:]
        for n in range(d.NP):
            put_out(2 * j, n, nn(k.ACTT[...], k.COT[:, n * BLK:(n + 1) * BLK]))
        for sh in range(2):
            row = pl.ds(sh * d.DH, d.DH)
            put_cols(2 * j + 1, sh, nn(k.N2T[row, :], k.DPRE[...]))
        tick(j, (2,))
        return 0

    lax.fori_loop(0, d.NJ, mlp, 0)

    g2 = full("ln2g")

    def norm2_back(i, sums):
        rows = pl.ds(pl.multiple_of(i * LR, LR), LR)
        xhat, r = norm_rows(k.HRES[rows, :])
        dn = k.DN2[rows, :]
        gg = dn * g2
        dh = k.COT[rows, :].astype(F32) + r * (
            gg - jnp.mean(gg, axis=-1, keepdims=True) - xhat * jnp.mean(gg * xhat, axis=-1, keepdims=True)
        )
        k.DN2[rows, :] = dh
        k.N2[rows, :] = dh.astype(BF16)
        add = lambda v: jnp.sum(v, axis=0, keepdims=True)
        return sums[0] + add(dn * xhat), sums[1] + add(dn), sums[2] + add(dh)

    zrow = jnp.zeros((1, d.D), F32)
    sums = lax.fori_loop(0, d.M // LR, norm2_back, (zrow, zrow, zrow))
    put_vec("ln2g", sums[0])
    put_vec("ln2b", sums[1])
    put_vec("projb", sums[2])

    def transpose_att(i, _):
        rows = pl.ds(pl.multiple_of(i * HA, HA), HA)
        k.N2T[:, rows] = k.ATT[rows, :].T
        return 0

    lax.fori_loop(0, d.M // HA, transpose_att, 0)

    def proj_cols(n, _):
        c = 2 * d.NJ + n
        cols = pl.ds(pl.multiple_of(n * BLK, BLK), BLK)
        for sh in range(2):
            put_cols(c, sh, nn(k.N2T[sh * d.DH:(sh + 1) * d.DH, :], k.N2[:, cols]))
        tick(d.NJ + n)
        return 0

    lax.fori_loop(0, d.NP, proj_cols, 0)

    def att_rows(i, _):
        rows = pl.ds(pl.multiple_of(i * RB, RB), RB)
        k.N1[rows, :] = nt(k.N2[rows, :], k.WP[...]).astype(BF16)
        return 0

    lax.fori_loop(0, d.M // RB, att_rows, 0)

    g1, be1 = full("ln1g"), full("ln1b")

    def transpose_n1(i, _):
        rows = pl.ds(pl.multiple_of(i * HA, HA), HA)
        xhat, _r = norm_rows(k.T[rows, :].astype(F32))
        k.N2T[:, rows] = (xhat * g1 + be1).astype(BF16).T
        return 0

    lax.fori_loop(0, d.M // HA, transpose_n1, 0)

    def attend_back(seq, hp):
        rows, cols = unit_refs(seq, hp)
        q2, k2, v2 = (k.QKV[rows, c] for c in cols)
        do2 = k.N1[rows, pl.ds(pl.multiple_of(hp * LANES, LANES), LANES)]
        dq = [None] * NQB
        dk = [None] * NQB
        dv = [None] * NQB

        def acc(lst, n, value):
            lst[n] = value if lst[n] is None else lst[n] + value

        for mask in head_mask:
            km = jnp.where(mask, k2, zero)
            for i in range(NQB):
                klen = (i + 1) * QB
                qm = jnp.where(mask, q2[i * QB:klen], zero)
                dom = jnp.where(mask, do2[i * QB:klen], zero)
                sc = nt(k2[:klen], qm)
                diag = jnp.where(tri_t, sc[klen - QB:], NEG)
                sc = diag if i == 0 else jnp.concatenate([sc[:klen - QB], diag], axis=0)
                top = jnp.max(sc, axis=0, keepdims=True)
                e = jnp.exp(sc - top)
                pr = e * (1.0 / jnp.sum(e, axis=0, keepdims=True))
                dp = nt(v2[:klen], dom)
                delta = jnp.sum(pr * dp, axis=0, keepdims=True)
                ds = (pr * (dp - delta)).astype(BF16)
                dvi = nn(pr.astype(BF16), dom)
                dki = nn(ds, qm)
                for n in range(i + 1):
                    acc(dv, n, dvi[n * QB:(n + 1) * QB])
                    acc(dk, n, dki[n * QB:(n + 1) * QB])
                acc(dq, i, tn(ds, km[:klen]))
        sq = sv = None
        for n in range(NQB):
            r = pl.ds(pl.multiple_of(seq * SEQ_LEN + n * QB, QB), QB)
            dqn = dq[n] * (HEAD_DIM ** -0.5)
            k.QKV[r, cols[0]] = dqn.astype(BF16)
            k.QKV[r, cols[1]] = dk[n].astype(BF16)
            k.QKV[r, cols[2]] = dv[n].astype(BF16)
            a, b = jnp.sum(dqn, axis=0, keepdims=True), jnp.sum(dv[n], axis=0, keepdims=True)
            sq, sv = (a, b) if sq is None else (sq + a, sv + b)
        at = pl.ds(pl.multiple_of(d.off["qvb"][0] + hp * LANES, LANES), LANES)
        for half, value in ((0, sq), (1, sv)):
            k.VG[half, :, at] = k.VG[half, :, at] + value

    for half in range(2):
        at, n = d.off["qvb"]
        k.VG[half, :, at:at + n] = jnp.zeros((1, n), F32)

    def group(grp, _):
        v0 = d.V0 + grp * d.GU

        def unit(u, _):
            attend_back(lax.div(u, 2), 2 * grp + lax.rem(u, 2))
            tick(v0 + u)
            return 0

        lax.fori_loop(0, d.GU, unit, 0)

        def part_step(part, _):
            c = 2 * d.NJ + d.NP + 3 * grp + part
            cols = pl.ds(pl.multiple_of(part * d.D + grp * BLK, BLK), BLK)
            for sh in range(2):
                put_cols(c, sh, nn(k.N2T[sh * d.DH:(sh + 1) * d.DH, :], k.QKV[:, cols]))

            return 0

        lax.fori_loop(0, 3, part_step, 0)
        return 0

    lax.fori_loop(0, d.NP, group, 0)

    HB = 256
    NB = d.M // HB

    def norm1_back(i):
        rows = pl.ds(i * HB, HB)
        dn = nt(k.QKV[rows, :], k.WQ[...])
        xhat, r = norm_rows(k.T[rows, :].astype(F32))
        gg = dn * g1
        dx = k.DN2[rows, :] + r * (
            gg - jnp.mean(gg, axis=-1, keepdims=True) - xhat * jnp.mean(gg * xhat, axis=-1, keepdims=True)
        )
        k.COT[rows, :] = dx.astype(BF16)
        return jnp.sum(dn * xhat, axis=0, keepdims=True), jnp.sum(dn, axis=0, keepdims=True)

    bout = full("outb")

    def out_rows(i):
        rows = pl.ds(i * HB, HB)
        k.N2[rows, :] = (k.HRES[rows, :] + nn(k.ACT[rows, :], k.WO[...]) + bout).astype(BF16)

    def vec_copy(i):
        src = k.VG.at[o] if i == 0 else k.VG.at[s]
        peer = x_peer if i == 0 else rep_peer(i - 1)
        return remote(src, k.VR.at[i], k.VS.at[i], k.VQ.at[i], peer)

    n_v = d.nb + 1
    xcopy = pltpu.make_async_copy(k.COT, dx_o, k.LS.at[0])
    bcopy = pltpu.make_async_copy(k.N2, out_o, k.LS.at[1])
    at_block, at_vec, sums = 0, 0, (zrow, zrow)
    for t in range(d.VD, d.NVS + d.E[-1]):
        tick(t)
        if at_block > NB and at_vec < n_v:
            vec_copy(at_vec).wait()
            k.VG[s] = k.VG[s] + k.VR[at_vec]
            at_vec += 1
            if at_vec < n_v:
                vec_copy(at_vec).start()
        for _ in range(DRAIN[t - d.VD] if t - d.VD < len(DRAIN) else 2 * NB):
            if at_block < NB:
                a, b = norm1_back(at_block)
                sums = sums[0] + a, sums[1] + b
                if at_block == NB - 1:
                    put_vec("ln1g", sums[0])
                    put_vec("ln1b", sums[1])
                    xcopy.start()
                    vec_copy(0).start()
            elif at_block < 2 * NB:
                out_rows(at_block - NB)
                if at_block == 2 * NB - 1:
                    bcopy.start()
            at_block += 1
    assert at_block >= 2 * NB and at_vec == n_v
    vo_o[...] = k.VG[s]
    xcopy.wait()
    bcopy.wait()


def per_device(d, tok, g1, be1, wq, qvb, wp, pb, g2, be2, wf, fb, wo, ob, cot):
    names, scratch = scratch_of(d)
    vec = sum(
        lax.pad(v.astype(F32), jnp.zeros((), F32), [(at, d.NV - at - n, 0)])
        for v, (at, n) in zip((g1, be1, qvb, pb, g2, be2, ob, fb), d.off.values())
    ).reshape(1, d.NV)
    hbm = pl.BlockSpec(memory_space=pl.ANY)
    vmem = pl.BlockSpec(memory_space=pltpu.VMEM)
    out, dx, gr, vo = pl.pallas_call(
        functools.partial(block_kernel, d, names),
        out_shape=(
            jax.ShapeDtypeStruct((d.M, d.D), BF16),
            jax.ShapeDtypeStruct((d.M, d.D), BF16),
            jax.ShapeDtypeStruct((d.NCH, 8, 2, d.PR, LANES), BF16),
            jax.ShapeDtypeStruct((1, d.NV), F32),
        ),
        in_specs=[hbm] * 6 + [vmem],
        out_specs=(hbm, hbm, hbm, vmem),
        scratch_shapes=scratch,
        compiler_params=pltpu.CompilerParams(
            collective_id=0, has_side_effects=True, vmem_limit_bytes=67_043_328
        ),
        name="block",
    )(tok, cot, wq, wp, wf, wo, vec)
    vecs_out = tuple(jax.ShapeDtypeStruct((n,), F32) for _, n in d.off.values())
    g_q, g_p, g_fc, g_out, *v = pl.pallas_call(
        functools.partial(finish_kernel, d),
        out_shape=tuple(
            jax.ShapeDtypeStruct(shape, F32)
            for shape in ((d.DH, 3 * d.D), (d.DH, d.D), (d.DH, d.FF), (d.FH, d.D))
        ) + vecs_out,
        in_specs=[hbm, vmem],
        out_specs=(hbm,) * 4 + (vmem,) * len(vecs_out),
        scratch_shapes=[
            pltpu.VMEM((d.NCH, 8, 2, d.PR, LANES), BF16),
            pltpu.VMEM((2 * d.NJ + 8 * d.NP, d.DH, LANES), F32),
            pltpu.VMEM((d.NJ, LANES, d.D), F32),
            pltpu.SemaphoreType.DMA((d.NCH,)),
            pltpu.SemaphoreType.DMA((d.NCH,)),
        ],
        compiler_params=pltpu.CompilerParams(vmem_limit_bytes=67_043_328),
        name="finish",
    )(gr, vo)
    v = dict(zip(d.off, v))
    return (
        out, dx, v["ln1g"], v["ln1b"], g_q, v["qvb"], g_p, v["projb"],
        v["ln2g"], v["ln2b"], g_fc, v["fcb"], g_out, v["outb"],
    )


def finish_kernel(d, gr, vo, g_q, g_p, g_fc, g_out, *refs):
    outs, (G, C, O, si, so) = refs[:len(d.off)], refs[len(d.off):]
    for ref, (at, n) in zip(outs, d.off.values()):
        ref[...] = vo[0, at:at + n]

    def load(c, _):
        pltpu.make_async_copy(gr.at[c], G.at[c], si.at[c]).start()
        return 0

    lax.fori_loop(0, d.NCH, load, 0)

    def arrived(c):
        pltpu.make_async_copy(gr.at[c], G.at[c], si.at[c]).wait()

    def cols_of(c, slot):
        arrived(c)
        for z in range(2):
            for p in range(8):
                C[slot + z, p * d.PR:(p + 1) * d.PR, :] = G[c, p, z].astype(F32)

    per = d.D // LANES // 2

    def out_copy(j):
        return pltpu.make_async_copy(O.at[j], g_out.at[pl.ds(mult(j * LANES, LANES), LANES), :], so.at[2 * j])

    def col_copies(dst, slot, cols, sem):
        return [
            pltpu.make_async_copy(C.at[slot + z], dst.at[:, pl.ds(mult(col, LANES), LANES)], sem)
            for z, col in enumerate(cols)
        ]

    def fc_copies(j):
        return col_copies(g_fc, 2 * j, (j * LANES, d.FH + j * LANES), so.at[2 * j + 1])

    def wide_copies(i):
        c, slot = 2 * d.NJ + i, 2 * (d.NJ + i)
        if i < d.NP:
            return col_copies(g_p, slot, (i * BLK, i * BLK + LANES), so.at[c])
        grp, part = divmod(i - d.NP, 3)
        col = part * d.D + grp * BLK
        return col_copies(g_q, slot, (col, col + LANES), so.at[c])

    def mlp(j, _):
        c = 2 * j
        arrived(c)
        for p in range(8):
            for t in range(2 * per):
                O[j, p * d.PO:(p + 1) * d.PO, t * LANES:(t + 1) * LANES] = G[
                    c, p, t // per, (t % per) * d.PO:(t % per + 1) * d.PO, :
                ].astype(F32)
        out_copy(j).start()
        cols_of(c + 1, 2 * j)
        for copy in fc_copies(j):
            copy.start()
        return 0

    lax.fori_loop(0, d.NJ, mlp, 0)
    for i in range(4 * d.NP):
        cols_of(2 * d.NJ + i, 2 * (d.NJ + i))
        for copy in wide_copies(i):
            copy.start()

    def drain(j, _):
        out_copy(j).wait()
        pair = C.at[pl.ds(0, 2)]
        pltpu.make_async_copy(pair, pair, so.at[2 * j + 1]).wait()
        return 0

    lax.fori_loop(0, d.NJ, drain, 0)
    for i in range(4 * d.NP):
        pair = C.at[pl.ds(0, 2)]
        pltpu.make_async_copy(pair, pair, so.at[2 * d.NJ + i]).wait()


def solution(mesh):
    def whole(tok, *rest):
        d = dims_of(mesh, tok.shape[0] // (mesh.shape["rep"] * mesh.shape["shard"]), tok.shape[1], rest[9].shape[0])
        both_axes, one, two = P(("rep", "shard"), None), P("shard"), P("shard", None)
        in_specs = (both_axes, one, one, two, one, two, one, one, one, two, one, two, one, both_axes)
        out_specs = (both_axes, both_axes, one, one, two, one, two, one, one, one, two, one, two, one)
        return jax.shard_map(
            functools.partial(per_device, d), mesh=mesh, in_specs=in_specs, out_specs=out_specs, check_vma=False
        )(tok, *rest)

    return whole
```

```python
import functools
import types

import jax
import jax.numpy as jnp
from jax import lax
from jax.experimental import pallas as pl
from jax.experimental.pallas import tpu as pltpu
from jax.sharding import PartitionSpec as P

HEAD_DIM = 64
SEQ_LEN = 512
EPS = 1e-05
GELU_C = 0.7978845608028654
F32, BF16 = jnp.float32, jnp.bfloat16
MESH = pl.DeviceIdType.MESH
LANES = 128
BLK = 256
NEG = -1e30
DRAIN = (0, 0, 1, 1, 1, 1, 1, 1, 1, 1)
VECS = ("ln1g", "ln1b", "qvb", "projb", "ln2g", "ln2b", "outb", "fcb")


def dims_of(mesh, rows, width, ff):
    d = types.SimpleNamespace()
    d.R, d.S = mesh.shape["rep"], mesh.shape["shard"]
    d.nb = d.R.bit_length() - 1
    assert d.S == 2 and d.R == 1 << d.nb and d.nb >= 4
    d.M, d.D, d.FF = rows, width, ff
    d.DH, d.FH = width // 2, ff // 2
    d.NJ = ff // BLK
    d.NP = width // BLK
    d.NH2 = width // LANES
    d.NSEQ = rows // SEQ_LEN
    d.NCH = 2 * d.NJ + 4 * d.NP
    d.PR = d.DH // 8
    d.PO = LANES // 8
    half = {"qvb": width, "fcb": ff // 2}
    d.off, at = {}, 0
    for name in VECS:
        d.off[name] = (at, half.get(name, width // 2))
        at += d.off[name][1]
    d.NV = at
    d.lag = [1, 3, 2, 2] + [1] * (d.nb - 4) + [2, 2, 1]
    d.NS = [2 * lag for lag in d.lag]
    d.NSX = max(d.NS)
    d.first_ag = d.nb
    d.B, d.E, at = [], [], 0
    for i, lag in enumerate(d.lag + [1]):
        at += i == d.first_ag
        d.B.append(at)
        at += lag
        d.E.append(at)
    d.V0 = d.NJ + d.NP
    d.GU = 2 * d.NSEQ
    assert d.GU >= 3
    d.VD = d.V0 + d.NP * d.GU
    d.NVS = d.VD + 3
    d.NQP = 6
    d.QW = 3 * width // d.NQP
    return d


def scratch_of(d):
    vm, sem = pltpu.VMEM, pltpu.SemaphoreType.DMA
    P8 = (2, d.PR, LANES)
    n_x = d.nb - 4
    items = [
        ("WQ", vm((d.D, 3 * d.D), BF16)),
        ("WP", vm((d.D, d.D), BF16)),
        ("WF", vm((d.NJ, d.D, BLK), BF16)),
        ("WO", vm((d.FF, d.D), BF16)),
        ("ACC", vm((d.NCH, 2, 8) + P8, BF16)),
        ("R0", vm((d.NS[0], 2, 2, 4) + P8, BF16)),
        ("R1", vm((d.NS[1], 2, 4) + P8, BF16)),
        ("R2", vm((d.NS[2], 2, 2) + P8, BF16)),
        ("R3", vm((d.NS[3], 3, 2, d.PR, LANES), BF16)),
        ("RX", vm((max(n_x, 1), d.NSX, 2, d.PR, LANES), BF16)),
        ("QKV", vm((d.M, 3 * d.D), BF16)),
        ("T", vm((d.M, d.D), BF16)),
        ("COT", vm((d.M, d.D), BF16)),
        ("N1", vm((d.M, d.D), BF16)),
        ("ATT", vm((d.M, d.D), BF16)),
        ("N2", vm((d.M, d.D), BF16)),
        ("N2T", vm((d.D, d.M), BF16)),
        ("HRES", vm((d.M, d.D), F32)),
        ("DN2", vm((d.M, d.D), F32)),
        ("ACT", vm((d.M, d.FF), BF16)),
        ("ACTT", vm((BLK, d.M), BF16)),
        ("DPRE", vm((d.M, BLK), BF16)),
        ("VA", vm((1, d.NV), F32)),
        ("VB", vm((1, d.NV), F32)),
        ("VX", vm((1, d.NV), F32)),
        ("VG", vm((2, 1, d.NV), F32)),
        ("VR", vm((d.nb + 1, 1, d.NV), F32)),
        ("LS", sem((4 + d.NJ,))),
        ("GS", sem((3, d.NQP + 1 + d.NJ))),
        ("GR", sem((3, d.NQP + 1 + d.NJ))),
        ("SS", sem((len(d.lag), d.NSX, 3))),
        ("SR", sem((len(d.lag), d.NSX, 3))),
        ("OS", sem((d.NSX,))),
        ("CR", pltpu.SemaphoreType.REGULAR((5,))),
        ("VS", sem((d.nb + 2,))),
        ("VQ", sem((d.nb + 2,))),
    ]
    return [n for n, _ in items], [s for _, s in items]


def nt(a, b):
    return lax.dot_general(a, b, (((1,), (1,)), ((), ())), preferred_element_type=F32)


def nn(a, b):
    return jnp.dot(a, b, preferred_element_type=F32)


def tn(a, b):
    return lax.dot_general(a, b, (((0,), (0,)), ((), ())), preferred_element_type=F32)


def norm_rows(v):
    c = v - jnp.mean(v, axis=-1, keepdims=True)
    r = lax.rsqrt(jnp.mean(c * c, axis=-1, keepdims=True) + EPS)
    return c * r, r


def mult(x, m):
    return x if isinstance(x, int) else pl.multiple_of(x, m)


def guarded(cond, fn):
    if isinstance(cond, bool):
        if cond:
            fn()
    else:
        pl.when(cond)(fn)


def both(a, b):
    if isinstance(a, bool):
        return b if a else False
    if isinstance(b, bool):
        return a if b else False
    return jnp.logical_and(a, b)


def block_kernel(d, names, tok, cot, wq, wp, wf, wo, vec, out_o, dx_o, gr_o, vo_o, *scratch):
    k = types.SimpleNamespace(**dict(zip(names, scratch)))
    rep, s = lax.axis_index("rep"), lax.axis_index("shard")
    bit = [lax.rem(lax.div(rep, 1 << i), 2) for i in range(d.nb)]

    def rep_peer(i):
        return {"rep": rep + (1 - 2 * bit[i]) * (1 << i), "shard": s}

    x_peer = {"rep": rep, "shard": 1 - s}
    b0, b1, b2, b3 = bit[:4]
    o = 1 - s

    barrier = pltpu.get_barrier_semaphore()
    peers = [x_peer] + [rep_peer(i) for i in range(d.nb)]
    peers.append({"rep": rep + (1 - 2 * b2) * 4 + (1 - 2 * b3) * 8, "shard": s})
    for peer in peers:
        pl.semaphore_signal(barrier, inc=1, device_id=peer, device_id_type=MESH)
    pl.semaphore_wait(barrier, len(peers))

    def remote(src, dst, ss, rs, peer):
        return pltpu.make_async_remote_copy(
            src_ref=src, dst_ref=dst, send_sem=ss, recv_sem=rs, device_id=peer, device_id_type=MESH
        )

    g = b0 * 2 + b1
    QR, OR = d.DH // 4, LANES // 4
    NQP, NG = d.NQP, d.NQP + 1 + d.NJ
    vcopy = remote(vec, k.VX, k.VS.at[d.nb + 1], k.VQ.at[d.nb + 1], x_peer)
    vcopy.start()
    tcopy = pltpu.make_async_copy(tok, k.T, k.LS.at[0])
    tcopy.start()

    def gather_copies(hop, p):
        if isinstance(p, int) and p <= NQP:
            ref, src = (k.WQ, wq) if p < NQP else (k.WP, wp)
            cols = pl.ds(p * d.QW, d.QW) if p < NQP else pl.ds(0, d.D)
            if hop == 0:
                return [(src.at[pl.ds(g * QR, QR), cols], ref.at[pl.ds(s * d.DH + g * QR, QR), cols])]
            if hop == 1:
                at = ref.at[pl.ds(o * d.DH + g * QR, QR), cols]
            else:
                at = ref.at[pl.ds(o * d.DH + b0 * 2 * QR, 2 * QR), cols]
            return [(at, at)]
        j = p - NQP - 1
        if hop == 0:
            pairs = []
            for strip in range(2):
                col = mult(strip * d.FH + j * LANES, LANES)
                pairs.append((
                    wf.at[pl.ds(g * QR, QR), pl.ds(col, LANES)],
                    k.WF.at[j, pl.ds(s * d.DH + g * QR, QR), pl.ds(strip * LANES, LANES)],
                ))
            pairs.append((
                wo.at[pl.ds(mult(j * LANES + g * OR, OR), OR), :],
                k.WO.at[pl.ds(j * BLK + s * LANES + g * OR, OR), :],
            ))
            return pairs
        if hop == 1:
            fa = k.WF.at[j, pl.ds(o * d.DH + g * QR, QR), :]
            oa = k.WO.at[pl.ds(j * BLK + o * LANES + g * OR, OR), :]
        else:
            fa = k.WF.at[j, pl.ds(o * d.DH + b0 * 2 * QR, 2 * QR), :]
            oa = k.WO.at[pl.ds(j * BLK + o * LANES + b0 * 2 * OR, 2 * OR), :]
        return [(fa, fa), (oa, oa)]

    hop_peer = [x_peer, rep_peer(1), rep_peer(0)]

    def g_start(hop, p):
        for a, b in gather_copies(hop, p):
            remote(a, b, k.GS.at[hop, p], k.GR.at[hop, p], hop_peer[hop]).start()

    def g_wait(hop, p):
        if isinstance(p, int) and p <= NQP:
            (a, b), = gather_copies(hop, p)
            remote(a, b, k.GS.at[hop, p], k.GR.at[hop, p], hop_peer[hop]).wait()
        else:
            rows = k.WF.at[0, pl.ds(0, d.D // 4 * (2 if hop == 2 else 1)), :]
            pltpu.make_async_copy(rows, rows, k.GS.at[hop, p]).wait()
            pltpu.make_async_copy(rows, rows, k.GR.at[hop, p]).wait()

    G_LAG = (0, 2, 3)

    def g_tick(t):
        for hop in range(2, -1, -1):
            q = t - G_LAG[hop]

            def do(hop=hop, q=q):
                g_wait(hop, q + NQP + 1)
                if hop < 2:
                    g_start(hop + 1, q + NQP + 1)

            guarded(both(q >= 0, q < d.NJ), do)

    own_q = pltpu.make_async_copy(wq, k.WQ.at[pl.ds(s * d.DH, d.DH), :], k.LS.at[1])
    own_q.start()
    for p in range(NQP + 1):
        g_start(0, p)
    own_p = pltpu.make_async_copy(wp, k.WP.at[pl.ds(s * d.DH, d.DH), :], k.LS.at[2])
    ccopy = pltpu.make_async_copy(cot, k.COT, k.LS.at[3])

    def start_blocks(j, _):
        g_start(0, j + NQP + 1)
        return 0

    def start_own(j, _):
        for strip in range(2):
            pltpu.make_async_copy(
                wf.at[:, pl.ds(mult(strip * d.FH + j * LANES, LANES), LANES)],
                k.WF.at[j, pl.ds(s * d.DH, d.DH), pl.ds(strip * LANES, LANES)],
                k.LS.at[4 + j],
            ).start()
        pltpu.make_async_copy(
            wo.at[pl.ds(mult(j * LANES, LANES), LANES), :],
            k.WO.at[pl.ds(j * BLK + s * LANES, LANES), :],
            k.LS.at[4 + j],
        ).start()
        return 0

    def wait_own(j):
        pltpu.make_async_copy(k.WF.at[0], k.WF.at[0], k.LS.at[4 + j]).wait()

    vcopy.wait()
    own, oth = vec[...], k.VX[...]
    first = s == 0
    k.VA[...] = jnp.where(first, own, oth)
    k.VB[...] = jnp.where(first, oth, own)

    def full(name):
        at, n = d.off[name]
        return jnp.concatenate([k.VA[:, at:at + n], k.VB[:, at:at + n]], axis=1)

    def put_vec(name, value):
        at, n = d.off[name]
        k.VG[0, :, at:at + n] = value[:, :n]
        k.VG[1, :, at:at + n] = value[:, n:]

    tcopy.wait()
    LR = 64

    def norm1(i, _):
        rows = pl.ds(pl.multiple_of(i * LR, LR), LR)
        xhat, _r = norm_rows(k.T[rows, :].astype(F32))
        k.N1[rows, :] = (xhat * full("ln1g") + full("ln1b")).astype(BF16)
        return 0

    half = d.M // LR // 2
    lax.fori_loop(0, half, norm1, 0)
    g_wait(0, 0)
    g_start(1, 0)
    lax.fori_loop(half, 2 * half, norm1, 0)
    own_q.wait()
    RB = 512
    per_part = NQP // 3

    def qkv_piece(p):
        part, col = p // per_part, p % per_part * d.QW
        bias = None
        if part != 1:
            at = d.off["qvb"][0] + col
            bias = (k.VA if part == 0 else k.VB)[:, at:at + d.QW]

        def step(i, _):
            rows = pl.ds(pl.multiple_of(i * RB, RB), RB)
            y = nn(k.N1[rows, :], k.WQ[:, p * d.QW:(p + 1) * d.QW])
            y = (y if bias is None else y + bias).astype(BF16)
            if part == 0:
                y = y * jnp.asarray(HEAD_DIM ** -0.5, BF16)
            k.QKV[rows, p * d.QW:(p + 1) * d.QW] = y
            return 0

        lax.fori_loop(0, d.M // RB, step, 0)

    own_p.start()
    ccopy.start()
    for p in range(1, NQP):
        g_wait(0, p)
        g_start(1, p)
        if p >= 2:
            g_wait(1, p - 2)
            g_start(2, p - 2)
        if p >= 4:
            g_wait(2, p - 4)
            qkv_piece(p - 4)
        if p == 1:
            lax.fori_loop(0, d.NJ, start_blocks, 0)
        if p == NQP - 1:
            lax.fori_loop(0, d.NJ, start_own, 0)
    g_wait(1, NQP - 2)
    g_start(2, NQP - 2)
    for p in range(NQP - 4, NQP):
        g_wait(2, p)
        qkv_piece(p)
        if p == 2:
            g_wait(1, NQP - 1)
            g_start(2, NQP - 1)
            g_wait(0, NQP)
            g_start(1, NQP)
    g_wait(1, NQP)
    g_start(2, NQP)

    lane = lax.broadcasted_iota(jnp.int32, (1, LANES), 1)
    head_mask = [lane < HEAD_DIM, lane >= HEAD_DIM]
    zero, one = jnp.zeros((), BF16), jnp.ones((), BF16)
    QB = 256
    NQB = SEQ_LEN // QB
    tri = lax.broadcasted_iota(jnp.int32, (QB, QB), 1) <= lax.broadcasted_iota(jnp.int32, (QB, QB), 0)
    tri_t = lax.broadcasted_iota(jnp.int32, (QB, QB), 0) <= lax.broadcasted_iota(jnp.int32, (QB, QB), 1)

    def unit_refs(seq, hp):
        rows = pl.ds(pl.multiple_of(seq * SEQ_LEN, SEQ_LEN), SEQ_LEN)
        cols = [pl.ds(pl.multiple_of(part * d.D + hp * LANES, LANES), LANES) for part in range(3)]
        return rows, cols

    def attend_loop(u, _):
        attend_body(2 * u)
        attend_body(2 * u + 1)
        g_tick(u)
        return 0

    def attend_body(u):
        seq, hp = lax.div(u, d.NH2), lax.rem(u, d.NH2)
        rows, cols = unit_refs(seq, hp)
        q2, k2, v2 = (k.QKV[rows, c] for c in cols)
        for i in range(NQB):
            klen = (i + 1) * QB
            parts = []
            for mask in head_mask:
                qm = jnp.where(mask, q2[i * QB:klen], zero)
                vm = jnp.where(mask, v2[:klen], one)
                sc = nt(qm, k2[:klen])
                diag = jnp.where(tri, sc[:, klen - QB:], NEG)
                sc = diag if i == 0 else jnp.concatenate([sc[:, :klen - QB], diag], axis=1)
                top = jnp.max(sc, axis=1, keepdims=True)
                e = jnp.exp(sc - top)
                parts.append(nn(e.astype(BF16), vm))
            den = jnp.where(head_mask[0], *(pltpu.roll(p, HEAD_DIM, 1) for p in parts))
            total = jnp.where(head_mask[0], *parts) / den
            out_rows = pl.ds(pl.multiple_of(seq * SEQ_LEN + i * QB, QB), QB)
            k.ATT[out_rows, pl.ds(pl.multiple_of(hp * LANES, LANES), LANES)] = total.astype(BF16)

    lax.fori_loop(0, d.NSEQ * d.NH2 // 2, attend_loop, 0)
    own_p.wait()
    g_wait(2, NQP)

    HA = SEQ_LEN

    def hres_rows(i, _):
        rows = pl.ds(pl.multiple_of(i * HA, HA), HA)
        h = k.T[rows, :].astype(F32) + nn(k.ATT[rows, :], k.WP[...]) + full("projb")
        k.HRES[rows, :] = h
        xhat, _r = norm_rows(h)
        n2 = (xhat * full("ln2g") + full("ln2b")).astype(BF16)
        k.N2[rows, :] = n2
        k.N2T[:, rows] = n2.T
        k.DN2[rows, :] = jnp.zeros((HA, d.D), F32)
        g_tick(n_att + i)
        return 0

    n_att = d.NSEQ * d.NH2 // 2
    lax.fori_loop(0, d.M // HA, hres_rows, 0)
    ccopy.wait()

    def cot_sum(i, total):
        rows = pl.ds(pl.multiple_of(i * LR, LR), LR)
        return total + jnp.sum(k.COT[rows, :].astype(F32), axis=0, keepdims=True)

    put_vec("outb", lax.fori_loop(0, d.M // LR, cot_sum, jnp.zeros((1, d.D), F32)))

    lo4, lo2 = 4 * b0, 4 * b0 + 2 * b1
    lo1 = lo2 + b2
    n_x = d.nb - 4
    last = len(d.lag)

    def quad_peer(q):
        c2 = 1 - b2 if q & 1 else b2
        c3 = 1 - b3 if q & 2 else b3
        return {"rep": rep + (c2 - b2) * 4 + (c3 - b3) * 8, "shard": s}, c2, c3

    def order(v, c, n):
        return v if n == 2 else c - d.NJ

    def stage(i, v, c, n):
        slot = lax.rem(order(v, c, n), d.NS[i])
        A, it, first = k.ACC, pl.ds(c, n), pl.ds(0, n)
        if i == 0:
            dst = k.R0.at[slot, first]
            return [(A.at[it, :, pl.ds(4 - lo4, 4)], dst, rep_peer(0), 0)], A.at[it, :, pl.ds(lo4, 4)], [dst]
        if i == 1:
            dst = k.R1.at[slot, first]
            return [(A.at[it, o, pl.ds(lo4, 4)], dst, x_peer, None)], A.at[it, s, pl.ds(lo4, 4)], [dst]
        if i == 2:
            dst = k.R2.at[slot, first]
            src = A.at[it, s, pl.ds(lo2 + 2 - 4 * b1, 2)]
            return [(src, dst, rep_peer(1), 1)], A.at[it, s, pl.ds(lo2, 2)], [dst]
        mine = A.at[it, s, lo1, b3]
        if i == 3:
            copies = []
            for q in (1, 2, 3):
                peer, c2, c3 = quad_peer(q)
                copies.append((A.at[it, s, lo2 + c2, c3], k.R3.at[slot, q - 1, first], peer, 1 + q))
            return copies, mine, [k.R3.at[slot, q, first] for q in range(3)]
        if i < d.first_ag:
            dst = k.RX.at[i - 4, slot, first]
            return [(mine, dst, rep_peer(i), None)], mine, [dst]
        if i == d.first_ag:
            return [(mine, mine, quad_peer(q)[0], 1 + q) for q in (1, 2, 3)], None, None
        bitno = 1 - (i - d.first_ag - 1)
        at = A.at[it, s, pl.ds(lo2, 2)] if bitno == 1 else A.at[it, s, pl.ds(lo4, 4)]
        return [(at, at, rep_peer(bitno), bitno)], None, None

    def chunks_of(v, kinds):
        if isinstance(v, int):
            grp, r = divmod(max(v - d.V0, 0), d.GU)
            found = [(0 <= v < d.NJ, 2 * v, 2), (d.NJ <= v < d.V0, v + d.NJ, 1)]
            found.append((v >= d.V0 and v < d.NVS and grp > 0 and r < 3, 2 * d.NJ + d.NP + 3 * (grp - 1) + r, 1))
            return [f for f in found if f[0]]
        found = []
        if 2 in kinds:
            found.append((jnp.logical_and(v >= 0, v < d.NJ), 2 * v, 2))
        if 1 in kinds:
            w = jnp.maximum(v - d.V0, 0)
            grp, r = lax.div(w, d.GU), lax.rem(w, d.GU)
            late = v >= d.V0
            c = jnp.where(late, 2 * d.NJ + d.NP + 3 * (grp - 1) + r, v + d.NJ)
            ok = jnp.where(late, jnp.logical_and(grp > 0, r < 3), v >= d.NJ)
            found.append((jnp.logical_and(ok, v < d.NVS), c, 1))
        return found

    def out_copy(v, c, n):
        it = pl.ds(c, n)
        return pltpu.make_async_copy(k.ACC.at[it, s], gr_o.at[it], k.OS.at[lax.rem(order(v, c, n), d.NSX)])

    def begin(i, v, c, n):
        if i == last:
            out_copy(v, c, n).start()
            return
        copies, _, _ = stage(i, v, c, n)
        slot = lax.rem(order(v, c, n), d.NS[i])
        for at, (src, dst, peer, credit) in enumerate(copies):
            if i >= d.first_ag:
                pl.semaphore_wait(k.CR.at[credit], 1)
            remote(src, dst, k.SS.at[i, slot, at], k.SR.at[i, slot, at], peer).start()

    def finish(i, v, c, n):
        if i == last:
            out_copy(v, c, n).wait()
            return
        copies, target, terms = stage(i, v, c, n)
        slot = lax.rem(order(v, c, n), d.NS[i])
        for at, (src, dst, peer, credit) in enumerate(copies):
            remote(src, dst, k.SS.at[i, slot, at], k.SR.at[i, slot, at], peer).wait()
        if terms is not None:
            total = target[...].astype(F32) + terms[0][...].astype(F32)
            for term in terms[1:]:
                total = total + term[...].astype(F32)
            target[...] = total.astype(BF16)
            for _, _, peer, credit in copies:
                if credit is not None:
                    pl.semaphore_signal(k.CR.at[credit], inc=1, device_id=peer, device_id_type=MESH)

    def tick(t, kinds=(2, 1)):
        for what, ticks in ((finish, d.E), (begin, d.B)):
            for i in range(last, -1, -1):
                v = t - ticks[i]
                for cond, c, n in chunks_of(v, kinds):
                    guarded(cond, functools.partial(what, i, v, c, n))

    def put_cols(c, sh, value):
        value = value.astype(BF16)
        for p in range(8):
            for z in range(2):
                k.ACC[c, sh, p, z, :, :] = value[p * d.PR:(p + 1) * d.PR, z * LANES:(z + 1) * LANES]

    def put_out(c, n, value):
        value = value.astype(BF16)
        per = d.D // LANES // 2
        for sh in range(2):
            for p in range(8):
                for h in range(BLK // LANES):
                    t = n * (BLK // LANES) + h
                    k.ACC[c, sh, p, t // per, pl.ds((t % per) * d.PO, d.PO), :] = value[
                        sh * LANES + p * d.PO:sh * LANES + (p + 1) * d.PO, h * LANES:(h + 1) * LANES
                    ]

    f_at = d.off["fcb"][0]
    MB = SEQ_LEN
    C1, C3 = GELU_C, GELU_C * 0.044715
    S1, S3 = 2.0 * GELU_C, 2.0 * GELU_C * 0.134145

    g_done = n_att + d.M // HA
    assert g_done >= G_LAG[2]

    def mlp(j, _):
        wait_own(j)
        g_tick(j + g_done)
        fcb = jnp.concatenate(
            [v[:, pl.ds(pl.multiple_of(f_at + j * LANES, LANES), LANES)] for v in (k.VA, k.VB)], axis=1
        )

        def rows_step(i):
            rows = pl.ds(i * MB, MB)
            wfj, woj = k.WF[j], k.WO[pl.ds(pl.multiple_of(j * BLK, BLK), BLK), :]
            c = k.COT[rows, :]
            pre = nn(k.N2[rows, :], wfj) + fcb
            d_act = nt(c, woj)
            sq = pre * pre
            h = 0.5 + 0.5 * jnp.tanh(pre * (C1 + C3 * sq))
            a = pre * h
            slope = h + a * (1.0 - h) * (S1 + S3 * sq)
            d_pre = d_act * slope
            ab, db = a.astype(BF16), d_pre.astype(BF16)
            k.ACTT[:, rows] = ab.T
            k.DPRE[rows, :] = db
            k.ACT[rows, pl.ds(pl.multiple_of(j * BLK, BLK), BLK)] = ab
            k.DN2[rows, :] += nt(db, wfj)
            return jnp.sum(d_pre, axis=0, keepdims=True)

        total = sum(rows_step(i) for i in range(d.M // MB))
        at = pl.ds(pl.multiple_of(f_at + j * LANES, LANES), LANES)
        k.VG[0, :, at] = total[:, :LANES]
        k.VG[1, :, at] = total[:, LANES:]
        for n in range(d.NP):
            put_out(2 * j, n, nn(k.ACTT[...], k.COT[:, n * BLK:(n + 1) * BLK]))
        for sh in range(2):
            row = pl.ds(sh * d.DH, d.DH)
            put_cols(2 * j + 1, sh, nn(k.N2T[row, :], k.DPRE[...]))
        tick(j, (2,))
        return 0

    lax.fori_loop(0, d.NJ, mlp, 0)

    g2 = full("ln2g")

    def norm2_back(i, sums):
        rows = pl.ds(pl.multiple_of(i * LR, LR), LR)
        xhat, r = norm_rows(k.HRES[rows, :])
        dn = k.DN2[rows, :]
        gg = dn * g2
        dh = k.COT[rows, :].astype(F32) + r * (
            gg - jnp.mean(gg, axis=-1, keepdims=True) - xhat * jnp.mean(gg * xhat, axis=-1, keepdims=True)
        )
        k.DN2[rows, :] = dh
        k.N2[rows, :] = dh.astype(BF16)
        add = lambda v: jnp.sum(v, axis=0, keepdims=True)
        return sums[0] + add(dn * xhat), sums[1] + add(dn), sums[2] + add(dh)

    zrow = jnp.zeros((1, d.D), F32)
    sums = lax.fori_loop(0, d.M // LR, norm2_back, (zrow, zrow, zrow))
    put_vec("ln2g", sums[0])
    put_vec("ln2b", sums[1])
    put_vec("projb", sums[2])

    def transpose_att(i, _):
        rows = pl.ds(pl.multiple_of(i * HA, HA), HA)
        k.N2T[:, rows] = k.ATT[rows, :].T
        return 0

    lax.fori_loop(0, d.M // HA, transpose_att, 0)

    def proj_cols(n):
        c = 2 * d.NJ + n
        cols = pl.ds(n * BLK, BLK)
        for sh in range(2):
            put_cols(c, sh, nn(k.N2T[sh * d.DH:(sh + 1) * d.DH, :], k.N2[:, cols]))

    def att_rows(i, _):
        rows = pl.ds(pl.multiple_of(i * RB, RB), RB)
        k.N1[rows, :] = nt(k.N2[rows, :], k.WP[...]).astype(BF16)
        return 0

    g1, be1 = full("ln1g"), full("ln1b")

    def transpose_n1(i, _):
        rows = pl.ds(pl.multiple_of(i * HA, HA), HA)
        xhat, _r = norm_rows(k.T[rows, :].astype(F32))
        k.N2T[:, rows] = (xhat * g1 + be1).astype(BF16).T
        return 0

    parts = [-(-n * (d.M // RB) // d.NP) for n in range(d.NP + 1)]
    for n in range(d.NP):
        proj_cols(n)
        if n == d.NP - 1:
            lax.fori_loop(0, d.M // HA, transpose_n1, 0)
        tick(d.NJ + n)
        lax.fori_loop(parts[n], parts[n + 1], att_rows, 0)

    def attend_back(seq, hp):
        rows, cols = unit_refs(seq, hp)
        q2, k2, v2 = (k.QKV[rows, c] for c in cols)
        do2 = k.N1[rows, pl.ds(pl.multiple_of(hp * LANES, LANES), LANES)]
        dq = [None] * NQB
        dk = [None] * NQB
        dv = [None] * NQB

        def acc(lst, n, value):
            lst[n] = value if lst[n] is None else lst[n] + value

        for mask in head_mask:
            km = jnp.where(mask, k2, zero)
            for i in range(NQB):
                klen = (i + 1) * QB
                qm = jnp.where(mask, q2[i * QB:klen], zero)
                dom = jnp.where(mask, do2[i * QB:klen], zero)
                sc = nt(k2[:klen], qm)
                diag = jnp.where(tri_t, sc[klen - QB:], NEG)
                sc = diag if i == 0 else jnp.concatenate([sc[:klen - QB], diag], axis=0)
                top = jnp.max(sc, axis=0, keepdims=True)
                e = jnp.exp(sc - top)
                pr = e * (1.0 / jnp.sum(e, axis=0, keepdims=True))
                dp = nt(v2[:klen], dom)
                delta = jnp.sum(pr * dp, axis=0, keepdims=True)
                ds = (pr * (dp - delta)).astype(BF16)
                dvi = nn(pr.astype(BF16), dom)
                dki = nn(ds, qm)
                for n in range(i + 1):
                    acc(dv, n, dvi[n * QB:(n + 1) * QB])
                    acc(dk, n, dki[n * QB:(n + 1) * QB])
                acc(dq, i, tn(ds, km[:klen]))
        sq = sv = None
        for n in range(NQB):
            r = pl.ds(pl.multiple_of(seq * SEQ_LEN + n * QB, QB), QB)
            dqn = dq[n] * (HEAD_DIM ** -0.5)
            k.QKV[r, cols[0]] = dqn.astype(BF16)
            k.QKV[r, cols[1]] = dk[n].astype(BF16)
            k.QKV[r, cols[2]] = dv[n].astype(BF16)
            a, b = jnp.sum(dqn, axis=0, keepdims=True), jnp.sum(dv[n], axis=0, keepdims=True)
            sq, sv = (a, b) if sq is None else (sq + a, sv + b)
        at = pl.ds(pl.multiple_of(d.off["qvb"][0] + hp * LANES, LANES), LANES)
        for half, value in ((0, sq), (1, sv)):
            k.VG[half, :, at] = k.VG[half, :, at] + value

    for half in range(2):
        at, n = d.off["qvb"]
        k.VG[half, :, at:at + n] = jnp.zeros((1, n), F32)

    def group(grp, _):
        v0 = d.V0 + grp * d.GU

        def unit(u, _):
            attend_back(lax.div(u, 2), 2 * grp + lax.rem(u, 2))
            tick(v0 + u)
            return 0

        lax.fori_loop(0, d.GU, unit, 0)

        def part_step(part, _):
            c = 2 * d.NJ + d.NP + 3 * grp + part
            cols = pl.ds(pl.multiple_of(part * d.D + grp * BLK, BLK), BLK)
            for sh in range(2):
                put_cols(c, sh, nn(k.N2T[sh * d.DH:(sh + 1) * d.DH, :], k.QKV[:, cols]))

            return 0

        lax.fori_loop(0, 3, part_step, 0)
        return 0

    lax.fori_loop(0, d.NP, group, 0)

    HB = 256
    NB = d.M // HB

    def norm1_back(i):
        rows = pl.ds(i * HB, HB)
        dn = nt(k.QKV[rows, :], k.WQ[...])
        xhat, r = norm_rows(k.T[rows, :].astype(F32))
        gg = dn * g1
        dx = k.DN2[rows, :] + r * (
            gg - jnp.mean(gg, axis=-1, keepdims=True) - xhat * jnp.mean(gg * xhat, axis=-1, keepdims=True)
        )
        k.COT[rows, :] = dx.astype(BF16)
        return jnp.sum(dn * xhat, axis=0, keepdims=True), jnp.sum(dn, axis=0, keepdims=True)

    bout = full("outb")

    def out_rows(i):
        rows = pl.ds(i * HB, HB)
        k.N2[rows, :] = (k.HRES[rows, :] + nn(k.ACT[rows, :], k.WO[...]) + bout).astype(BF16)

    def vec_copy(i):
        src = k.VG.at[o] if i == 0 else k.VG.at[s]
        peer = x_peer if i == 0 else rep_peer(i - 1)
        return remote(src, k.VR.at[i], k.VS.at[i], k.VQ.at[i], peer)

    n_v = d.nb + 1
    xcopy = pltpu.make_async_copy(k.COT, dx_o, k.LS.at[0])
    bcopy = pltpu.make_async_copy(k.N2, out_o, k.LS.at[1])
    at_block, at_vec, sums = 0, 0, (zrow, zrow)
    for t in range(d.VD, d.NVS + d.E[-1]):
        tick(t)
        if at_block > NB and at_vec < n_v:
            vec_copy(at_vec).wait()
            k.VG[s] = k.VG[s] + k.VR[at_vec]
            at_vec += 1
            if at_vec < n_v:
                vec_copy(at_vec).start()
        for _ in range(DRAIN[t - d.VD] if t - d.VD < len(DRAIN) else 2 * NB):
            if at_block < NB:
                a, b = norm1_back(at_block)
                sums = sums[0] + a, sums[1] + b
                if at_block == NB - 1:
                    put_vec("ln1g", sums[0])
                    put_vec("ln1b", sums[1])
                    xcopy.start()
                    vec_copy(0).start()
            elif at_block < 2 * NB:
                out_rows(at_block - NB)
                if at_block == 2 * NB - 1:
                    bcopy.start()
            at_block += 1
    assert at_block >= 2 * NB and at_vec == n_v
    vo_o[...] = k.VG[s]
    xcopy.wait()
    bcopy.wait()


def per_device(d, tok, g1, be1, wq, qvb, wp, pb, g2, be2, wf, fb, wo, ob, cot):
    names, scratch = scratch_of(d)
    vec = sum(
        lax.pad(v.astype(F32), jnp.zeros((), F32), [(at, d.NV - at - n, 0)])
        for v, (at, n) in zip((g1, be1, qvb, pb, g2, be2, ob, fb), d.off.values())
    ).reshape(1, d.NV)
    hbm = pl.BlockSpec(memory_space=pl.ANY)
    vmem = pl.BlockSpec(memory_space=pltpu.VMEM)
    out, dx, gr, vo = pl.pallas_call(
        functools.partial(block_kernel, d, names),
        out_shape=(
            jax.ShapeDtypeStruct((d.M, d.D), BF16),
            jax.ShapeDtypeStruct((d.M, d.D), BF16),
            jax.ShapeDtypeStruct((d.NCH, 8, 2, d.PR, LANES), BF16),
            jax.ShapeDtypeStruct((1, d.NV), F32),
        ),
        in_specs=[hbm] * 6 + [vmem],
        out_specs=(hbm, hbm, hbm, vmem),
        scratch_shapes=scratch,
        compiler_params=pltpu.CompilerParams(
            collective_id=0, has_side_effects=True, vmem_limit_bytes=67_043_328
        ),
        name="block",
    )(tok, cot, wq, wp, wf, wo, vec)
    vecs_out = tuple(jax.ShapeDtypeStruct((n,), F32) for _, n in d.off.values())
    out, dx, g_q, g_p, g_fc, g_out, *v = pl.pallas_call(
        functools.partial(finish_kernel, d),
        out_shape=(jax.ShapeDtypeStruct((d.M, d.D), BF16),) * 2 + tuple(
            jax.ShapeDtypeStruct(shape, F32)
            for shape in ((d.DH, 3 * d.D), (d.DH, d.D), (d.DH, d.FF), (d.FH, d.D))
        ) + vecs_out,
        in_specs=[hbm] * 3 + [vmem],
        out_specs=(hbm,) * 6 + (vmem,) * len(vecs_out),
        scratch_shapes=[
            pltpu.VMEM((d.NCH, 8, 2, d.PR, LANES), BF16),
            pltpu.VMEM((2 * d.NJ + 8 * d.NP, d.DH, LANES), F32),
            pltpu.VMEM((d.NJ, LANES, d.D), F32),
            pltpu.VMEM((2, d.M, d.D), BF16),
            pltpu.SemaphoreType.DMA((d.NCH,)),
            pltpu.SemaphoreType.DMA((d.NCH,)),
            pltpu.SemaphoreType.DMA((4,)),
        ],
        compiler_params=pltpu.CompilerParams(vmem_limit_bytes=67_043_328),
        name="finish",
    )(out, dx, gr, vo)
    v = dict(zip(d.off, v))
    return (
        out, dx, v["ln1g"], v["ln1b"], g_q, v["qvb"], g_p, v["projb"],
        v["ln2g"], v["ln2b"], g_fc, v["fcb"], g_out, v["outb"],
    )


def finish_kernel(d, out_i, dx_i, gr, vo, out_o, dx_o, g_q, g_p, g_fc, g_out, *refs):
    outs, (G, C, O, X, si, so, sx) = refs[:len(d.off)], refs[len(d.off):]
    for ref, (at, n) in zip(outs, d.off.values()):
        ref[...] = vo[0, at:at + n]

    def load(c, _):
        pltpu.make_async_copy(gr.at[c], G.at[c], si.at[c]).start()
        return 0

    lax.fori_loop(0, d.NCH, load, 0)
    rows_in = [pltpu.make_async_copy(r, X.at[i], sx.at[i]) for i, r in enumerate((out_i, dx_i))]
    rows_out = [pltpu.make_async_copy(X.at[i], r, sx.at[2 + i]) for i, r in enumerate((out_o, dx_o))]
    for copy in rows_in:
        copy.start()

    def arrived(c):
        pltpu.make_async_copy(gr.at[c], G.at[c], si.at[c]).wait()

    def cols_of(c, slot):
        arrived(c)
        for z in range(2):
            for p in range(8):
                C[slot + z, p * d.PR:(p + 1) * d.PR, :] = G[c, p, z].astype(F32)

    per = d.D // LANES // 2

    def out_copy(j):
        return pltpu.make_async_copy(O.at[j], g_out.at[pl.ds(mult(j * LANES, LANES), LANES), :], so.at[2 * j])

    def col_copies(dst, slot, cols, sem):
        return [
            pltpu.make_async_copy(C.at[slot + z], dst.at[:, pl.ds(mult(col, LANES), LANES)], sem)
            for z, col in enumerate(cols)
        ]

    def fc_copies(j):
        return col_copies(g_fc, 2 * j, (j * LANES, d.FH + j * LANES), so.at[2 * j + 1])

    def wide_copies(i):
        c, slot = 2 * d.NJ + i, 2 * (d.NJ + i)
        if i < d.NP:
            return col_copies(g_p, slot, (i * BLK, i * BLK + LANES), so.at[c])
        grp, part = divmod(i - d.NP, 3)
        col = part * d.D + grp * BLK
        return col_copies(g_q, slot, (col, col + LANES), so.at[c])

    def mlp(j, _):
        c = 2 * j
        arrived(c)
        for p in range(8):
            for t in range(2 * per):
                O[j, p * d.PO:(p + 1) * d.PO, t * LANES:(t + 1) * LANES] = G[
                    c, p, t // per, (t % per) * d.PO:(t % per + 1) * d.PO, :
                ].astype(F32)
        out_copy(j).start()
        cols_of(c + 1, 2 * j)
        for copy in fc_copies(j):
            copy.start()
        return 0

    lax.fori_loop(0, d.NJ, mlp, 0)
    for a, b in zip(rows_in, rows_out):
        a.wait()
        b.start()
    for i in range(4 * d.NP):
        cols_of(2 * d.NJ + i, 2 * (d.NJ + i))
        for copy in wide_copies(i):
            copy.start()

    def drain(j, _):
        out_copy(j).wait()
        pair = C.at[pl.ds(0, 2)]
        pltpu.make_async_copy(pair, pair, so.at[2 * j + 1]).wait()
        return 0

    lax.fori_loop(0, d.NJ, drain, 0)
    for copy in rows_out:
        copy.wait()
    for i in range(4 * d.NP):
        pair = C.at[pl.ds(0, 2)]
        pltpu.make_async_copy(pair, pair, so.at[2 * d.NJ + i]).wait()


def solution(mesh):
    def whole(tok, *rest):
        d = dims_of(mesh, tok.shape[0] // (mesh.shape["rep"] * mesh.shape["shard"]), tok.shape[1], rest[9].shape[0])
        both_axes, one, two = P(("rep", "shard"), None), P("shard"), P("shard", None)
        in_specs = (both_axes, one, one, two, one, two, one, one, one, two, one, two, one, both_axes)
        out_specs = (both_axes, both_axes, one, one, two, one, two, one, one, one, two, one, two, one)
        return jax.shard_map(
            functools.partial(per_device, d), mesh=mesh, in_specs=in_specs, out_specs=out_specs, check_vma=False
        )(tok, *rest)

    return whole
```
